32 devices in a mesh: groups: 2 (over y), seq: 4 (over z), head: 4 (over x, core).
Axes of the slice: x: 2, y: 2, z: 4, core: 2. Of those that a mesh axis runs over, the one named last changes fastest.
Arguments:
- tile_tokens: bfloat16 [16, 256, 1536], P(('groups', 'seq')), parts along dimension 0, may hold values from -6 to 6
- tile_gain: float32 [1536], replicated, may hold values from 0.1 to 1.9
- w_gate_up: bfloat16 [2, 1536, 4096], P(None, 'seq', 'head'), may hold values from -0.15625 to 0.15625
- w_down: bfloat16 [4096, 1536], P('head', 'seq'), may hold values from -0.09375 to 0.09375
- layer_scale: float32 [1536], replicated, may hold values from 1 to 8
- fc_gain: float32 [1536], replicated, may hold values from 0.1 to 1.9
- w_embed: bfloat16 [1536, 768], P(None, 'head'), may hold values from -0.15625 to 0.15625
- embed_bias: float32 [768], P('head'), may hold values from -3 to 3
- pre_emb: bfloat16 [2032, 768], P(('groups', 'seq'), 'head'), parts along dimension 0, may hold values from -6 to 6
- tile_order: int32 [2048], P('groups'), parts along dimension 0, may hold values from 0 to 1023, as said below
- valid_count: int32 [2], P('groups'), parts along dimension 0, may hold values from 256 to 1024
- slide_gain: float32 [768], replicated, may hold values from 0.1 to 1.9
- w_qkv: bfloat16 [3, 768, 768], P(None, None, 'head'), may hold values from -1.25 to 1.25
- sub_gain: float32 [768], P('head'), may hold values from 0.1 to 1.9
- w_out: bfloat16 [768, 768], P('head'), may hold values from -0.21875 to 0.21875
Outputs:
- mixed: float32 [2048, 768], P(('groups', 'seq'), 'head'), parts along dimension 0
The draws below stay inside these ranges and needn't reach their ends.
There are 2 independent parts, one for each index of `groups`. The reference program is written for one: setup_inputs(seed, part) draws one part's arguments, and reference() takes and returns one part's arrays. A program takes and returns all parts, laid end to end along the dimension named above; an argument that names none is the same for every part. Nothing has to cross between parts.
Inputs may be any that keep to these rules, and one draw needn't show every extreme that they name: `tile_order`: A permutation of 0 to 1023. For every block of 256 positions (d * 256 to (d + 1) * 256 - 1) and every block of 256 stored rows, exactly 64 positions of the first take rows of the second.
All inputs are finite; a program needn't handle non-finite values.
Results may differ from the reference program's by a relative error of at most 0.0046.
Values may be sent and summed in bfloat16 or wider, within the bound.
A program may use at most 64 MiB of HBM per device.

```python
import math
import jax
import jax.numpy as jnp
from jax import lax

DV = 1536
FF = 4096
DS = 768
HEADS = 16
HEAD_DIM = 48
PATCH = 256
NEW_DEV = 2
SEQ_DEV = 256
DILATION_SECOND = 4
DILATION_THIRD = 16
NEW = 8
PRE_DEV = 254
PRE = 1016
SLIDE_POSITIONS = 1024
PEER = 64
SEGMENT_FIRST = 1024
SEGMENT_SECOND = 1024


def shuffle_row(row_key, row_values):
    return jax.random.permutation(row_key, row_values)


def draw_tile_order(key, part):
    blocks = SLIDE_POSITIONS // SEQ_DEV
    source_key, target_key = jax.random.split(jax.random.fold_in(key, 11))
    source_keys = jax.random.split(source_key, blocks)
    local_rows = jnp.broadcast_to(jnp.arange(SEQ_DEV, dtype=jnp.int32), (blocks, SEQ_DEV))
    shuffled = jax.vmap(shuffle_row)(source_keys, local_rows)
    stored = shuffled + (jnp.arange(blocks, dtype=jnp.int32) * SEQ_DEV)[:, None]
    arriving = stored.reshape(blocks, blocks, PEER).transpose(1, 0, 2).reshape(blocks, SEQ_DEV)
    target_keys = jax.random.split(target_key, blocks)
    placed = jax.vmap(shuffle_row)(target_keys, arriving)
    return placed.reshape(SLIDE_POSITIONS).astype(jnp.int32)


def draw_w_qkv(key, part):
    query_key = jax.random.fold_in(jax.random.fold_in(key, 7), 0)
    stacked = jax.random.normal(query_key, (3, DS, DS), jnp.float32) / math.sqrt(DS)
    return jnp.clip(stacked, -1.25, 1.25).astype(jnp.bfloat16)


def shard_levels(own_key, dims, pieces, low, high):
    level, own = 1.0, jax.random.fold_in(own_key, 6)
    for position, blocks in pieces:
        steps = jnp.exp(jax.random.uniform(jax.random.fold_in(own, position), (blocks,), jnp.float32, low / len(pieces), high / len(pieces)))
        level = level * jnp.repeat(steps, dims[position] // blocks).reshape([-1 if axis == position else 1 for axis in range(len(dims))])
    return level


def centred(own_key, extent, deviation, reach, cuts=(), kind=jnp.bfloat16):
    values = jax.random.normal(own_key, extent, jnp.float32) * deviation
    if len(cuts) > 0:
        values = shard_levels(own_key, extent, cuts, -0.22, 0.18) * values
    return jnp.clip(values, min=-reach, max=reach).astype(kind)


def setup_inputs(seed: int = 0, part: int = 0) -> dict:
    key_of = jax.random.split(jax.random.key(seed), 16)
    part_splits = jax.random.split(jax.random.fold_in(key_of[15], part), 16)
    return {
        "tile_tokens": centred(part_splits[0], (NEW, PATCH, DV), 1.0, 6.0, ((0, 4),)),
        "tile_gain": jnp.clip(1.0 + 0.18 * jax.random.normal(key_of[1], (DV,), jnp.float32), 0.1, 1.9),
        "w_gate_up": centred(key_of[2], (2, DV, FF), DV ** -0.5, 0.15625, ((1, 4), (2, 4))),
        "w_down": centred(key_of[3], (FF, DV), FF ** -0.5, 0.09375, ((0, 4), (1, 4))),
        "layer_scale": jnp.clip(jnp.exp(jax.random.uniform(key_of[4], (DV,), jnp.float32, math.log(1.0), math.log(8.0))), 1.0, 8.0),
        "fc_gain": jnp.clip(1.0 + 0.18 * jax.random.normal(key_of[5], (DV,), jnp.float32), 0.1, 1.9),
        "w_embed": centred(key_of[6], (DV, DS), DV ** -0.5, 0.15625, ((1, 4),)),
        "embed_bias": centred(key_of[7], (DS,), 0.5, 3.0, ((0, 4),), jnp.float32),
        "pre_emb": centred(part_splits[8], (PRE, DS), 1.0, 6.0, ((0, 4), (1, 4))),
        "tile_order": draw_tile_order(jax.random.fold_in(jax.random.fold_in(key_of[15], part), 71), part),
        "valid_count": jax.random.randint(part_splits[10], (1,), SLIDE_POSITIONS // 4, SLIDE_POSITIONS + 1).astype(jnp.int32),
        "slide_gain": jnp.clip(1.0 + 0.18 * jax.random.normal(key_of[11], (DS,), jnp.float32), 0.1, 1.9),
        "w_qkv": draw_w_qkv(jax.random.fold_in(key_of[15], 71), part),
        "sub_gain": jnp.clip(1.0 + 0.18 * jax.random.normal(key_of[13], (DS,), jnp.float32), 0.1, 1.9),
        "w_out": centred(key_of[14], (DS, DS), DS ** -0.5, 0.21875, ((0, 4),)),
    }


layer_eps = 1e-05
masked_score = -1e+30

def normalize(values, gain):
    centered = values - lax.optimization_barrier(jnp.mean(values, axis=-1, keepdims=True))
    variance = lax.optimization_barrier(jnp.mean(centered * centered, axis=-1, keepdims=True))
    return centered * lax.rsqrt(variance + layer_eps) * gain

def dilated_level(projected_rows, valid_limit, segment, dilation):
    seg_count = SLIDE_POSITIONS // segment
    seg_width = segment // dilation
    offsets = jnp.arange(HEADS, dtype=jnp.int32) % dilation
    choose = jnp.arange(dilation, dtype=jnp.int32)[:, None] == offsets[None, :]
    arranged = projected_rows.reshape(3, seg_count, seg_width, dilation, HEADS, HEAD_DIM)
    sparse = lax.optimization_barrier(jnp.sum(jnp.where(choose[None, None, None, :, :, None], arranged, jnp.zeros((), projected_rows.dtype)), axis=3))
    starts = jnp.arange(seg_count, dtype=jnp.int32) * segment
    steps_in = jnp.arange(seg_width, dtype=jnp.int32) * dilation
    key_pos = starts[:, None, None] + steps_in[None, :, None] + offsets[None, None, :]

    def one_segment(inputs):
        query_rows, key_rows, value_rows, positions = inputs
        scores = jnp.einsum('qhe,khe->hqk', query_rows.astype(jnp.float32), key_rows.astype(jnp.float32)) / math.sqrt(HEAD_DIM)
        scores = jnp.where((positions < valid_limit).T[:, None, :], scores, masked_score)
        highest = lax.optimization_barrier(jnp.max(scores, axis=-1, keepdims=True))
        exponent = jnp.exp(scores - highest)
        mass_sum = lax.optimization_barrier(jnp.sum(exponent, axis=-1, keepdims=True))
        weights = (exponent / mass_sum).astype(jnp.bfloat16)
        attended = jnp.einsum('hqk,khe->qhe', weights.astype(jnp.float32), value_rows.astype(jnp.float32))
        return (attended, (highest[..., 0] + jnp.log(mass_sum[..., 0])).T)
    attended, log_mass = lax.map(one_segment, (sparse[0], sparse[1], sparse[2], key_pos))
    spread_out = jnp.where(choose[None, None, :, :, None], attended[:, :, None, :, :], 0.0).reshape(SLIDE_POSITIONS, HEADS, HEAD_DIM)
    spread_mass = jnp.where(choose[None, None, :, :], log_mass[:, :, None, :], masked_score).reshape(SLIDE_POSITIONS, HEADS)
    selected = jnp.broadcast_to(choose[None, None, :, :], (seg_count, seg_width, dilation, HEADS)).reshape(SLIDE_POSITIONS, HEADS)
    return (spread_out, spread_mass, selected)

def reference(tile_tokens, tile_gain, w_gate_up, w_down, layer_scale, fc_gain, w_embed, embed_bias, pre_emb, tile_order, valid_count, slide_gain, w_qkv, sub_gain, w_out):

    def tile_layer(tile_rows):
        normed = normalize(tile_rows.astype(jnp.float32), tile_gain).astype(jnp.bfloat16)
        gate_part = jnp.dot(normed, w_gate_up[0], preferred_element_type=jnp.float32)
        upward = jnp.dot(normed, w_gate_up[1], preferred_element_type=jnp.float32)
        hidden = (jax.nn.silu(gate_part) * upward).astype(jnp.bfloat16)
        mlp_out = jnp.dot(hidden, w_down, preferred_element_type=jnp.float32)
        return lax.optimization_barrier(jnp.mean(tile_rows.astype(jnp.float32) + layer_scale * mlp_out, axis=0))
    pooled = lax.map(tile_layer, tile_tokens)
    feature = normalize(pooled, fc_gain).astype(jnp.bfloat16)
    new_rows = (jnp.dot(feature, w_embed, preferred_element_type=jnp.float32) + embed_bias).astype(jnp.bfloat16)
    blocks = SLIDE_POSITIONS // SEQ_DEV
    stored = jnp.concatenate([new_rows.reshape(blocks, NEW_DEV, DS), pre_emb.reshape(blocks, PRE_DEV, DS)], axis=1).reshape(SLIDE_POSITIONS, DS)
    sequence = jnp.take(stored, tile_order, axis=0)
    slide_normed = normalize(sequence.astype(jnp.float32), slide_gain).astype(jnp.bfloat16)
    projected_rows = jnp.stack([jnp.dot(slide_normed, w_qkv[which_one], preferred_element_type=jnp.float32).astype(jnp.bfloat16) for which_one in range(3)])
    valid_limit = valid_count[0]
    level_list = ((SEGMENT_FIRST, 1), (SEGMENT_SECOND, DILATION_SECOND), (SLIDE_POSITIONS, DILATION_THIRD))
    results = [dilated_level(projected_rows, valid_limit, segment, dilation) for segment, dilation in level_list]
    outputs = jnp.stack([level_result[0] for level_result in results])
    masses = jnp.stack([level_result[1] for level_result in results])
    selects = jnp.stack([level_result[2] for level_result in results])
    ceiling = lax.optimization_barrier(jnp.max(masses, axis=0))
    shares = jnp.where(selects, jnp.exp(masses - ceiling), 0.0)
    combined = lax.optimization_barrier(jnp.sum(shares[..., None] * outputs, axis=0)) / lax.optimization_barrier(jnp.sum(shares, axis=0))[..., None]
    positions = jnp.arange(SLIDE_POSITIONS, dtype=jnp.int32)
    combined = jnp.where((positions < valid_limit)[:, None, None], combined, 0.0).reshape(SLIDE_POSITIONS, DS)
    mean_value = lax.optimization_barrier(jnp.mean(combined, axis=1, keepdims=True))
    mean_square = lax.optimization_barrier(jnp.mean(combined * combined, axis=1, keepdims=True))
    settled = ((combined - mean_value) * lax.rsqrt(mean_square - mean_value * mean_value + layer_eps) * sub_gain).astype(jnp.bfloat16)
    return sequence.astype(jnp.float32) + jnp.dot(settled, w_out, preferred_element_type=jnp.float32)
```

```python
import functools
import math

import jax
import jax.numpy as jnp
from jax import lax
from jax.experimental import pallas as pl
from jax.experimental.pallas import tpu as pltpu
from jax.sharding import PartitionSpec as P

DS = 768
HEAD_DIM = 48
SPAN0 = 1024
SPAN1 = 4096
DILATION_SECOND = 4
DILATION_THIRD = 16


layer_eps = 1e-05
masked_score = -1e30


def from_partner(value, axis, bit):
    mask = 2**bit
    pairs = [(source, source ^ mask) for source in range(lax.axis_size(axis))]
    return lax.ppermute(value, axis, pairs)


def normalize(values, gain):
    centered = values - jnp.mean(values, axis=-1, keepdims=True)
    variance = jnp.mean(centered * centered, axis=-1, keepdims=True)
    return centered * lax.rsqrt(variance + layer_eps) * gain


def select_rows(stacked, dilation, offsets):
    group_count, row_count, row_width = stacked.shape
    head_count = offsets.shape[0]
    arranged = stacked.reshape(
        group_count, row_count // dilation, dilation, head_count, row_width // head_count
    )
    choose = jnp.arange(dilation, dtype=jnp.int32)[:, None] == offsets[None, :]
    chosen = jnp.sum(
        jnp.where(choose[None, None, :, :, None], arranged, jnp.zeros((), stacked.dtype)), axis=2
    )
    return chosen.reshape(group_count, row_count // dilation, row_width)


def scatter_rows(attended, log_mass, dilation, offsets):
    query_count, head_count, head_size = attended.shape
    choose = jnp.arange(dilation, dtype=jnp.int32)[:, None] == offsets[None, :]
    spread_out = jnp.where(choose[None, :, :, None], attended[:, None, :, :], 0.0).reshape(
        query_count * dilation, head_count, head_size
    )
    spread_mass = jnp.where(choose[None, :, :], log_mass[:, None, :], masked_score).reshape(
        query_count * dilation, head_count
    )
    selected = jnp.broadcast_to(choose[None, :, :], (query_count, dilation, head_count)).reshape(
        query_count * dilation, head_count
    )
    return (spread_out, spread_mass, selected)


def attend(query_rows, key_rows, value_rows, positions, valid_limit, head_count):
    head_size = query_rows.shape[1] // head_count
    query_heads = query_rows.reshape(query_rows.shape[0], head_count, head_size)
    key_heads = key_rows.reshape(key_rows.shape[0], head_count, head_size)
    value_heads = value_rows.reshape(value_rows.shape[0], head_count, head_size)
    scores = jnp.einsum(
        "qhe,khe->hqk", query_heads, key_heads, preferred_element_type=jnp.float32
    ) / math.sqrt(head_size)
    scores = jnp.where((positions < valid_limit)[:, None, :], scores, masked_score)
    highest = jnp.max(scores, axis=-1, keepdims=True)
    exponent = jnp.exp(scores - highest)
    mass_sum = jnp.sum(exponent, axis=-1, keepdims=True)
    weights = (exponent / mass_sum).astype(jnp.bfloat16)
    attended = jnp.einsum("hqk,khe->qhe", weights, value_heads, preferred_element_type=jnp.float32)
    return (attended, (highest[..., 0] + jnp.log(mass_sum[..., 0])).T)


def general_body(
    tile_tokens,
    tile_gain,
    w_gate_up,
    w_down,
    layer_scale,
    fc_gain,
    w_embed,
    embed_bias,
    pre_emb,
    tile_order,
    valid_count,
    slide_gain,
    w_qkv,
    sub_gain,
    w_out,
):
    new_count, patch_count, tile_width = tile_tokens.shape
    token_rows = tile_tokens.reshape(new_count * patch_count, tile_width)
    normed = normalize(token_rows.astype(jnp.float32), tile_gain).astype(jnp.bfloat16)
    hidden_width = w_gate_up.shape[2]
    gate_up = jnp.einsum(
        "rk,gkf->grf",
        normed,
        lax.all_gather(w_gate_up, "seq", axis=1, tiled=True),
        preferred_element_type=jnp.float32,
    )
    hidden = (jax.nn.silu(gate_up[0]) * gate_up[1]).astype(jnp.bfloat16)
    pooled_hidden = jnp.mean(
        hidden.reshape(new_count, patch_count, hidden_width), axis=1, dtype=jnp.float32
    )
    everyone = lax.all_gather(pooled_hidden, "seq", axis=0, tiled=True)
    local_part = jnp.dot(everyone, w_down.astype(jnp.float32), precision=lax.Precision.HIGHEST)
    pooled_part = lax.all_to_all(local_part, "seq", split_axis=0, concat_axis=1, tiled=True)
    summed = lax.psum(pooled_part, "head")
    pooled = jnp.mean(tile_tokens, axis=1, dtype=jnp.float32) + layer_scale * summed
    feature = normalize(pooled, fc_gain).astype(jnp.bfloat16)
    new_rows = (jnp.dot(feature, w_embed, preferred_element_type=jnp.float32) + embed_bias).astype(
        jnp.bfloat16
    )
    stored = jnp.concatenate([new_rows, pre_emb], axis=0)
    block_rows = stored.shape[0]
    total_rows = tile_order.shape[0]
    peer_rows = block_rows // lax.axis_size("seq")
    device = lax.axis_index("seq")
    local_index = jnp.arange(block_rows, dtype=jnp.int32)
    inverse = (
        jnp.zeros((total_rows,), jnp.int32)
        .at[tile_order]
        .set(jnp.arange(total_rows, dtype=jnp.int32))
    )
    placed = lax.dynamic_slice_in_dim(inverse, device * block_rows, block_rows)
    target = placed // block_rows
    before = (target[:, None] == target[None, :]) & (placed[None, :] < placed[:, None])
    slot_index = target * peer_rows + jnp.sum(before, axis=1, dtype=jnp.int32)
    routing = (slot_index[None, :] == local_index[:, None]).astype(jnp.bfloat16)
    outgoing = jnp.dot(routing, stored, preferred_element_type=jnp.float32).astype(jnp.bfloat16)
    incoming = lax.all_to_all(outgoing, "seq", split_axis=0, concat_axis=0, tiled=True)
    wanted = lax.dynamic_slice_in_dim(tile_order, device * block_rows, block_rows)
    source = wanted // block_rows
    earlier = (source[:, None] == source[None, :]) & (local_index[None, :] < local_index[:, None])
    arrival = source * peer_rows + jnp.sum(earlier, axis=1, dtype=jnp.int32)
    own_part = jnp.take(incoming, arrival, axis=0)
    sequence = lax.all_gather(own_part, "head", axis=1, tiled=True)
    slide_normed = normalize(sequence.astype(jnp.float32), slide_gain).astype(jnp.bfloat16)
    projected_rows = jnp.einsum(
        "rd,gdc->grc", slide_normed, w_qkv, preferred_element_type=jnp.float32
    ).astype(jnp.bfloat16)
    cols_here = projected_rows.shape[2]
    head_count = cols_here // HEAD_DIM
    head_indices = lax.axis_index("head") * head_count + jnp.arange(head_count, dtype=jnp.int32)
    valid_limit = valid_count[0]
    row_index = device * block_rows + local_index
    near_devices = min(SPAN0, total_rows) // block_rows
    near_rows = projected_rows[1:]
    for bit_index in range(near_devices.bit_length() - 1):
        partner = from_partner(near_rows, "seq", bit_index)
        upper_half = device // (1 << bit_index) % 2 == 1
        near_rows = jnp.where(
            upper_half,
            jnp.concatenate([partner, near_rows], 1),
            jnp.concatenate([near_rows, partner], 1),
        )
    near_start = device // near_devices * near_devices * block_rows
    near_pos = jnp.broadcast_to(
        near_start + jnp.arange(near_rows.shape[1], dtype=jnp.int32),
        (head_count, near_rows.shape[1]),
    )
    near_out, near_mass = attend(
        projected_rows[0], near_rows[0], near_rows[1], near_pos, valid_limit, head_count
    )
    near_sel = jnp.ones((block_rows, head_count), dtype=bool)
    middle_level_offsets = head_indices % DILATION_SECOND
    middle_level = select_rows(projected_rows, DILATION_SECOND, middle_level_offsets)
    middle_devices = min(SPAN1, total_rows) // block_rows
    middle_key_value = middle_level[1:]
    every_row = lax.all_gather(middle_key_value, "seq", axis=1, tiled=True)
    group_rows = middle_devices * middle_key_value.shape[1]
    middle_key_value = lax.dynamic_slice_in_dim(
        every_row, device // middle_devices * group_rows, group_rows, 1
    )
    middle_start = device // middle_devices * middle_devices * block_rows
    middle_pos = (
        middle_start
        + middle_level_offsets[:, None]
        + DILATION_SECOND * jnp.arange(middle_key_value.shape[1], dtype=jnp.int32)[None, :]
    )
    middle_attention, middle_log_sum = attend(
        middle_level[0],
        middle_key_value[0],
        middle_key_value[1],
        middle_pos,
        valid_limit,
        head_count,
    )
    middle_output, middle_level_mass, middle_selected = scatter_rows(
        middle_attention, middle_log_sum, DILATION_SECOND, middle_level_offsets
    )
    distant_offsets = head_indices % DILATION_THIRD
    distant_local_rows = select_rows(projected_rows, DILATION_THIRD, distant_offsets)
    distant_key_value = lax.all_gather(distant_local_rows[1:], "seq", axis=1, tiled=True)
    distant_positions = (
        distant_offsets[:, None]
        + DILATION_THIRD * jnp.arange(distant_key_value.shape[1], dtype=jnp.int32)[None, :]
    )
    distant_attention, distant_log_sum = attend(
        distant_local_rows[0],
        distant_key_value[0],
        distant_key_value[1],
        distant_positions,
        valid_limit,
        head_count,
    )
    distant_output, distant_mass, distant_selected = scatter_rows(
        distant_attention, distant_log_sum, DILATION_THIRD, distant_offsets
    )
    outputs = jnp.stack([near_out, middle_output, distant_output])
    masses = jnp.stack([near_mass, middle_level_mass, distant_mass])
    selects = jnp.stack([near_sel, middle_selected, distant_selected])
    ceiling = jnp.max(masses, axis=0)
    shares = jnp.where(selects, jnp.exp(masses - ceiling), 0.0)
    combined = jnp.sum(shares[..., None] * outputs, axis=0) / jnp.sum(shares, axis=0)[..., None]
    combined = jnp.where((row_index < valid_limit)[:, None, None], combined, 0.0).reshape(
        block_rows, cols_here
    )
    row_total, row_square = lax.psum(
        (jnp.sum(combined, axis=1), jnp.sum(combined * combined, axis=1)), "head"
    )
    mean_value = row_total / DS
    mean_square = row_square / DS
    scaling = lax.rsqrt(mean_square - mean_value * mean_value + layer_eps)
    settled = ((combined - mean_value[:, None]) * scaling[:, None] * sub_gain).astype(jnp.bfloat16)
    partial_rows = jnp.dot(settled, w_out, preferred_element_type=jnp.float32)
    branch_sum = lax.psum_scatter(partial_rows, "head", scatter_dimension=1, tiled=True)
    return own_part.astype(jnp.float32) + branch_sum


MESH = pl.DeviceIdType.MESH
LANES = 128


def remote(src, dst, send_sem, recv_sem, device):
    return pltpu.make_async_remote_copy(
        src_ref=src,
        dst_ref=dst,
        send_sem=send_sem,
        recv_sem=recv_sem,
        device_id=device,
        device_id_type=MESH,
    )


def dot_rows(left, right):
    return lax.dot_general(
        left, right, (((1,), (1,)), ((), ())), preferred_element_type=jnp.float32
    )


def encode_kernel(
    tiles,
    valid_ref,
    tok_hbm,
    gain_ref,
    scale_ref,
    fc_ref,
    w_hbm,
    down_hbm,
    embed_hbm,
    pre_ref,
    wcol_ref,
    bias_ref,
    sub_ref,
    order_ref,
    slide_ref,
    qkv_hbm,
    out_ref,
    tok_ref,
    down_ref,
    embed_ref,
    qkv_ref,
    qkv_parts,
    wcol_parts,
    narrow_ref,
    pre_out,
    new_out,
    wcol_out,
    sub_out,
    seq_rows,
    projected,
    fresh_pick,
    fresh_rows,
    own_query,
    mid_out,
    mid_mass,
    far_out,
    far_mass,
    slots,
    normed,
    wall,
    acc,
    pool_mine,
    pooled,
    sums,
    means,
    parts,
    local_sem,
    send_tok,
    recv_tok,
    send_w,
    recv_w,
    send_pre,
    recv_pre,
    send_fan,
    recv_fan,
    send_aux,
    recv_aux,
    send_pool,
    recv_pool,
    send_mean,
    recv_mean,
    send_part,
    recv_part,
    send_new,
    recv_new,
    send_mix,
    recv_mix,
):
    n = lax.axis_size("seq")
    heads = lax.axis_size("head")
    z = lax.axis_index("seq")
    hd = lax.axis_index("head")
    y = lax.axis_index("groups")
    rows, width = tok_hbm.shape
    patch = rows // tiles
    depth, hidden_width = w_hbm.shape[1:]
    quarter = rows // heads
    share = hidden_width // 4
    blocks_k = depth // LANES
    blocks_c = share // LANES
    narrow = wcol_ref.shape[0]

    part = lax.rem(z, 2)
    pair = z // 2
    partner = z + 1 - 2 * part
    at_end = (z == 0) | (z == n - 1)
    inside = jnp.logical_not(at_end)
    inner = n - 1 - z
    outward = jnp.where(z < 2, 0, n - 1)
    toward = jnp.where(z < 2, 1, n - 1)
    across = lax.rem(hd + 2, heads)
    mate = hd + 1 - 2 * lax.rem(hd, 2)
    beyond = lax.rem(mate + 2, heads)

    def seq_peer(k):
        return lax.rem(z + k, n)

    def ahead(k):
        return lax.rem(z + k * toward, n)

    def head_peer(k):
        return lax.rem(hd + k, heads)

    def head_source(k):
        return lax.rem(hd + heads - k, heads)

    def quarter_rows(index):
        return pl.ds(pl.multiple_of(index * quarter, quarter), quarter)

    def unit(u):
        return u // blocks_c, u % blocks_c

    def weight_block(owner, u):
        r, c = unit(u)
        place = (lax.rem(owner, 2) * 2 + y) * share + c * LANES
        return w_hbm.at[
            :, pl.ds(r * LANES, LANES), pl.ds(pl.multiple_of(place, LANES), LANES)
        ]

    def wall_block(source, u):
        r, c = unit(u)
        return wall.at[r, c, :, pl.ds(pl.multiple_of(source * LANES, LANES), LANES), :]

    units = blocks_k * blocks_c
    half = quarter // 2
    first_quarters = (hd, across, mate, beyond)
    token_loads = [
        pltpu.make_async_copy(
            tok_hbm.at[quarter_rows(q)], tok_ref.at[quarter_rows(q)], local_sem.at[i]
        )
        for i, q in enumerate(first_quarters)
    ]
    loads = [
        pltpu.make_async_copy(source, target, local_sem.at[4 + i])
        for i, (source, target) in enumerate(
            ((qkv_hbm, qkv_ref), (down_hbm, down_ref), (embed_hbm, embed_ref))
        )
    ]
    weight_loads = [
        pltpu.make_async_copy(weight_block(z, u), wall_block(z, u), local_sem.at[7])
        for u in range(units)
    ]
    barrier = pltpu.get_barrier_semaphore()
    count = 0
    for k in range(n):
        for j in range(heads):
            if k or j:
                pl.semaphore_signal(
                    barrier,
                    inc=1,
                    device_id={"seq": seq_peer(k), "head": head_peer(j)},
                    device_id_type=MESH,
                )
                count += 1
    for k in range(n):
        pl.semaphore_signal(
            barrier, inc=1, device_id={"groups": 1 - y, "seq": seq_peer(k)}, device_id_type=MESH
        )
        count += 1
    for load in token_loads + loads + weight_loads:
        load.start()

    block = 64

    def norm_quarter(position):
        index = first_quarters[position]
        token_loads[position].wait()

        def norm_rows(i, total):
            at = pl.ds(pl.multiple_of(index * quarter + i * block, block), block)
            values = tok_ref[at, :].astype(jnp.float32)
            out = normalize(values, gain_ref[...].reshape(1, width)).astype(jnp.bfloat16)
            normed[y * 2 + part, index, pl.ds(pl.multiple_of(i * block, block), block), :] = out
            return total + jnp.sum(values, axis=0, keepdims=True)

        sums[index] = lax.fori_loop(
            0, quarter // block, norm_rows, jnp.zeros((1, width), jnp.float32)
        )

    norm_quarter(0)
    pl.semaphore_wait(barrier, count)

    def send(source, target, sends, receives, device):
        remote(source, target, sends, receives, device).start()

    def send_weight(k, u):
        target = ahead(k)
        send(
            weight_block(target, u), wall_block(z, u), send_w.at[0], recv_w.at[u], {"seq": target}
        )

    own_set = y * 2 + part
    z_set = y * 2 + 1 - part
    y_set = (1 - y) * 2 + part
    d_set = (1 - y) * 2 + 1 - part

    def token_copy(which, index, event, part_of, device):
        slot = normed.at[which, index, pl.ds(part_of * half, half)]
        return remote(slot, slot, send_tok.at[0], recv_tok.at[event, part_of], device)

    def fan_copy(block_index, share_index, event, device):
        slot = pre_out.at[block_index, share_index]
        return remote(slot, slot, send_fan.at[0], recv_fan.at[event, block_index], device)

    for index in range(2):
        target = jnp.where(
            at_end,
            jnp.where(z == 0, 1 + index, n - 2 - index),
            outward if index == 0 else inner,
        )
        send(pre_ref, pre_out.at[z, hd], send_pre.at[0], recv_pre.at[z], {"seq": target})
    token_copy(own_set, hd, 0, 0, {"seq": partner}).start()
    for part_of in range(2):
        token_copy(own_set, hd, 4, part_of, {"groups": 1 - y}).start()

    @pl.when(at_end)
    def _():
        token_copy(own_set, hd, 0, 1, {"seq": partner}).start()

    @pl.when(at_end)
    def _():
        for u in range(units):
            send_weight(2, u)
        for u in range(units):
            send_weight(1, u)
            send_weight(3, u)

    @pl.when(inside)
    def _():
        for u in range(units):
            send_weight(1, u)

    pre_out[z, hd] = pre_ref[...]
    norm_quarter(1)

    def fan_first(b):
        fan_copy(b, hd, 0, {"head": across}).start()
        fan_copy(b, hd, 1, {"head": mate}).start()

    def fan_second(b):
        fan_copy(b, across, 0, {"head": across}).wait_recv()
        fan_copy(b, across, 2, {"head": mate}).start()

    def stored_block(b, forward=False):
        slot = pre_out.at[b, hd]
        remote(slot, slot, send_pre.at[0], recv_pre.at[b], {"seq": partner}).wait_recv()
        if forward:
            send(slot, slot, send_pre.at[1], recv_pre.at[b], {"seq": outward})
        fan_first(b)

    fan_first(z)
    second_end = jnp.where(z == 0, 2, n - 3)

    @pl.when(at_end)
    def _():
        stored_block(partner)

    @pl.when(inside)
    def _():
        stored_block(inner, True)
        token_copy(own_set, hd, 0, 1, {"seq": partner}).start()
        stored_block(outward)

    norm_quarter(2)
    norm_quarter(3)
    for tile in range(tiles):
        per = heads // tiles
        means[z, pl.ds(tile, 1), :] = (
            sum(sums[tile * per + i] for i in range(per)) / patch
        )
    for k in range(1, n):
        send(means.at[z], means.at[z], send_mean.at[0], recv_mean.at[0], {"seq": seq_peer(k)})
    narrow_ref[pl.ds(0, 1), :] = bias_ref[...].reshape(1, narrow)
    narrow_ref[pl.ds(1, 1), :] = sub_ref[...].reshape(1, narrow)
    for j in range(heads):
        wcol_parts[j] = wcol_ref[:, j * narrow : (j + 1) * narrow]
    wcol_out[hd] = wcol_parts[hd]
    sub_out[hd] = narrow_ref[...]

    def token_event(which, index, event, part_of, forwards):
        token_copy(which, index, event, part_of, {"head": mate}).wait_recv()
        for to, device in forwards:
            token_copy(which, index, to, part_of, device).start()

    from_z = ((8, {"groups": 1 - y}), (1, {"head": across}), (2, {"head": mate}))
    token_event(y_set, hd, 4, 0, ((6, {"head": mate}),))
    fan_second(z)

    @pl.when(inside)
    def _():
        stored_block(n - 1 - outward, True)
        for u in range(units):
            send_weight(3, u)

    token_event(z_set, hd, 0, 0, from_z)
    token_event(y_set, hd, 4, 1, ((6, {"head": mate}),))

    @pl.when(at_end)
    def _():
        fan_second(partner)
        stored_block(second_end)

    @pl.when(inside)
    def _():
        fan_second(inner)
        fan_second(outward)

    token_event(z_set, hd, 0, 1, from_z)
    for part_of in range(2):
        token_copy(own_set, across, 5, part_of, {"groups": 1 - y}).start()

    @pl.when(at_end)
    def _():
        stored_block(n - 1 - z)
        fan_second(second_end)
        fan_second(n - 1 - z)

    @pl.when(inside)
    def _():
        fan_second(n - 1 - outward)

    for k in range(1, heads):
        send(
            wcol_parts.at[head_peer(k)],
            wcol_out.at[hd],
            send_aux.at[0],
            recv_aux.at[0],
            {"head": head_peer(k)},
        )
        send(narrow_ref, sub_out.at[hd], send_aux.at[1], recv_aux.at[1], {"head": head_peer(k)})

    total_rows = order_ref.shape[0]
    cols, stored_rows = pre_ref.shape
    classes = DILATION_THIRD
    class_rows = total_rows // classes
    own_rows = stored_rows // classes

    def row_norm(pieces):
        features = heads * cols
        mean = sum(jnp.sum(p, axis=1, keepdims=True) for p in pieces) / features
        centered = [p - mean for p in pieces]
        variance = sum(jnp.sum(p * p, axis=1, keepdims=True) for p in centered) / features
        scaling = lax.rsqrt(variance + layer_eps)
        return [
            (
                p * scaling * slide_ref[...].reshape(1, features)[:, j * cols : (j + 1) * cols]
            ).astype(jnp.bfloat16)
            for j, p in enumerate(centered)
        ]

    def project(pieces, g):
        return sum(dot_rows(piece, qkv_parts[g, j]) for j, piece in enumerate(pieces))

    step = stored_rows

    def sequence_step(t):
        at = pl.ds(t * step, step)
        order = order_ref[at, :]
        lane = lax.broadcasted_iota(jnp.int32, (step, LANES), 1)
        wanted = jnp.where(lane < n * tiles, lane // tiles * stored_rows + lane % tiles, -1)
        fresh_pick[at, :] = jnp.where(order == wanted, 1.0, 0.0).astype(jnp.bfloat16)
        index = lax.broadcasted_iota(jnp.int32, (step, stored_rows), 1)
        picks = [
            jnp.where(order == index + b * stored_rows, 1.0, 0.0).astype(jnp.bfloat16)
            for b in range(n)
        ]
        pieces = []
        for j in range(heads):
            piece = sum(dot_rows(picks[b], pre_out[b, j]) for b in range(n))
            seq_rows[j, at, :] = piece.astype(jnp.bfloat16)
            pieces.append(piece)
        normal = row_norm(pieces)
        for g in range(3):
            projected[g, at, :] = project(normal, g).astype(jnp.bfloat16)

    loads[0].wait()
    for g in range(3):
        for j in range(heads):
            qkv_parts[g, j] = qkv_ref[g, :, j * cols : (j + 1) * cols]
    for b in range(n):
        for event, source in ((1, mate), (2, beyond)):
            fan_copy(b, source, event, {"head": mate}).wait_recv()
    relays = (
        (z_set, across, 1, ((3, {"head": mate}),)),
        (d_set, hd, 8, ((9, {"head": across}), (10, {"head": mate}))),
        (y_set, across, 5, ((7, {"head": mate}),)),
        (d_set, across, 9, ((11, {"head": mate}),)),
    )
    for t in range(total_rows // step):
        sequence_step(t)
        if t == 0:

            @pl.when(inside)
            def _():
                for u in range(units):
                    send_weight(2, u)

        for which, index, event, forwards in relays[t : t + 1]:
            for part_of in range(2):
                token_event(which, index, event, part_of, forwards)
    for which, index, event, forwards in relays[total_rows // step :]:
        for part_of in range(2):
            token_event(which, index, event, part_of, forwards)
    for which, first in ((z_set, 0), (y_set, 4), (d_set, 8)):
        for part_of in range(2):
            token_event(which, mate, first + 2, part_of, ())
            token_event(which, beyond, first + 3, part_of, ())

    whole = wall.at[:, :, :, pl.ds(0, LANES), :]
    pltpu.make_async_copy(whole, whole, local_sem.at[7]).wait()

    def multiply(u):
        r, c = unit(u)
        others = wall.at[r, c, :, pl.ds(0, (n - 1) * LANES), :]
        remote(others, others, send_w.at[0], recv_w.at[u], {"seq": partner}).wait_recv()

        @pl.loop(0, 4)
        def _(s):
            w = jnp.concatenate([wall[r, c, 0], wall[r, c, 1]], axis=1)
            x = jnp.concatenate(
                [
                    normed[s, :, :, b * depth + r * LANES : b * depth + (r + 1) * LANES].reshape(
                        rows, LANES
                    )
                    for b in range(n)
                ],
                axis=1,
            )
            value = jnp.dot(x, w, preferred_element_type=jnp.float32)
            if r == 0:
                acc[c, s] = value
            else:
                acc[c, s] += value

    def pool(c):
        for s in range(4):
            for tile in range(tiles):
                at = pl.ds(tile * patch, patch)
                gate = acc[c, s, at, :LANES]
                hidden = (gate / (1.0 + jnp.exp(-gate)) * acc[c, s, at, LANES:]).astype(
                    jnp.bfloat16
                )
                pool_mine[s // 2, c, pl.ds((s % 2) * tiles + tile, 1), :] = (
                    jnp.sum(hidden.astype(jnp.float32), axis=0, keepdims=True) / patch
                )
        place = y * n + z
        pooled[place, c] = pool_mine[y, c]
        for k in range(n):
            for other in range(2):
                if k or other:
                    yy = 1 - y if other else y
                    send(
                        pool_mine.at[yy, c],
                        pooled.at[place, c],
                        send_pool.at[c],
                        recv_pool.at[c],
                        {"groups": yy, "seq": seq_peer(k)},
                    )

    for u in range(units):
        multiply(u)
        r, c = unit(u)
        if r == blocks_k - 1:
            pool(c)

    seen = means.at[pl.ds(0, n - 1)]
    remote(seen, seen, send_mean.at[0], recv_mean.at[0], {"seq": partner}).wait_recv()
    for c in range(blocks_c):
        slot = pooled.at[pl.ds(0, 2 * n - 1), c]
        remote(slot, slot, send_pool.at[c], recv_pool.at[c], {"seq": partner}).wait_recv()
    loads[1].wait()
    loads[2].wait()
    everyone = jnp.concatenate(
        [
            jnp.concatenate(
                [
                    pooled[yy * n + b + m, c]
                    for m in range(2)
                    for yy in range(2)
                    for c in range(blocks_c)
                ],
                axis=1,
            )
            for b in range(0, n, 2)
        ],
        axis=0,
    )
    high = everyone.astype(jnp.bfloat16)
    rest = everyone - high.astype(jnp.float32)
    middle = rest.astype(jnp.bfloat16)
    low = (rest - middle.astype(jnp.float32)).astype(jnp.bfloat16)
    local_part = jnp.zeros((n * tiles, down_ref.shape[1]), jnp.float32)
    for piece in (low, middle, high):
        local_part += jnp.dot(piece, down_ref[...], preferred_element_type=jnp.float32)
    here = z * heads + hd
    parts[here] = local_part
    for k in range(n):
        for j in range(heads):
            if k or j:
                send(
                    parts.at[here],
                    parts.at[here],
                    send_part.at[0],
                    recv_part.at[0],
                    {"seq": seq_peer(k), "head": head_peer(j)},
                )
    slot = parts.at[pl.ds(0, n * heads - 1)]
    remote(slot, slot, send_part.at[0], recv_part.at[0], {"seq": partner}).wait_recv()
    summed = jnp.concatenate(
        [sum(parts[b * heads + j] for j in range(heads)) for b in range(n)], axis=1
    )
    average = jnp.concatenate([means[b] for b in range(n)], axis=0)
    feature = normalize(
        average + scale_ref[...].reshape(1, width) * summed, fc_ref[...].reshape(1, width)
    ).astype(jnp.bfloat16)
    fresh = dot_rows(feature, embed_ref[...]) + narrow_ref[pl.ds(0, 1), :]
    new_out[hd] = fresh
    for k in range(1, heads):
        send(new_out.at[hd], new_out.at[hd], send_new.at[0], recv_new.at[0], {"head": head_peer(k)})
    for buffer, receives in (
        (new_out, recv_new.at[0]),
        (wcol_out, recv_aux.at[0]),
        (sub_out, recv_aux.at[1]),
    ):
        slot = buffer.at[pl.ds(0, heads - 1)]
        remote(slot, slot, send_new.at[0], receives, {"head": mate}).wait_recv()

    pieces = [new_out[j].astype(jnp.bfloat16).astype(jnp.float32) for j in range(heads)]
    normal = row_norm(pieces)
    fresh_rows[...] = jnp.zeros(fresh_rows.shape, jnp.float32)
    filled = pl.ds(0, n * tiles)
    for g in range(3):
        fresh_rows[g, filled, :] = project(normal, g)
    fresh_rows[3, filled, :] = new_out[hd]
    own_at = pl.ds(pl.multiple_of(z * own_rows, own_rows), own_rows)
    updated = []
    for g in range(3):
        placed = jnp.dot(
            fresh_pick[...],
            fresh_rows[g].astype(jnp.bfloat16),
            preferred_element_type=jnp.float32,
        )
        projected[g] = (projected[g].astype(jnp.float32) + placed).astype(jnp.bfloat16)
    seq_rows[hd] = (
        seq_rows[hd].astype(jnp.float32)
        + jnp.dot(
            fresh_pick[...],
            fresh_rows[3].astype(jnp.bfloat16),
            preferred_element_type=jnp.float32,
        )
    ).astype(jnp.bfloat16)

    def class_part(buffer, lead, c):
        return buffer[lead, pl.ds(pl.multiple_of(c * class_rows, class_rows), class_rows), :]

    for c in range(classes):
        at = pl.ds(
            pl.multiple_of(c * class_rows + z * own_rows, own_rows), own_rows
        )
        own_query[c] = projected[0, at, :]
        out_ref[pl.ds(c * own_rows, own_rows), :] = seq_rows[hd, at, :].astype(jnp.float32)

    limit = valid_ref[0]
    head_count = cols // HEAD_DIM
    lane_head = lax.broadcasted_iota(jnp.int32, (1, cols), 1) // HEAD_DIM
    factor = 1.0 / math.sqrt(HEAD_DIM)

    def weigh(queries, keys, values, positions):
        scores = (
            lax.dot_general(
                queries, keys, (((1,), (1,)), ((), ())), preferred_element_type=jnp.float32
            )
            * factor
        )
        scores = jnp.where(positions < limit, scores, masked_score)
        peak = jnp.max(scores, axis=1, keepdims=True)
        exponent = jnp.exp(scores - peak)
        mass = jnp.sum(exponent, axis=1, keepdims=True)
        weights = (exponent * (1.0 / mass)).astype(jnp.bfloat16)
        return (
            jnp.dot(weights, values, preferred_element_type=jnp.float32),
            peak + jnp.log(mass),
        )

    block_size = classes * own_rows
    row_index = lax.broadcasted_iota(jnp.int32, (block_size, 1), 0)
    row_class = row_index // own_rows
    row_position = z * block_size + row_index % own_rows * classes + row_class
    near_lane = lax.broadcasted_iota(jnp.int32, (1, total_rows), 1)
    near_position = near_lane % class_rows * classes + near_lane // class_rows
    repeat = classes // DILATION_SECOND
    mid_lane = lax.broadcasted_iota(jnp.int32, (1, repeat * class_rows), 1)
    far_lane = lax.broadcasted_iota(jnp.int32, (1, class_rows), 1)
    mid_out[...] = jnp.zeros(mid_out.shape, jnp.float32)
    mid_mass[...] = jnp.zeros(mid_mass.shape, jnp.float32)
    far_out[...] = jnp.zeros(far_out.shape, jnp.float32)
    far_mass[...] = jnp.zeros(far_mass.shape, jnp.float32)
    all_queries = own_query[...].reshape(block_size, cols)
    nothing = jnp.zeros((), jnp.bfloat16)
    combined = jnp.zeros((block_size, cols), jnp.float32)
    for j in range(head_count):
        here = lane_head == j
        mid_offset = lax.rem(hd * head_count + j, DILATION_SECOND)
        far_offset = lax.rem(hd * head_count + j, DILATION_THIRD)
        near, near_log = weigh(
            jnp.where(here, all_queries, nothing), projected[1], projected[2], near_position
        )
        mids = [mid_offset + DILATION_SECOND * t for t in range(repeat)]
        mid, mid_log = weigh(
            jnp.where(here, jnp.concatenate([own_query[c] for c in mids], axis=0), nothing),
            jnp.concatenate([class_part(projected, 1, c) for c in mids], axis=0),
            jnp.concatenate([class_part(projected, 2, c) for c in mids], axis=0),
            mid_lane % class_rows * classes
            + mid_lane // class_rows * DILATION_SECOND
            + mid_offset,
        )
        far, far_log = weigh(
            jnp.where(here, own_query[far_offset], nothing),
            class_part(projected, 1, far_offset),
            class_part(projected, 2, far_offset),
            far_lane * classes + far_offset,
        )
        for t, c in enumerate(mids):
            mid_out[j, c] = mid[t * own_rows : (t + 1) * own_rows]
            mid_mass[j, c] = jnp.broadcast_to(
                mid_log[t * own_rows : (t + 1) * own_rows], (own_rows, 128)
            )
        far_out[j, far_offset] = far
        far_mass[j, far_offset] = jnp.broadcast_to(far_log, (own_rows, 128))
        mid_log = mid_mass[j].reshape(block_size, 128)[:, :1]
        far_log = far_mass[j].reshape(block_size, 128)[:, :1]
        mid_used = row_class % DILATION_SECOND == mid_offset
        far_used = row_class == far_offset
        ceiling = jnp.maximum(near_log, jnp.where(mid_used, mid_log, near_log))
        ceiling = jnp.maximum(ceiling, jnp.where(far_used, far_log, near_log))
        near_share = jnp.exp(near_log - ceiling)
        mid_share = jnp.where(mid_used, jnp.exp(mid_log - ceiling), 0.0)
        far_share = jnp.where(far_used, jnp.exp(far_log - ceiling), 0.0)
        mixture = (
            near_share * near
            + mid_share * mid_out[j].reshape(block_size, cols)
            + far_share * far_out[j].reshape(block_size, cols)
        ) / (near_share + mid_share + far_share)
        combined = jnp.where(here, mixture, combined)
    combined = jnp.where(row_position < limit, combined, 0.0)

    slots[hd] = combined.astype(jnp.bfloat16)
    for k in range(1, heads):
        send(slots.at[hd], slots.at[hd], send_mix.at[0], recv_mix.at[0], {"head": head_peer(k)})
    slot = slots.at[pl.ds(0, heads - 1)]
    remote(slot, slot, send_mix.at[0], recv_mix.at[0], {"head": mate}).wait_recv()
    pieces = [slots[j].astype(jnp.float32) for j in range(heads)]
    features = heads * cols
    mean = sum(jnp.sum(p, axis=1, keepdims=True) for p in pieces) / features
    square = sum(jnp.sum(p * p, axis=1, keepdims=True) for p in pieces) / features
    scaling = lax.rsqrt(square - mean * mean + layer_eps)
    branch = jnp.zeros(out_ref.shape, jnp.float32)
    for j in range(heads):
        gain = sub_out[j][1:2]
        settled = ((pieces[j] - mean) * scaling * gain).astype(jnp.bfloat16)
        branch += jnp.dot(settled, wcol_out[j], preferred_element_type=jnp.float32)
    out_ref[...] += branch

    def drain(slot, sends):
        remote(slot, slot, sends, recv_new.at[0], {"head": mate}).wait_send()

    drain(normed.at[pl.ds(0, 3)], send_tok.at[0])
    drain(wall.at[:, :, :, pl.ds(0, (n - 1) * LANES), :], send_w.at[0])
    drain(pre_out.at[0, pl.ds(0, 2)], send_pre.at[0])

    @pl.when(inside)
    def _():
        drain(pre_out.at[0, pl.ds(0, 2)], send_pre.at[1])

    drain(pre_out.at[pl.ds(0, 3)], send_fan.at[0])
    drain(wcol_out.at[pl.ds(0, heads - 1)], send_aux.at[0])
    drain(sub_out.at[pl.ds(0, heads - 1)], send_aux.at[1])
    for c in range(blocks_c):
        drain(pooled.at[pl.ds(0, 2 * n - 1), c], send_pool.at[c])
    drain(means.at[pl.ds(0, n - 1)], send_mean.at[0])
    drain(parts.at[pl.ds(0, n * heads - 1)], send_part.at[0])
    drain(new_out.at[pl.ds(0, heads - 1)], send_new.at[0])
    drain(slots.at[pl.ds(0, heads - 1)], send_mix.at[0])


def near_body(
    tile_tokens,
    tile_gain,
    w_gate_up,
    w_down,
    layer_scale,
    fc_gain,
    w_embed,
    embed_bias,
    pre_emb,
    tile_order,
    valid_count,
    slide_gain,
    w_qkv,
    sub_gain,
    w_out,
):
    n = lax.axis_size("seq")
    heads = lax.axis_size("head")
    tiles, patch, width = tile_tokens.shape
    depth, hidden_width = w_gate_up.shape[1:]
    rows = tiles * patch
    cols = w_embed.shape[1]
    head_count = cols // HEAD_DIM
    total_rows = tile_order.shape[0]
    block_rows = total_rows // n
    classes = DILATION_THIRD
    own_rows = block_rows // classes
    by_class = tile_order.reshape(total_rows // classes, classes).T.reshape(total_rows, 1)
    vmem = pl.BlockSpec(memory_space=pltpu.VMEM)
    anywhere = pl.BlockSpec(memory_space=pl.ANY)
    dma = pltpu.SemaphoreType.DMA
    f32, bf16 = jnp.float32, jnp.bfloat16
    quarter = rows // heads
    blocks_k = depth // LANES
    blocks_c = hidden_width // 4 // LANES
    out = pl.pallas_call(
        functools.partial(encode_kernel, tiles),
        out_shape=jax.ShapeDtypeStruct((block_rows, cols), f32),
        in_specs=[
            pl.BlockSpec(memory_space=pltpu.SMEM),
            anywhere,
            vmem,
            vmem,
            vmem,
            anywhere,
            anywhere,
            anywhere,
            vmem,
            vmem,
            vmem,
            vmem,
            vmem,
            vmem,
            anywhere,
        ],
        out_specs=vmem,
        scratch_shapes=[
            pltpu.VMEM((rows, width), bf16),
            pltpu.VMEM(w_down.shape, bf16),
            pltpu.VMEM((cols, width), bf16),
            pltpu.VMEM((3, cols, heads * cols), bf16),
            pltpu.VMEM((3, heads, cols, cols), bf16),
            pltpu.VMEM((heads, cols, cols), bf16),
            pltpu.VMEM((2, cols), f32),
            pltpu.VMEM((n, heads, cols, block_rows), bf16),
            pltpu.VMEM((heads, n * tiles, cols), f32),
            pltpu.VMEM((heads, cols, cols), bf16),
            pltpu.VMEM((heads, 2, cols), f32),
            pltpu.VMEM((heads, total_rows, cols), bf16),
            pltpu.VMEM((3, total_rows, cols), bf16),
            pltpu.VMEM((total_rows, LANES), bf16),
            pltpu.VMEM((4, LANES, cols), f32),
            pltpu.VMEM((classes, own_rows, cols), bf16),
            pltpu.VMEM((head_count, classes, own_rows, cols), f32),
            pltpu.VMEM((head_count, classes, own_rows, LANES), f32),
            pltpu.VMEM((head_count, classes, own_rows, cols), f32),
            pltpu.VMEM((head_count, classes, own_rows, LANES), f32),
            pltpu.VMEM((heads, block_rows, cols), bf16),
            pltpu.VMEM((4, heads, quarter, width), bf16),
            pltpu.VMEM((blocks_k, blocks_c, 2, n * LANES, LANES), bf16),
            pltpu.VMEM((blocks_c, 4, rows, 2 * LANES), f32),
            pltpu.VMEM((2, blocks_c, 2 * tiles, LANES), f32),
            pltpu.VMEM((2 * n, blocks_c, 2 * tiles, LANES), f32),
            pltpu.VMEM((heads, 1, width), f32),
            pltpu.VMEM((n, tiles, width), f32),
            pltpu.VMEM((n * heads, n * tiles, w_down.shape[1]), f32),
            dma((8,)),
            dma((1,)),
            dma((12, 2)),
            dma((1,)),
            dma((blocks_k * blocks_c,)),
            dma((2,)),
            dma((n,)),
            dma((1,)),
            dma((3, n)),
            dma((2,)),
            dma((2,)),
            dma((blocks_c,)),
            dma((blocks_c,)),
            dma((1,)),
            dma((1,)),
            dma((1,)),
            dma((1,)),
            dma((1,)),
            dma((1,)),
            dma((1,)),
            dma((1,)),
        ],
        compiler_params=pltpu.CompilerParams(
            collective_id=0, has_side_effects=True, vmem_limit_bytes=58 * 1024 * 1024
        ),
    )(
        valid_count,
        tile_tokens.reshape(rows, width),
        tile_gain,
        layer_scale,
        fc_gain,
        w_gate_up,
        w_down,
        w_embed.T,
        jnp.pad(pre_emb.T, ((0, 0), (tiles, 0))),
        w_out,
        embed_bias,
        sub_gain,
        by_class,
        slide_gain,
        w_qkv.swapaxes(1, 2),
    )
    return out.reshape(classes, own_rows, cols).transpose(1, 0, 2).reshape(block_rows, cols)


def body(*args):
    total_rows = args[9].shape[0]
    mesh_fits = all(lax.axis_size(a) == k for a, k in (("groups", 2), ("seq", 4), ("head", 4)))
    if total_rows <= SPAN0 and mesh_fits:
        return near_body(*args)
    return general_body(*args)


def solution(mesh):
    placed = (
        P(("groups", "seq"), None, None),
        P(),
        P(None, "seq", "head"),
        P("head", "seq"),
        P(),
        P(),
        P(None, "head"),
        P("head"),
        P(("groups", "seq"), "head"),
        P("groups"),
        P("groups"),
        P(),
        P(None, None, "head"),
        P("head"),
        P("head", None),
    )
    return jax.shard_map(
        body, mesh=mesh, in_specs=placed, out_specs=P(("groups", "seq"), "head"), check_vma=False
    )
```

```python
import functools
import math

import jax
import jax.numpy as jnp
from jax import lax
from jax.experimental import pallas as pl
from jax.experimental.pallas import tpu as pltpu
from jax.sharding import PartitionSpec as P

DS = 768
HEAD_DIM = 48
SPAN0 = 1024
SPAN1 = 4096
DILATION_SECOND = 4
DILATION_THIRD = 16


layer_eps = 1e-05
masked_score = -1e30


def from_partner(value, axis, bit):
    mask = 2**bit
    pairs = [(source, source ^ mask) for source in range(lax.axis_size(axis))]
    return lax.ppermute(value, axis, pairs)


def normalize(values, gain):
    centered = values - jnp.mean(values, axis=-1, keepdims=True)
    variance = jnp.mean(centered * centered, axis=-1, keepdims=True)
    return centered * lax.rsqrt(variance + layer_eps) * gain


def select_rows(stacked, dilation, offsets):
    group_count, row_count, row_width = stacked.shape
    head_count = offsets.shape[0]
    arranged = stacked.reshape(
        group_count, row_count // dilation, dilation, head_count, row_width // head_count
    )
    choose = jnp.arange(dilation, dtype=jnp.int32)[:, None] == offsets[None, :]
    chosen = jnp.sum(
        jnp.where(choose[None, None, :, :, None], arranged, jnp.zeros((), stacked.dtype)), axis=2
    )
    return chosen.reshape(group_count, row_count // dilation, row_width)


def scatter_rows(attended, log_mass, dilation, offsets):
    query_count, head_count, head_size = attended.shape
    choose = jnp.arange(dilation, dtype=jnp.int32)[:, None] == offsets[None, :]
    spread_out = jnp.where(choose[None, :, :, None], attended[:, None, :, :], 0.0).reshape(
        query_count * dilation, head_count, head_size
    )
    spread_mass = jnp.where(choose[None, :, :], log_mass[:, None, :], masked_score).reshape(
        query_count * dilation, head_count
    )
    selected = jnp.broadcast_to(choose[None, :, :], (query_count, dilation, head_count)).reshape(
        query_count * dilation, head_count
    )
    return (spread_out, spread_mass, selected)


def attend(query_rows, key_rows, value_rows, positions, valid_limit, head_count):
    head_size = query_rows.shape[1] // head_count
    query_heads = query_rows.reshape(query_rows.shape[0], head_count, head_size)
    key_heads = key_rows.reshape(key_rows.shape[0], head_count, head_size)
    value_heads = value_rows.reshape(value_rows.shape[0], head_count, head_size)
    scores = jnp.einsum(
        "qhe,khe->hqk", query_heads, key_heads, preferred_element_type=jnp.float32
    ) / math.sqrt(head_size)
    scores = jnp.where((positions < valid_limit)[:, None, :], scores, masked_score)
    highest = jnp.max(scores, axis=-1, keepdims=True)
    exponent = jnp.exp(scores - highest)
    mass_sum = jnp.sum(exponent, axis=-1, keepdims=True)
    weights = (exponent / mass_sum).astype(jnp.bfloat16)
    attended = jnp.einsum("hqk,khe->qhe", weights, value_heads, preferred_element_type=jnp.float32)
    return (attended, (highest[..., 0] + jnp.log(mass_sum[..., 0])).T)


def general_body(
    tile_tokens,
    tile_gain,
    w_gate_up,
    w_down,
    layer_scale,
    fc_gain,
    w_embed,
    embed_bias,
    pre_emb,
    tile_order,
    valid_count,
    slide_gain,
    w_qkv,
    sub_gain,
    w_out,
):
    new_count, patch_count, tile_width = tile_tokens.shape
    token_rows = tile_tokens.reshape(new_count * patch_count, tile_width)
    normed = normalize(token_rows.astype(jnp.float32), tile_gain).astype(jnp.bfloat16)
    hidden_width = w_gate_up.shape[2]
    gate_up = jnp.einsum(
        "rk,gkf->grf",
        normed,
        lax.all_gather(w_gate_up, "seq", axis=1, tiled=True),
        preferred_element_type=jnp.float32,
    )
    hidden = (jax.nn.silu(gate_up[0]) * gate_up[1]).astype(jnp.bfloat16)
    pooled_hidden = jnp.mean(
        hidden.reshape(new_count, patch_count, hidden_width), axis=1, dtype=jnp.float32
    )
    everyone = lax.all_gather(pooled_hidden, "seq", axis=0, tiled=True)
    local_part = jnp.dot(everyone, w_down.astype(jnp.float32), precision=lax.Precision.HIGHEST)
    pooled_part = lax.all_to_all(local_part, "seq", split_axis=0, concat_axis=1, tiled=True)
    summed = lax.psum(pooled_part, "head")
    pooled = jnp.mean(tile_tokens, axis=1, dtype=jnp.float32) + layer_scale * summed
    feature = normalize(pooled, fc_gain).astype(jnp.bfloat16)
    new_rows = (jnp.dot(feature, w_embed, preferred_element_type=jnp.float32) + embed_bias).astype(
        jnp.bfloat16
    )
    stored = jnp.concatenate([new_rows, pre_emb], axis=0)
    block_rows = stored.shape[0]
    total_rows = tile_order.shape[0]
    peer_rows = block_rows // lax.axis_size("seq")
    device = lax.axis_index("seq")
    local_index = jnp.arange(block_rows, dtype=jnp.int32)
    inverse = (
        jnp.zeros((total_rows,), jnp.int32)
        .at[tile_order]
        .set(jnp.arange(total_rows, dtype=jnp.int32))
    )
    placed = lax.dynamic_slice_in_dim(inverse, device * block_rows, block_rows)
    target = placed // block_rows
    before = (target[:, None] == target[None, :]) & (placed[None, :] < placed[:, None])
    slot_index = target * peer_rows + jnp.sum(before, axis=1, dtype=jnp.int32)
    routing = (slot_index[None, :] == local_index[:, None]).astype(jnp.bfloat16)
    outgoing = jnp.dot(routing, stored, preferred_element_type=jnp.float32).astype(jnp.bfloat16)
    incoming = lax.all_to_all(outgoing, "seq", split_axis=0, concat_axis=0, tiled=True)
    wanted = lax.dynamic_slice_in_dim(tile_order, device * block_rows, block_rows)
    source = wanted // block_rows
    earlier = (source[:, None] == source[None, :]) & (local_index[None, :] < local_index[:, None])
    arrival = source * peer_rows + jnp.sum(earlier, axis=1, dtype=jnp.int32)
    own_part = jnp.take(incoming, arrival, axis=0)
    sequence = lax.all_gather(own_part, "head", axis=1, tiled=True)
    slide_normed = normalize(sequence.astype(jnp.float32), slide_gain).astype(jnp.bfloat16)
    projected_rows = jnp.einsum(
        "rd,gdc->grc", slide_normed, w_qkv, preferred_element_type=jnp.float32
    ).astype(jnp.bfloat16)
    cols_here = projected_rows.shape[2]
    head_count = cols_here // HEAD_DIM
    head_indices = lax.axis_index("head") * head_count + jnp.arange(head_count, dtype=jnp.int32)
    valid_limit = valid_count[0]
    row_index = device * block_rows + local_index
    near_devices = min(SPAN0, total_rows) // block_rows
    near_rows = projected_rows[1:]
    for bit_index in range(near_devices.bit_length() - 1):
        partner = from_partner(near_rows, "seq", bit_index)
        upper_half = device // (1 << bit_index) % 2 == 1
        near_rows = jnp.where(
            upper_half,
            jnp.concatenate([partner, near_rows], 1),
            jnp.concatenate([near_rows, partner], 1),
        )
    near_start = device // near_devices * near_devices * block_rows
    near_pos = jnp.broadcast_to(
        near_start + jnp.arange(near_rows.shape[1], dtype=jnp.int32),
        (head_count, near_rows.shape[1]),
    )
    near_out, near_mass = attend(
        projected_rows[0], near_rows[0], near_rows[1], near_pos, valid_limit, head_count
    )
    near_sel = jnp.ones((block_rows, head_count), dtype=bool)
    middle_level_offsets = head_indices % DILATION_SECOND
    middle_level = select_rows(projected_rows, DILATION_SECOND, middle_level_offsets)
    middle_devices = min(SPAN1, total_rows) // block_rows
    middle_key_value = middle_level[1:]
    every_row = lax.all_gather(middle_key_value, "seq", axis=1, tiled=True)
    group_rows = middle_devices * middle_key_value.shape[1]
    middle_key_value = lax.dynamic_slice_in_dim(
        every_row, device // middle_devices * group_rows, group_rows, 1
    )
    middle_start = device // middle_devices * middle_devices * block_rows
    middle_pos = (
        middle_start
        + middle_level_offsets[:, None]
        + DILATION_SECOND * jnp.arange(middle_key_value.shape[1], dtype=jnp.int32)[None, :]
    )
    middle_attention, middle_log_sum = attend(
        middle_level[0],
        middle_key_value[0],
        middle_key_value[1],
        middle_pos,
        valid_limit,
        head_count,
    )
    middle_output, middle_level_mass, middle_selected = scatter_rows(
        middle_attention, middle_log_sum, DILATION_SECOND, middle_level_offsets
    )
    distant_offsets = head_indices % DILATION_THIRD
    distant_local_rows = select_rows(projected_rows, DILATION_THIRD, distant_offsets)
    distant_key_value = lax.all_gather(distant_local_rows[1:], "seq", axis=1, tiled=True)
    distant_positions = (
        distant_offsets[:, None]
        + DILATION_THIRD * jnp.arange(distant_key_value.shape[1], dtype=jnp.int32)[None, :]
    )
    distant_attention, distant_log_sum = attend(
        distant_local_rows[0],
        distant_key_value[0],
        distant_key_value[1],
        distant_positions,
        valid_limit,
        head_count,
    )
    distant_output, distant_mass, distant_selected = scatter_rows(
        distant_attention, distant_log_sum, DILATION_THIRD, distant_offsets
    )
    outputs = jnp.stack([near_out, middle_output, distant_output])
    masses = jnp.stack([near_mass, middle_level_mass, distant_mass])
    selects = jnp.stack([near_sel, middle_selected, distant_selected])
    ceiling = jnp.max(masses, axis=0)
    shares = jnp.where(selects, jnp.exp(masses - ceiling), 0.0)
    combined = jnp.sum(shares[..., None] * outputs, axis=0) / jnp.sum(shares, axis=0)[..., None]
    combined = jnp.where((row_index < valid_limit)[:, None, None], combined, 0.0).reshape(
        block_rows, cols_here
    )
    row_total, row_square = lax.psum(
        (jnp.sum(combined, axis=1), jnp.sum(combined * combined, axis=1)), "head"
    )
    mean_value = row_total / DS
    mean_square = row_square / DS
    scaling = lax.rsqrt(mean_square - mean_value * mean_value + layer_eps)
    settled = ((combined - mean_value[:, None]) * scaling[:, None] * sub_gain).astype(jnp.bfloat16)
    partial_rows = jnp.dot(settled, w_out, preferred_element_type=jnp.float32)
    branch_sum = lax.psum_scatter(partial_rows, "head", scatter_dimension=1, tiled=True)
    return own_part.astype(jnp.float32) + branch_sum


MESH = pl.DeviceIdType.MESH
LANES = 128


def remote(src, dst, send_sem, recv_sem, device):
    return pltpu.make_async_remote_copy(
        src_ref=src,
        dst_ref=dst,
        send_sem=send_sem,
        recv_sem=recv_sem,
        device_id=device,
        device_id_type=MESH,
    )


def dot_rows(left, right):
    return lax.dot_general(
        left, right, (((1,), (1,)), ((), ())), preferred_element_type=jnp.float32
    )


def encode_kernel(
    tiles,
    valid_ref,
    tok_hbm,
    gain_ref,
    scale_ref,
    fc_ref,
    w_hbm,
    down_hbm,
    embed_hbm,
    pre_ref,
    wcol_ref,
    bias_ref,
    sub_ref,
    order_ref,
    slide_ref,
    qkv_hbm,
    out_ref,
    tok_ref,
    down_ref,
    embed_ref,
    qkv_ref,
    wcol_parts,
    narrow_ref,
    pre_own,
    pre_out,
    new_out,
    wcol_out,
    sub_out,
    sequence,
    queries,
    key_rows,
    value_cols,
    fresh,
    keep_rows,
    keep_cols,
    slide_col,
    sub_col,
    mix_old,
    mix_query,
    mix_mass,
    new_kv,
    new_mix,
    normed,
    wall,
    acc,
    pool_mine,
    pooled,
    sums,
    means,
    parts,
    local_sem,
    send_tok,
    recv_tok,
    send_w,
    recv_w,
    send_pre,
    recv_pre,
    send_fan,
    recv_fan,
    send_aux,
    recv_aux,
    send_pool,
    recv_pool,
    send_mean,
    recv_mean,
    send_part,
    recv_part,
    send_new,
    recv_new,
    send_mix,
    recv_mix,
    send_kv,
    recv_kv,
):
    n = lax.axis_size("seq")
    heads = lax.axis_size("head")
    z = lax.axis_index("seq")
    hd = lax.axis_index("head")
    y = lax.axis_index("groups")
    rows, width = tok_hbm.shape
    patch = rows // tiles
    depth, hidden_width = w_hbm.shape[1:]
    quarter = rows // heads
    share = hidden_width // 4
    blocks_k = depth // LANES
    blocks_c = share // LANES
    narrow = wcol_ref.shape[0]

    part = lax.rem(z, 2)
    pair = z // 2
    partner = z + 1 - 2 * part
    at_end = (z == 0) | (z == n - 1)
    inside = jnp.logical_not(at_end)
    inner = n - 1 - z
    outward = jnp.where(z < 2, 0, n - 1)
    toward = jnp.where(z < 2, 1, n - 1)
    across = lax.rem(hd + 2, heads)
    mate = hd + 1 - 2 * lax.rem(hd, 2)
    beyond = lax.rem(mate + 2, heads)

    def seq_peer(k):
        return lax.rem(z + k, n)

    def ahead(k):
        return lax.rem(z + k * toward, n)

    def head_peer(k):
        return lax.rem(hd + k, heads)

    def head_source(k):
        return lax.rem(hd + heads - k, heads)

    def quarter_rows(index):
        return pl.ds(pl.multiple_of(index * quarter, quarter), quarter)

    def unit(u):
        return u // blocks_c, u % blocks_c

    def weight_block(owner, u):
        r, c = unit(u)
        place = (lax.rem(owner, 2) * 2 + y) * share + c * LANES
        return w_hbm.at[
            :, pl.ds(r * LANES, LANES), pl.ds(pl.multiple_of(place, LANES), LANES)
        ]

    def wall_block(source, u):
        r, c = unit(u)
        return wall.at[r, c, :, pl.ds(pl.multiple_of(source * LANES, LANES), LANES), :]

    units = blocks_k * blocks_c
    half = quarter // 2
    first_quarters = (hd, across, mate, beyond)
    token_loads = [
        pltpu.make_async_copy(
            tok_hbm.at[quarter_rows(q)], tok_ref.at[quarter_rows(q)], local_sem.at[i]
        )
        for i, q in enumerate(first_quarters)
    ]
    loads = [
        pltpu.make_async_copy(source, target, local_sem.at[4 + i])
        for i, (source, target) in enumerate(
            ((qkv_hbm, qkv_ref), (down_hbm, down_ref), (embed_hbm, embed_ref))
        )
    ]
    weight_loads = [
        pltpu.make_async_copy(weight_block(z, u), wall_block(z, u), local_sem.at[7])
        for u in range(units)
    ]
    barrier = pltpu.get_barrier_semaphore()
    count = 0
    for k in range(n):
        for j in range(heads):
            if k or j:
                pl.semaphore_signal(
                    barrier,
                    inc=1,
                    device_id={"seq": seq_peer(k), "head": head_peer(j)},
                    device_id_type=MESH,
                )
                count += 1
    for k in range(n):
        pl.semaphore_signal(
            barrier, inc=1, device_id={"groups": 1 - y, "seq": seq_peer(k)}, device_id_type=MESH
        )
        count += 1
    for load in token_loads + loads + weight_loads:
        load.start()

    block = 64

    def norm_quarter(position):
        index = first_quarters[position]
        token_loads[position].wait()

        def norm_rows(i, total):
            at = pl.ds(pl.multiple_of(index * quarter + i * block, block), block)
            values = tok_ref[at, :].astype(jnp.float32)
            out = normalize(values, gain_ref[...].reshape(1, width)).astype(jnp.bfloat16)
            normed[y * 2 + part, index, pl.ds(pl.multiple_of(i * block, block), block), :] = out
            return total + jnp.sum(values, axis=0, keepdims=True)

        sums[index] = lax.fori_loop(
            0, quarter // block, norm_rows, jnp.zeros((1, width), jnp.float32)
        )

    cols, stored_count = pre_ref.shape
    stored_rows = stored_count + tiles
    pre_own[...] = jnp.concatenate(
        [pre_ref[...], jnp.zeros((cols, tiles), jnp.bfloat16)], axis=1
    )
    norm_quarter(0)
    pl.semaphore_wait(barrier, count)

    def send(source, target, sends, receives, device):
        remote(source, target, sends, receives, device).start()

    def send_weight(k, u):
        target = ahead(k)
        send(
            weight_block(target, u), wall_block(z, u), send_w.at[0], recv_w.at[u], {"seq": target}
        )

    own_set = y * 2 + part
    z_set = y * 2 + 1 - part
    y_set = (1 - y) * 2 + part
    d_set = (1 - y) * 2 + 1 - part

    def token_copy(which, index, event, part_of, device):
        slot = normed.at[which, index, pl.ds(part_of * half, half)]
        return remote(slot, slot, send_tok.at[0], recv_tok.at[event, part_of], device)

    def fan_copy(block_index, share_index, event, device):
        slot = pre_out.at[block_index, share_index]
        return remote(slot, slot, send_fan.at[0], recv_fan.at[event, block_index], device)

    for index in range(2):
        target = jnp.where(
            at_end,
            jnp.where(z == 0, 1 + index, n - 2 - index),
            outward if index == 0 else inner,
        )
        send(pre_own, pre_out.at[z, hd], send_pre.at[0], recv_pre.at[z], {"seq": target})
    token_copy(own_set, hd, 0, 0, {"seq": partner}).start()
    for part_of in range(2):
        token_copy(own_set, hd, 4, part_of, {"groups": 1 - y}).start()

    @pl.when(at_end)
    def _():
        token_copy(own_set, hd, 0, 1, {"seq": partner}).start()

    @pl.when(at_end)
    def _():
        for u in range(units):
            send_weight(2, u)
        for u in range(units):
            send_weight(1, u)
            send_weight(3, u)

    @pl.when(inside)
    def _():
        for u in range(units):
            send_weight(1, u)

    pre_out[z, hd] = pre_own[...]
    norm_quarter(1)

    def fan_first(b):
        fan_copy(b, hd, 0, {"head": across}).start()
        fan_copy(b, hd, 1, {"head": mate}).start()

    def fan_second(b):
        fan_copy(b, across, 0, {"head": across}).wait_recv()
        fan_copy(b, across, 2, {"head": mate}).start()

    def stored_block(b, forward=False):
        slot = pre_out.at[b, hd]
        remote(slot, slot, send_pre.at[0], recv_pre.at[b], {"seq": partner}).wait_recv()
        if forward:
            send(slot, slot, send_pre.at[1], recv_pre.at[b], {"seq": outward})
        fan_first(b)

    fan_first(z)
    second_end = jnp.where(z == 0, 2, n - 3)

    @pl.when(at_end)
    def _():
        stored_block(partner)

    @pl.when(inside)
    def _():
        stored_block(inner, True)
        token_copy(own_set, hd, 0, 1, {"seq": partner}).start()
        stored_block(outward)

    norm_quarter(2)
    norm_quarter(3)
    for tile in range(tiles):
        per = heads // tiles
        means[z, pl.ds(tile, 1), :] = (
            sum(sums[tile * per + i] for i in range(per)) / patch
        )
    for k in range(1, n):
        send(means.at[z], means.at[z], send_mean.at[0], recv_mean.at[0], {"seq": seq_peer(k)})
    narrow_ref[pl.ds(0, 1), :] = bias_ref[...].reshape(1, narrow)
    narrow_ref[pl.ds(1, 1), :] = sub_ref[...].reshape(1, narrow)
    for j in range(heads):
        wcol_parts[j] = wcol_ref[:, j * narrow : (j + 1) * narrow].T
    wcol_out[hd] = wcol_parts[hd]
    sub_out[hd] = narrow_ref[...]

    def column(row):
        size = row.shape[1]
        same = lax.broadcasted_iota(jnp.int32, (size, size), 0) == lax.broadcasted_iota(
            jnp.int32, (size, size), 1
        )
        return jnp.sum(jnp.where(same, row, 0.0), axis=1, keepdims=True)

    features = heads * cols
    for start in range(0, features, LANES):
        at = pl.ds(start, LANES)
        slide_col[at, :] = column(slide_ref[...].reshape(1, features)[:, start : start + LANES])

    def token_event(which, index, event, part_of, forwards):
        token_copy(which, index, event, part_of, {"head": mate}).wait_recv()
        for to, device in forwards:
            token_copy(which, index, to, part_of, device).start()

    from_z = ((8, {"groups": 1 - y}), (1, {"head": across}), (2, {"head": mate}))
    token_event(y_set, hd, 4, 0, ((6, {"head": mate}),))
    fan_second(z)

    @pl.when(inside)
    def _():
        stored_block(n - 1 - outward, True)
        for u in range(units):
            send_weight(3, u)

    token_event(z_set, hd, 0, 0, from_z)
    token_event(y_set, hd, 4, 1, ((6, {"head": mate}),))

    @pl.when(at_end)
    def _():
        fan_second(partner)
        stored_block(second_end)

    @pl.when(inside)
    def _():
        fan_second(inner)
        fan_second(outward)

    token_event(z_set, hd, 0, 1, from_z)
    for part_of in range(2):
        token_copy(own_set, across, 5, part_of, {"groups": 1 - y}).start()

    @pl.when(at_end)
    def _():
        stored_block(n - 1 - z)
        fan_second(second_end)
        fan_second(n - 1 - z)

    @pl.when(inside)
    def _():
        fan_second(n - 1 - outward)

    for k in range(1, heads):
        send(
            wcol_parts.at[head_peer(k)],
            wcol_out.at[hd],
            send_aux.at[0],
            recv_aux.at[0],
            {"head": head_peer(k)},
        )
        send(narrow_ref, sub_out.at[hd], send_aux.at[1], recv_aux.at[1], {"head": head_peer(k)})

    step = stored_rows
    total_rows = n * step
    limit = valid_ref[0]
    new_count = n * tiles
    factor = 1.0 / math.sqrt(HEAD_DIM)
    head_count = cols // HEAD_DIM

    def multiplicity(first, second, offset):
        middle = (first % DILATION_SECOND == offset % DILATION_SECOND) & (
            second % DILATION_SECOND == offset % DILATION_SECOND
        )
        distant = (first % DILATION_THIRD == offset % DILATION_THIRD) & (
            second % DILATION_THIRD == offset % DILATION_THIRD
        )
        return 1.0 + jnp.where(middle, 1.0, 0.0) + jnp.where(distant, 1.0, 0.0)

    def sequence_step(t):
        at = pl.ds(t * step, step)
        per = step // LANES
        order = jnp.concatenate([order_ref[pl.ds(t * per + i, 1), :] for i in range(per)], axis=1)
        label = lax.broadcasted_iota(jnp.int32, (step, step), 0)
        label = jnp.where(label < stored_count, label + tiles, -n * step)
        picks = jnp.concatenate(
            [jnp.where(order == label + b * step, 1.0, 0.0).astype(jnp.bfloat16) for b in range(n)],
            axis=0,
        )
        label = lax.broadcasted_iota(jnp.int32, (LANES, step), 0)
        wanted = jnp.where(label < new_count, label // tiles * step + label % tiles, -1)
        found = jnp.where(order == wanted, 1.0, 0.0)
        fresh[t] = found.astype(jnp.bfloat16)
        lane = lax.broadcasted_iota(jnp.int32, (1, step), 1) + t * step
        keep_cols[:, t * step : (t + 1) * step] = jnp.where(
            lane < limit, 1.0 - jnp.sum(found, axis=0, keepdims=True), 0.0
        )
        row = lax.broadcasted_iota(jnp.int32, (step, 1), 0) + t * step
        keep_rows[at, :] = jnp.where(
            row < limit, 1.0 - jnp.sum(found.T, axis=1, keepdims=True), 0.0
        )
        stored = jnp.concatenate(
            [jnp.concatenate([pre_out[b, j] for b in range(n)], axis=1) for j in range(heads)],
            axis=0,
        )
        values = jnp.dot(stored, picks, preferred_element_type=jnp.float32)
        sequence[t] = values.astype(jnp.bfloat16).reshape(heads, cols, step)
        centered = values - jnp.sum(values, axis=0, keepdims=True) / features
        variance = jnp.sum(centered * centered, axis=0, keepdims=True) / features
        normal = (centered * lax.rsqrt(variance + layer_eps) * slide_col[...]).astype(jnp.bfloat16)
        result = jnp.dot(
            qkv_ref[...].reshape(3 * cols, features), normal, preferred_element_type=jnp.float32
        ).astype(jnp.bfloat16)
        queries[t] = result[:cols]
        key_rows[at, :] = result[cols : 2 * cols].T
        value_cols[:, t * step : (t + 1) * step] = result[2 * cols :]

    def attend_stored():
        query = queries[z]
        row_head = lax.broadcasted_iota(jnp.int32, (cols, 1), 0) // HEAD_DIM
        key_at = lax.broadcasted_iota(jnp.int32, (total_rows, 1), 0)
        query_at = lax.broadcasted_iota(jnp.int32, (1, step), 1) + z * step
        for h in range(head_count):
            own = jnp.where(row_head == h, query, jnp.zeros((), jnp.bfloat16))
            scores = jnp.dot(key_rows[...], own, preferred_element_type=jnp.float32) * factor
            scores = jnp.where(keep_rows[...] > 0.0, scores, masked_score)
            peak = jnp.max(scores, axis=0, keepdims=True)
            weights = jnp.exp(scores - peak) * multiplicity(
                key_at, query_at, hd * head_count + h
            )
            at = slice(h * HEAD_DIM, (h + 1) * HEAD_DIM)
            values = jnp.concatenate(
                [value_cols[at, :], jnp.ones((16, total_rows), jnp.bfloat16)], axis=0
            )
            total = jnp.dot(
                values, weights.astype(jnp.bfloat16), preferred_element_type=jnp.float32
            )
            mass = total[HEAD_DIM : HEAD_DIM + 1]
            mix_old[hd, at, :] = (total[:HEAD_DIM] / mass).astype(jnp.bfloat16)
            mix_mass[hd, h * 8 : (h + 1) * 8, :] = jnp.broadcast_to(peak + jnp.log(mass), (8, step))
        mix_query[hd] = query
        for k in range(1, heads):
            for index, buffer in enumerate((mix_query, mix_mass, mix_old)):
                send(
                    buffer.at[hd],
                    buffer.at[hd],
                    send_mix.at[index],
                    recv_mix.at[index],
                    {"head": head_peer(k)},
                )

    loads[0].wait()
    for b in range(n):
        for event, source in ((1, mate), (2, beyond)):
            fan_copy(b, source, event, {"head": mate}).wait_recv()
    relays = (
        (z_set, across, 1, ((3, {"head": mate}),)),
        (d_set, hd, 8, ((9, {"head": across}), (10, {"head": mate}))),
        (y_set, across, 5, ((7, {"head": mate}),)),
        (d_set, across, 9, ((11, {"head": mate}),)),
    )
    for t in range(total_rows // step):
        sequence_step(t)
        if t == 0:

            @pl.when(inside)
            def _():
                for u in range(units):
                    send_weight(2, u)

        for which, index, event, forwards in relays[t : t + 1] if t < 3 else ():
            for part_of in range(2):
                token_event(which, index, event, part_of, forwards)
    attend_stored()
    for which, index, event, forwards in relays[3:]:
        for part_of in range(2):
            token_event(which, index, event, part_of, forwards)
    for which, first in ((z_set, 0), (y_set, 4), (d_set, 8)):
        for part_of in range(2):
            token_event(which, mate, first + 2, part_of, ())
            token_event(which, beyond, first + 3, part_of, ())

    for buffer, receives in ((wcol_out, recv_aux.at[0]), (sub_out, recv_aux.at[1])):
        slot = buffer.at[pl.ds(0, heads - 1)]
        remote(slot, slot, send_new.at[0], receives, {"head": mate}).wait_recv()
    for j in range(heads):
        sub_col[pl.ds(j * cols, cols), :] = column(sub_out[j, 1:2])
    whole = wall.at[:, :, :, pl.ds(0, LANES), :]
    pltpu.make_async_copy(whole, whole, local_sem.at[7]).wait()

    def multiply(u):
        r, c = unit(u)
        others = wall.at[r, c, :, pl.ds(0, (n - 1) * LANES), :]
        remote(others, others, send_w.at[0], recv_w.at[u], {"seq": partner}).wait_recv()

        @pl.loop(0, 4)
        def _(s):
            w = jnp.concatenate([wall[r, c, 0], wall[r, c, 1]], axis=1)
            x = jnp.concatenate(
                [
                    normed[s, :, :, b * depth + r * LANES : b * depth + (r + 1) * LANES].reshape(
                        rows, LANES
                    )
                    for b in range(n)
                ],
                axis=1,
            )
            value = jnp.dot(x, w, preferred_element_type=jnp.float32)
            if r == 0:
                acc[c, s] = value
            else:
                acc[c, s] += value

    def pool(c):
        for s in range(4):
            for tile in range(tiles):
                at = pl.ds(tile * patch, patch)
                gate = acc[c, s, at, :LANES]
                hidden = (gate / (1.0 + jnp.exp(-gate)) * acc[c, s, at, LANES:]).astype(
                    jnp.bfloat16
                )
                pool_mine[s // 2, c, pl.ds((s % 2) * tiles + tile, 1), :] = (
                    jnp.sum(hidden.astype(jnp.float32), axis=0, keepdims=True) / patch
                )
        place = y * n + z
        pooled[place, c] = pool_mine[y, c]
        for k in range(n):
            for other in range(2):
                if k or other:
                    yy = 1 - y if other else y
                    send(
                        pool_mine.at[yy, c],
                        pooled.at[place, c],
                        send_pool.at[c],
                        recv_pool.at[c],
                        {"groups": yy, "seq": seq_peer(k)},
                    )

    for u in range(units):
        multiply(u)
        r, c = unit(u)
        if r == blocks_k - 1:
            pool(c)

    seen = means.at[pl.ds(0, n - 1)]
    remote(seen, seen, send_mean.at[0], recv_mean.at[0], {"seq": partner}).wait_recv()
    for c in range(blocks_c):
        slot = pooled.at[pl.ds(0, 2 * n - 1), c]
        remote(slot, slot, send_pool.at[c], recv_pool.at[c], {"seq": partner}).wait_recv()
    loads[1].wait()
    loads[2].wait()
    everyone = jnp.concatenate(
        [
            jnp.concatenate(
                [
                    pooled[yy * n + b + m, c]
                    for m in range(2)
                    for yy in range(2)
                    for c in range(blocks_c)
                ],
                axis=1,
            )
            for b in range(0, n, 2)
        ],
        axis=0,
    )
    high = everyone.astype(jnp.bfloat16)
    rest = everyone - high.astype(jnp.float32)
    middle = rest.astype(jnp.bfloat16)
    low = (rest - middle.astype(jnp.float32)).astype(jnp.bfloat16)
    local_part = jnp.zeros((n * tiles, down_ref.shape[1]), jnp.float32)
    for piece in (low, middle, high):
        local_part += jnp.dot(piece, down_ref[...], preferred_element_type=jnp.float32)
    here = z * heads + hd
    parts[here] = local_part
    for k in range(n):
        for j in range(heads):
            if k or j:
                send(
                    parts.at[here],
                    parts.at[here],
                    send_part.at[0],
                    recv_part.at[0],
                    {"seq": seq_peer(k), "head": head_peer(j)},
                )
    slot = parts.at[pl.ds(0, n * heads - 1)]
    remote(slot, slot, send_part.at[0], recv_part.at[0], {"seq": partner}).wait_recv()
    summed = jnp.concatenate(
        [sum(parts[b * heads + j] for j in range(heads)) for b in range(n)], axis=1
    )
    average = jnp.concatenate([means[b] for b in range(n)], axis=0)
    feature = normalize(
        average + scale_ref[...].reshape(1, width) * summed, fc_ref[...].reshape(1, width)
    ).astype(jnp.bfloat16)
    new_out[hd] = (dot_rows(feature, embed_ref[...]) + narrow_ref[pl.ds(0, 1), :]).astype(
        jnp.bfloat16
    )
    for k in range(1, heads):
        send(new_out.at[hd], new_out.at[hd], send_new.at[0], recv_new.at[0], {"head": head_peer(k)})

    def peers(buffer, receives):
        slot = buffer.at[pl.ds(0, heads - 1)]
        remote(slot, slot, send_new.at[0], receives, {"head": mate}).wait_recv()

    peers(new_out, recv_new.at[0])
    fresh_values = jnp.concatenate([new_out[j].astype(jnp.float32) for j in range(heads)], axis=1)
    normal = normalize(fresh_values, slide_ref[...].reshape(1, features)).astype(jnp.bfloat16)
    new_query, new_key, new_value = [
        dot_rows(normal, qkv_ref[g]).astype(jnp.bfloat16) for g in range(3)
    ]
    new_kv[hd, 0] = new_key
    new_kv[hd, 1] = new_value
    for k in range(1, heads):
        send(new_kv.at[hd], new_kv.at[hd], send_kv.at[0], recv_kv.at[0], {"head": head_peer(k)})
    lane_head = lax.broadcasted_iota(jnp.int32, (1, cols), 1) // HEAD_DIM
    nothing = jnp.zeros((), jnp.bfloat16)

    def by_head(rows_in):
        return jnp.concatenate(
            [jnp.where(lane_head == h, rows_in, nothing) for h in range(head_count)], axis=0
        )

    key_at = lax.broadcasted_iota(jnp.int32, (new_count, total_rows), 1)
    placed = jnp.concatenate([fresh[t, :new_count].astype(jnp.float32) for t in range(n)], axis=1)
    new_at = jnp.sum(placed * key_at.astype(jnp.float32), axis=1, keepdims=True).astype(jnp.int32)
    other = lax.broadcasted_iota(jnp.int32, (1, LANES), 1)
    new_lane = jnp.sum(
        jnp.where(other == lax.broadcasted_iota(jnp.int32, (new_count, LANES), 0), new_at, 0),
        axis=0,
        keepdims=True,
    )[:, :new_count]

    many = by_head(new_query)
    scores = dot_rows(many, key_rows[...]) * factor
    scores = jnp.where(keep_cols[...] > 0.0, scores, masked_score)
    recent = dot_rows(many, new_key) * factor
    recent = jnp.where(new_lane < limit, recent, masked_score)
    peak = jnp.maximum(
        jnp.max(scores, axis=1, keepdims=True), jnp.max(recent, axis=1, keepdims=True)
    )
    row_at = jnp.concatenate([new_at] * head_count, axis=0)
    offset = hd * head_count + lax.broadcasted_iota(
        jnp.int32, (head_count * new_count, 1), 0
    ) // new_count
    weights = jnp.exp(scores - peak) * multiplicity(key_at[:1], row_at, offset)
    recent = jnp.exp(recent - peak) * multiplicity(new_lane, row_at, offset)
    mass = jnp.sum(weights, axis=1, keepdims=True) + jnp.sum(recent, axis=1, keepdims=True)
    attended = (
        dot_rows(weights.astype(jnp.bfloat16), value_cols[...])
        + jnp.dot(recent.astype(jnp.bfloat16), new_value, preferred_element_type=jnp.float32)
    ) / mass
    new_mix[hd] = sum(
        jnp.where(lane_head == h, attended[h * new_count : (h + 1) * new_count], 0.0)
        for h in range(head_count)
    ).astype(jnp.bfloat16)
    for k in range(1, heads):
        send(new_mix.at[hd], new_mix.at[hd], send_kv.at[1], recv_kv.at[1], {"head": head_peer(k)})

    for index, buffer in enumerate((mix_query, mix_mass, mix_old)):
        peers(buffer, recv_mix.at[index])
    peers(new_kv, recv_kv.at[0])
    query_at = lax.broadcasted_iota(jnp.int32, (1, step), 1) + z * step
    here_fresh = fresh[z, :new_count]
    known = 1.0 - jnp.sum(here_fresh.astype(jnp.float32), axis=0, keepdims=True)
    known = jnp.where(query_at < limit, known, 0.0)
    betas, alphas = [], []
    for j in range(heads):
        scores = (
            jnp.dot(by_head(new_kv[j, 0]), mix_query[j], preferred_element_type=jnp.float32)
            * factor
        )
        scores = jnp.where(row_at < limit, scores, masked_score)
        offset = j * head_count + lax.broadcasted_iota(
            jnp.int32, (head_count * new_count, 1), 0
        ) // new_count
        grouped = (head_count, new_count, step)
        scores = scores.reshape(grouped)
        stored_mass = mix_mass[j].reshape(grouped)
        ceiling = jnp.maximum(jnp.max(scores, axis=1, keepdims=True), stored_mass)
        weights = jnp.exp(scores - ceiling) * multiplicity(row_at, query_at, offset).reshape(grouped)
        old = jnp.exp(stored_mass - ceiling)
        inverse = known / (old + jnp.sum(weights, axis=1, keepdims=True))
        betas.append((weights * inverse).reshape(head_count * new_count, step))
        alphas.append(old * inverse)

    peers(new_mix, recv_kv.at[1])
    inside_limit = jnp.where(query_at < limit, here_fresh.astype(jnp.float32), 0.0)

    def contract(left, right):
        return lax.dot_general(
            left, right, (((0,), (0,)), ((), ())), preferred_element_type=jnp.float32
        )

    pieces = []
    for j in range(heads):
        left = jnp.concatenate([by_head(new_kv[j, 1]), new_mix[j]], axis=0)
        right = jnp.concatenate([betas[j], inside_limit], axis=0).astype(jnp.bfloat16)
        share_of = jnp.concatenate(
            [
                mix_old[j, h * HEAD_DIM : (h + 1) * HEAD_DIM, :].astype(jnp.float32)
                * alphas[j][h, :1]
                for h in range(head_count)
            ],
            axis=0,
        )
        pieces.append(share_of + contract(left, right))
    mean = sum(jnp.sum(p, axis=0, keepdims=True) for p in pieces) / features
    square = sum(jnp.sum(p * p, axis=0, keepdims=True) for p in pieces) / features
    scaling = lax.rsqrt(square - mean * mean + layer_eps)
    branch = sequence[z, hd].astype(jnp.float32) + contract(new_out[hd], here_fresh)
    for j in range(heads):
        gain = sub_col[pl.ds(j * cols, cols), :]
        settled = ((pieces[j] - mean) * scaling * gain).astype(jnp.bfloat16)
        branch += jnp.dot(wcol_out[j], settled, preferred_element_type=jnp.float32)
    out_ref[...] = branch

    def drain(slot, sends):
        remote(slot, slot, sends, recv_new.at[0], {"head": mate}).wait_send()

    drain(normed.at[pl.ds(0, 3)], send_tok.at[0])
    drain(wall.at[:, :, :, pl.ds(0, (n - 1) * LANES), :], send_w.at[0])
    drain(pre_out.at[0, pl.ds(0, 2)], send_pre.at[0])

    @pl.when(inside)
    def _():
        drain(pre_out.at[0, pl.ds(0, 2)], send_pre.at[1])

    drain(pre_out.at[pl.ds(0, 3)], send_fan.at[0])
    drain(wcol_out.at[pl.ds(0, heads - 1)], send_aux.at[0])
    drain(sub_out.at[pl.ds(0, heads - 1)], send_aux.at[1])
    for c in range(blocks_c):
        drain(pooled.at[pl.ds(0, 2 * n - 1), c], send_pool.at[c])
    drain(means.at[pl.ds(0, n - 1)], send_mean.at[0])
    drain(parts.at[pl.ds(0, n * heads - 1)], send_part.at[0])
    drain(new_out.at[pl.ds(0, heads - 1)], send_new.at[0])
    for index, buffer in enumerate((mix_query, mix_mass, mix_old)):
        drain(buffer.at[pl.ds(0, heads - 1)], send_mix.at[index])
    drain(new_kv.at[pl.ds(0, heads - 1)], send_kv.at[0])
    drain(new_mix.at[pl.ds(0, heads - 1)], send_kv.at[1])


def near_body(
    tile_tokens,
    tile_gain,
    w_gate_up,
    w_down,
    layer_scale,
    fc_gain,
    w_embed,
    embed_bias,
    pre_emb,
    tile_order,
    valid_count,
    slide_gain,
    w_qkv,
    sub_gain,
    w_out,
):
    n = lax.axis_size("seq")
    heads = lax.axis_size("head")
    tiles, patch, width = tile_tokens.shape
    depth, hidden_width = w_gate_up.shape[1:]
    rows = tiles * patch
    cols = w_embed.shape[1]
    head_count = cols // HEAD_DIM
    total_rows = tile_order.shape[0]
    block_rows = total_rows // n
    vmem = pl.BlockSpec(memory_space=pltpu.VMEM)
    anywhere = pl.BlockSpec(memory_space=pl.ANY)
    dma = pltpu.SemaphoreType.DMA
    f32, bf16 = jnp.float32, jnp.bfloat16
    quarter = rows // heads
    blocks_k = depth // LANES
    blocks_c = hidden_width // 4 // LANES
    out = pl.pallas_call(
        functools.partial(encode_kernel, tiles),
        out_shape=jax.ShapeDtypeStruct((cols, block_rows), f32),
        in_specs=[
            pl.BlockSpec(memory_space=pltpu.SMEM),
            anywhere,
            vmem,
            vmem,
            vmem,
            anywhere,
            anywhere,
            anywhere,
            vmem,
            vmem,
            vmem,
            vmem,
            vmem,
            vmem,
            anywhere,
        ],
        out_specs=vmem,
        scratch_shapes=[
            pltpu.VMEM((rows, width), bf16),
            pltpu.VMEM(w_down.shape, bf16),
            pltpu.VMEM((cols, width), bf16),
            pltpu.VMEM((3, cols, heads * cols), bf16),
            pltpu.VMEM((heads, cols, cols), bf16),
            pltpu.VMEM((2, cols), f32),
            pltpu.VMEM((cols, block_rows), bf16),
            pltpu.VMEM((n, heads, cols, block_rows), bf16),
            pltpu.VMEM((heads, n * tiles, cols), bf16),
            pltpu.VMEM((heads, cols, cols), bf16),
            pltpu.VMEM((heads, 2, cols), f32),
            pltpu.VMEM((n, heads, cols, block_rows), bf16),
            pltpu.VMEM((n, cols, block_rows), bf16),
            pltpu.VMEM((total_rows, cols), bf16),
            pltpu.VMEM((cols, total_rows), bf16),
            pltpu.VMEM((n, LANES, block_rows), bf16),
            pltpu.VMEM((total_rows, 1), f32),
            pltpu.VMEM((1, total_rows), f32),
            pltpu.VMEM((heads * cols, 1), f32),
            pltpu.VMEM((heads * cols, 1), f32),
            pltpu.VMEM((heads, cols, block_rows), bf16),
            pltpu.VMEM((heads, cols, block_rows), bf16),
            pltpu.VMEM((heads, head_count * 8, block_rows), f32),
            pltpu.VMEM((heads, 2, n * tiles, cols), bf16),
            pltpu.VMEM((heads, n * tiles, cols), bf16),
            pltpu.VMEM((4, heads, quarter, width), bf16),
            pltpu.VMEM((blocks_k, blocks_c, 2, n * LANES, LANES), bf16),
            pltpu.VMEM((blocks_c, 4, rows, 2 * LANES), f32),
            pltpu.VMEM((2, blocks_c, 2 * tiles, LANES), f32),
            pltpu.VMEM((2 * n, blocks_c, 2 * tiles, LANES), f32),
            pltpu.VMEM((heads, 1, width), f32),
            pltpu.VMEM((n, tiles, width), f32),
            pltpu.VMEM((n * heads, n * tiles, w_down.shape[1]), f32),
            dma((8,)),
            dma((1,)),
            dma((12, 2)),
            dma((1,)),
            dma((blocks_k * blocks_c,)),
            dma((2,)),
            dma((n,)),
            dma((1,)),
            dma((3, n)),
            dma((2,)),
            dma((2,)),
            dma((blocks_c,)),
            dma((blocks_c,)),
            dma((1,)),
            dma((1,)),
            dma((1,)),
            dma((1,)),
            dma((1,)),
            dma((1,)),
            dma((3,)),
            dma((3,)),
            dma((2,)),
            dma((2,)),
        ],
        compiler_params=pltpu.CompilerParams(
            collective_id=0, has_side_effects=True, vmem_limit_bytes=58 * 1024 * 1024
        ),
    )(
        valid_count,
        tile_tokens.reshape(rows, width),
        tile_gain,
        layer_scale,
        fc_gain,
        w_gate_up,
        w_down,
        w_embed.T,
        pre_emb.T,
        w_out,
        embed_bias,
        sub_gain,
        tile_order.reshape(total_rows // LANES, LANES),
        slide_gain,
        w_qkv.swapaxes(1, 2),
    )
    return out.T


def body(*args):
    total_rows = args[9].shape[0]
    mesh_fits = all(lax.axis_size(a) == k for a, k in (("groups", 2), ("seq", 4), ("head", 4)))
    if total_rows <= SPAN0 and mesh_fits:
        return near_body(*args)
    return general_body(*args)


def solution(mesh):
    placed = (
        P(("groups", "seq"), None, None),
        P(),
        P(None, "seq", "head"),
        P("head", "seq"),
        P(),
        P(),
        P(None, "head"),
        P("head"),
        P(("groups", "seq"), "head"),
        P("groups"),
        P("groups"),
        P(),
        P(None, None, "head"),
        P("head"),
        P("head", None),
    )
    return jax.shard_map(
        body, mesh=mesh, in_specs=placed, out_specs=P(("groups", "seq"), "head"), check_vma=False
    )
```

```python
import functools
import math

import jax
import jax.numpy as jnp
from jax import lax
from jax.experimental import pallas as pl
from jax.experimental.pallas import tpu as pltpu
from jax.sharding import PartitionSpec as P

DS = 768
HEAD_DIM = 48
SPAN0 = 1024
SPAN1 = 4096
DILATION_SECOND = 4
DILATION_THIRD = 16


layer_eps = 1e-05
masked_score = -1e30


def from_partner(value, axis, bit):
    mask = 2**bit
    pairs = [(source, source ^ mask) for source in range(lax.axis_size(axis))]
    return lax.ppermute(value, axis, pairs)


def normalize(values, gain):
    centered = values - jnp.mean(values, axis=-1, keepdims=True)
    variance = jnp.mean(centered * centered, axis=-1, keepdims=True)
    return centered * lax.rsqrt(variance + layer_eps) * gain


def select_rows(stacked, dilation, offsets):
    group_count, row_count, row_width = stacked.shape
    head_count = offsets.shape[0]
    arranged = stacked.reshape(
        group_count, row_count // dilation, dilation, head_count, row_width // head_count
    )
    choose = jnp.arange(dilation, dtype=jnp.int32)[:, None] == offsets[None, :]
    chosen = jnp.sum(
        jnp.where(choose[None, None, :, :, None], arranged, jnp.zeros((), stacked.dtype)), axis=2
    )
    return chosen.reshape(group_count, row_count // dilation, row_width)


def scatter_rows(attended, log_mass, dilation, offsets):
    query_count, head_count, head_size = attended.shape
    choose = jnp.arange(dilation, dtype=jnp.int32)[:, None] == offsets[None, :]
    spread_out = jnp.where(choose[None, :, :, None], attended[:, None, :, :], 0.0).reshape(
        query_count * dilation, head_count, head_size
    )
    spread_mass = jnp.where(choose[None, :, :], log_mass[:, None, :], masked_score).reshape(
        query_count * dilation, head_count
    )
    selected = jnp.broadcast_to(choose[None, :, :], (query_count, dilation, head_count)).reshape(
        query_count * dilation, head_count
    )
    return (spread_out, spread_mass, selected)


def attend(query_rows, key_rows, value_rows, positions, valid_limit, head_count):
    head_size = query_rows.shape[1] // head_count
    query_heads = query_rows.reshape(query_rows.shape[0], head_count, head_size)
    key_heads = key_rows.reshape(key_rows.shape[0], head_count, head_size)
    value_heads = value_rows.reshape(value_rows.shape[0], head_count, head_size)
    scores = jnp.einsum(
        "qhe,khe->hqk", query_heads, key_heads, preferred_element_type=jnp.float32
    ) / math.sqrt(head_size)
    scores = jnp.where((positions < valid_limit)[:, None, :], scores, masked_score)
    highest = jnp.max(scores, axis=-1, keepdims=True)
    exponent = jnp.exp(scores - highest)
    mass_sum = jnp.sum(exponent, axis=-1, keepdims=True)
    weights = (exponent / mass_sum).astype(jnp.bfloat16)
    attended = jnp.einsum("hqk,khe->qhe", weights, value_heads, preferred_element_type=jnp.float32)
    return (attended, (highest[..., 0] + jnp.log(mass_sum[..., 0])).T)


def general_body(
    tile_tokens,
    tile_gain,
    w_gate_up,
    w_down,
    layer_scale,
    fc_gain,
    w_embed,
    embed_bias,
    pre_emb,
    tile_order,
    valid_count,
    slide_gain,
    w_qkv,
    sub_gain,
    w_out,
):
    new_count, patch_count, tile_width = tile_tokens.shape
    token_rows = tile_tokens.reshape(new_count * patch_count, tile_width)
    normed = normalize(token_rows.astype(jnp.float32), tile_gain).astype(jnp.bfloat16)
    hidden_width = w_gate_up.shape[2]
    gate_up = jnp.einsum(
        "rk,gkf->grf",
        normed,
        lax.all_gather(w_gate_up, "seq", axis=1, tiled=True),
        preferred_element_type=jnp.float32,
    )
    hidden = (jax.nn.silu(gate_up[0]) * gate_up[1]).astype(jnp.bfloat16)
    pooled_hidden = jnp.mean(
        hidden.reshape(new_count, patch_count, hidden_width), axis=1, dtype=jnp.float32
    )
    everyone = lax.all_gather(pooled_hidden, "seq", axis=0, tiled=True)
    local_part = jnp.dot(everyone, w_down.astype(jnp.float32), precision=lax.Precision.HIGHEST)
    pooled_part = lax.all_to_all(local_part, "seq", split_axis=0, concat_axis=1, tiled=True)
    summed = lax.psum(pooled_part, "head")
    pooled = jnp.mean(tile_tokens, axis=1, dtype=jnp.float32) + layer_scale * summed
    feature = normalize(pooled, fc_gain).astype(jnp.bfloat16)
    new_rows = (jnp.dot(feature, w_embed, preferred_element_type=jnp.float32) + embed_bias).astype(
        jnp.bfloat16
    )
    stored = jnp.concatenate([new_rows, pre_emb], axis=0)
    block_rows = stored.shape[0]
    total_rows = tile_order.shape[0]
    peer_rows = block_rows // lax.axis_size("seq")
    device = lax.axis_index("seq")
    local_index = jnp.arange(block_rows, dtype=jnp.int32)
    inverse = (
        jnp.zeros((total_rows,), jnp.int32)
        .at[tile_order]
        .set(jnp.arange(total_rows, dtype=jnp.int32))
    )
    placed = lax.dynamic_slice_in_dim(inverse, device * block_rows, block_rows)
    target = placed // block_rows
    before = (target[:, None] == target[None, :]) & (placed[None, :] < placed[:, None])
    slot_index = target * peer_rows + jnp.sum(before, axis=1, dtype=jnp.int32)
    routing = (slot_index[None, :] == local_index[:, None]).astype(jnp.bfloat16)
    outgoing = jnp.dot(routing, stored, preferred_element_type=jnp.float32).astype(jnp.bfloat16)
    incoming = lax.all_to_all(outgoing, "seq", split_axis=0, concat_axis=0, tiled=True)
    wanted = lax.dynamic_slice_in_dim(tile_order, device * block_rows, block_rows)
    source = wanted // block_rows
    earlier = (source[:, None] == source[None, :]) & (local_index[None, :] < local_index[:, None])
    arrival = source * peer_rows + jnp.sum(earlier, axis=1, dtype=jnp.int32)
    own_part = jnp.take(incoming, arrival, axis=0)
    sequence = lax.all_gather(own_part, "head", axis=1, tiled=True)
    slide_normed = normalize(sequence.astype(jnp.float32), slide_gain).astype(jnp.bfloat16)
    projected_rows = jnp.einsum(
        "rd,gdc->grc", slide_normed, w_qkv, preferred_element_type=jnp.float32
    ).astype(jnp.bfloat16)
    cols_here = projected_rows.shape[2]
    head_count = cols_here // HEAD_DIM
    head_indices = lax.axis_index("head") * head_count + jnp.arange(head_count, dtype=jnp.int32)
    valid_limit = valid_count[0]
    row_index = device * block_rows + local_index
    near_devices = min(SPAN0, total_rows) // block_rows
    near_rows = projected_rows[1:]
    for bit_index in range(near_devices.bit_length() - 1):
        partner = from_partner(near_rows, "seq", bit_index)
        upper_half = device // (1 << bit_index) % 2 == 1
        near_rows = jnp.where(
            upper_half,
            jnp.concatenate([partner, near_rows], 1),
            jnp.concatenate([near_rows, partner], 1),
        )
    near_start = device // near_devices * near_devices * block_rows
    near_pos = jnp.broadcast_to(
        near_start + jnp.arange(near_rows.shape[1], dtype=jnp.int32),
        (head_count, near_rows.shape[1]),
    )
    near_out, near_mass = attend(
        projected_rows[0], near_rows[0], near_rows[1], near_pos, valid_limit, head_count
    )
    near_sel = jnp.ones((block_rows, head_count), dtype=bool)
    middle_level_offsets = head_indices % DILATION_SECOND
    middle_level = select_rows(projected_rows, DILATION_SECOND, middle_level_offsets)
    middle_devices = min(SPAN1, total_rows) // block_rows
    middle_key_value = middle_level[1:]
    every_row = lax.all_gather(middle_key_value, "seq", axis=1, tiled=True)
    group_rows = middle_devices * middle_key_value.shape[1]
    middle_key_value = lax.dynamic_slice_in_dim(
        every_row, device // middle_devices * group_rows, group_rows, 1
    )
    middle_start = device // middle_devices * middle_devices * block_rows
    middle_pos = (
        middle_start
        + middle_level_offsets[:, None]
        + DILATION_SECOND * jnp.arange(middle_key_value.shape[1], dtype=jnp.int32)[None, :]
    )
    middle_attention, middle_log_sum = attend(
        middle_level[0],
        middle_key_value[0],
        middle_key_value[1],
        middle_pos,
        valid_limit,
        head_count,
    )
    middle_output, middle_level_mass, middle_selected = scatter_rows(
        middle_attention, middle_log_sum, DILATION_SECOND, middle_level_offsets
    )
    distant_offsets = head_indices % DILATION_THIRD
    distant_local_rows = select_rows(projected_rows, DILATION_THIRD, distant_offsets)
    distant_key_value = lax.all_gather(distant_local_rows[1:], "seq", axis=1, tiled=True)
    distant_positions = (
        distant_offsets[:, None]
        + DILATION_THIRD * jnp.arange(distant_key_value.shape[1], dtype=jnp.int32)[None, :]
    )
    distant_attention, distant_log_sum = attend(
        distant_local_rows[0],
        distant_key_value[0],
        distant_key_value[1],
        distant_positions,
        valid_limit,
        head_count,
    )
    distant_output, distant_mass, distant_selected = scatter_rows(
        distant_attention, distant_log_sum, DILATION_THIRD, distant_offsets
    )
    outputs = jnp.stack([near_out, middle_output, distant_output])
    masses = jnp.stack([near_mass, middle_level_mass, distant_mass])
    selects = jnp.stack([near_sel, middle_selected, distant_selected])
    ceiling = jnp.max(masses, axis=0)
    shares = jnp.where(selects, jnp.exp(masses - ceiling), 0.0)
    combined = jnp.sum(shares[..., None] * outputs, axis=0) / jnp.sum(shares, axis=0)[..., None]
    combined = jnp.where((row_index < valid_limit)[:, None, None], combined, 0.0).reshape(
        block_rows, cols_here
    )
    row_total, row_square = lax.psum(
        (jnp.sum(combined, axis=1), jnp.sum(combined * combined, axis=1)), "head"
    )
    mean_value = row_total / DS
    mean_square = row_square / DS
    scaling = lax.rsqrt(mean_square - mean_value * mean_value + layer_eps)
    settled = ((combined - mean_value[:, None]) * scaling[:, None] * sub_gain).astype(jnp.bfloat16)
    partial_rows = jnp.dot(settled, w_out, preferred_element_type=jnp.float32)
    branch_sum = lax.psum_scatter(partial_rows, "head", scatter_dimension=1, tiled=True)
    return own_part.astype(jnp.float32) + branch_sum


MESH = pl.DeviceIdType.MESH
LANES = 128


def remote(src, dst, send_sem, recv_sem, device):
    return pltpu.make_async_remote_copy(
        src_ref=src,
        dst_ref=dst,
        send_sem=send_sem,
        recv_sem=recv_sem,
        device_id=device,
        device_id_type=MESH,
    )


def dot_rows(left, right):
    return lax.dot_general(
        left, right, (((1,), (1,)), ((), ())), preferred_element_type=jnp.float32
    )


def encode_kernel(
    tiles,
    valid_ref,
    tok_hbm,
    gain_hbm,
    scale_hbm,
    fc_hbm,
    w_hbm,
    down_hbm,
    embed_hbm,
    pre_hbm,
    wcol_hbm,
    bias_hbm,
    sub_hbm,
    order_hbm,
    slide_hbm,
    qkv_hbm,
    out_ref,
    gain_ref,
    scale_ref,
    fc_ref,
    pre_ref,
    wcol_ref,
    bias_ref,
    sub_ref,
    order_ref,
    slide_ref,
    tok_ref,
    down_ref,
    embed_ref,
    qkv_ref,
    wcol_parts,
    narrow_ref,
    pre_own,
    pre_out,
    new_out,
    wcol_out,
    sub_out,
    sequence,
    queries,
    key_rows,
    value_cols,
    fresh,
    keep_rows,
    keep_cols,
    slide_col,
    sub_col,
    mix_old,
    mix_query,
    mix_mass,
    new_kv,
    new_mix,
    normed,
    wall,
    acc,
    pool_mine,
    pooled,
    sums,
    means,
    parts,
    local_sem,
    send_tok,
    recv_tok,
    send_w,
    recv_w,
    send_pre,
    recv_pre,
    send_fan,
    recv_fan,
    send_aux,
    recv_aux,
    send_pool,
    recv_pool,
    send_mean,
    recv_mean,
    send_part,
    recv_part,
    send_new,
    recv_new,
    send_mix,
    recv_mix,
    send_kv,
    recv_kv,
):
    n = lax.axis_size("seq")
    heads = lax.axis_size("head")
    z = lax.axis_index("seq")
    hd = lax.axis_index("head")
    y = lax.axis_index("groups")
    rows, width = tok_hbm.shape
    patch = rows // tiles
    depth, hidden_width = w_hbm.shape[1:]
    quarter = rows // heads
    share = hidden_width // 4
    blocks_k = depth // LANES
    blocks_c = share // LANES
    narrow = wcol_hbm.shape[0]

    part = lax.rem(z, 2)
    pair = z // 2
    partner = z + 1 - 2 * part
    at_end = (z == 0) | (z == n - 1)
    inside = jnp.logical_not(at_end)
    inner = n - 1 - z
    outward = jnp.where(z < 2, 0, n - 1)
    toward = jnp.where(z < 2, 1, n - 1)
    across = lax.rem(hd + 2, heads)
    mate = hd + 1 - 2 * lax.rem(hd, 2)
    beyond = lax.rem(mate + 2, heads)

    def seq_peer(k):
        return lax.rem(z + k, n)

    def ahead(k):
        return lax.rem(z + k * toward, n)

    def head_peer(k):
        return lax.rem(hd + k, heads)

    def head_source(k):
        return lax.rem(hd + heads - k, heads)

    def quarter_rows(index):
        return pl.ds(pl.multiple_of(index * quarter, quarter), quarter)

    def unit(u):
        return u // blocks_c, u % blocks_c

    def weight_block(owner, u):
        r, c = unit(u)
        place = (lax.rem(owner, 2) * 2 + y) * share + c * LANES
        return w_hbm.at[
            :, pl.ds(r * LANES, LANES), pl.ds(pl.multiple_of(place, LANES), LANES)
        ]

    def wall_block(source, u):
        r, c = unit(u)
        return wall.at[r, c, :, pl.ds(pl.multiple_of(source * LANES, LANES), LANES), :]

    units = blocks_k * blocks_c
    half = quarter // 2
    first_quarters = (hd, across, mate, beyond)
    token_loads = [
        pltpu.make_async_copy(
            tok_hbm.at[quarter_rows(q)], tok_ref.at[quarter_rows(q)], local_sem.at[i]
        )
        for i, q in enumerate(first_quarters)
    ]
    loads = [
        pltpu.make_async_copy(source, target, local_sem.at[4 + i])
        for i, (source, target) in enumerate(
            ((qkv_hbm, qkv_ref), (down_hbm, down_ref), (embed_hbm, embed_ref.at[hd]))
        )
    ]
    weight_loads = [
        pltpu.make_async_copy(weight_block(z, u), wall_block(z, u), local_sem.at[7])
        for u in range(units)
    ]
    barrier = pltpu.get_barrier_semaphore()
    count = 0
    for k in range(n):
        for j in range(heads):
            if k or j:
                pl.semaphore_signal(
                    barrier,
                    inc=1,
                    device_id={"seq": seq_peer(k), "head": head_peer(j)},
                    device_id_type=MESH,
                )
                count += 1
    for k in range(n):
        pl.semaphore_signal(
            barrier, inc=1, device_id={"groups": 1 - y, "seq": seq_peer(k)}, device_id_type=MESH
        )
        count += 1
    small_loads = [
        pltpu.make_async_copy(source, target, local_sem.at[8 + i])
        for i, (source, target) in enumerate(
            (
                (pre_hbm, pre_ref),
                (gain_hbm, gain_ref),
                (scale_hbm, scale_ref),
                (fc_hbm, fc_ref),
                (wcol_hbm, wcol_ref),
                (bias_hbm, bias_ref),
                (sub_hbm, sub_ref),
                (order_hbm, order_ref),
                (slide_hbm, slide_ref),
            )
        )
    ]
    for load in token_loads[:1] + small_loads + token_loads[1:] + weight_loads + loads:
        load.start()

    block = 64

    def norm_quarter(position):
        index = first_quarters[position]
        token_loads[position].wait()

        def norm_rows(i, total):
            at = pl.ds(pl.multiple_of(index * quarter + i * block, block), block)
            values = tok_ref[at, :].astype(jnp.float32)
            out = normalize(values, gain_ref[...].reshape(1, width)).astype(jnp.bfloat16)
            normed[y * 2 + part, index, pl.ds(pl.multiple_of(i * block, block), block), :] = out
            return total + jnp.sum(values, axis=0, keepdims=True)

        sums[index] = lax.fori_loop(
            0, quarter // block, norm_rows, jnp.zeros((1, width), jnp.float32)
        )

    cols, stored_count = pre_hbm.shape
    stored_rows = stored_count + tiles
    small_loads[0].wait()
    small_loads[1].wait()
    pre_own[...] = jnp.concatenate(
        [pre_ref[...], jnp.zeros((cols, tiles), jnp.bfloat16)], axis=1
    )
    norm_quarter(0)
    pl.semaphore_wait(barrier, count)

    def send(source, target, sends, receives, device):
        remote(source, target, sends, receives, device).start()

    def send_weight(k, u):
        target = ahead(k)
        send(
            weight_block(target, u), wall_block(z, u), send_w.at[0], recv_w.at[u], {"seq": target}
        )

    own_set = y * 2 + part
    z_set = y * 2 + 1 - part
    y_set = (1 - y) * 2 + part
    d_set = (1 - y) * 2 + 1 - part

    def token_copy(which, index, event, part_of, device):
        slot = normed.at[which, index, pl.ds(part_of * half, half)]
        return remote(slot, slot, send_tok.at[0], recv_tok.at[event, part_of], device)

    def fan_copy(block_index, share_index, event, device):
        slot = pre_out.at[block_index, share_index]
        return remote(slot, slot, send_fan.at[0], recv_fan.at[event, block_index], device)

    for index in range(2):
        target = jnp.where(
            at_end,
            jnp.where(z == 0, 1 + index, n - 2 - index),
            outward if index == 0 else inner,
        )
        send(pre_own, pre_out.at[z, hd], send_pre.at[0], recv_pre.at[z], {"seq": target})
    token_copy(own_set, hd, 0, 0, {"seq": partner}).start()
    for part_of in range(2):
        token_copy(own_set, hd, 4, part_of, {"groups": 1 - y}).start()

    @pl.when(at_end)
    def _():
        token_copy(own_set, hd, 0, 1, {"seq": partner}).start()

    @pl.when(at_end)
    def _():
        for u in range(units):
            send_weight(2, u)
        for u in range(units):
            send_weight(1, u)
            send_weight(3, u)

    @pl.when(inside)
    def _():
        for u in range(units):
            send_weight(1, u)

    cols_half = cols // 2

    def embed_half(owner, which):
        return embed_ref.at[
            owner, pl.ds(pl.multiple_of(which * cols_half, cols_half), cols_half)
        ]

    def embed_copy(owner, which, event, device):
        slot = embed_half(owner, which)
        return remote(slot, slot, send_new.at[1], recv_new.at[event], device)

    loads[2].wait()
    own_embed = embed_ref.at[hd]
    send(own_embed, own_embed, send_new.at[0], recv_new.at[0], {"head": mate})
    embed_copy(hd, y, 1, {"head": across}).start()
    pre_out[z, hd] = pre_own[...]
    norm_quarter(1)

    def fan_first(b):
        fan_copy(b, hd, 0, {"head": across}).start()
        fan_copy(b, hd, 1, {"head": mate}).start()

    def fan_second(b):
        fan_copy(b, across, 0, {"head": across}).wait_recv()
        fan_copy(b, across, 2, {"head": mate}).start()

    def stored_block(b, forward=False):
        slot = pre_out.at[b, hd]
        remote(slot, slot, send_pre.at[0], recv_pre.at[b], {"seq": partner}).wait_recv()
        if forward:
            send(slot, slot, send_pre.at[1], recv_pre.at[b], {"seq": outward})
        fan_first(b)

    fan_first(z)
    second_end = jnp.where(z == 0, 2, n - 3)

    @pl.when(at_end)
    def _():
        stored_block(partner)

    @pl.when(inside)
    def _():
        stored_block(inner, True)
        token_copy(own_set, hd, 0, 1, {"seq": partner}).start()
        stored_block(outward)

    norm_quarter(2)
    norm_quarter(3)
    for tile in range(tiles):
        per = heads // tiles
        means[z, pl.ds(tile, 1), :] = (
            sum(sums[tile * per + i] for i in range(per)) / patch
        )
    for k in range(1, n):
        send(means.at[z], means.at[z], send_mean.at[0], recv_mean.at[0], {"seq": seq_peer(k)})
    for load in small_loads[2:]:
        load.wait()
    narrow_ref[pl.ds(0, 1), :] = bias_ref[...].reshape(1, narrow)
    narrow_ref[pl.ds(1, 1), :] = sub_ref[...].reshape(1, narrow)
    for j in range(heads):
        wcol_parts[j] = wcol_ref[:, j * narrow : (j + 1) * narrow].T
    wcol_out[hd] = wcol_parts[hd]
    sub_out[hd] = narrow_ref[...]

    def column(row):
        size = row.shape[1]
        same = lax.broadcasted_iota(jnp.int32, (size, size), 0) == lax.broadcasted_iota(
            jnp.int32, (size, size), 1
        )
        return jnp.sum(jnp.where(same, row, 0.0), axis=1, keepdims=True)

    features = heads * cols
    for start in range(0, features, LANES):
        at = pl.ds(start, LANES)
        slide_col[at, :] = column(slide_ref[...].reshape(1, features)[:, start : start + LANES])

    def token_event(which, index, event, part_of, forwards):
        token_copy(which, index, event, part_of, {"head": mate}).wait_recv()
        for to, device in forwards:
            token_copy(which, index, to, part_of, device).start()

    from_z = ((8, {"groups": 1 - y}), (1, {"head": across}), (2, {"head": mate}))
    token_event(y_set, hd, 4, 0, ((6, {"head": mate}),))

    @pl.when(inside)
    def _():
        stored_block(n - 1 - outward, True)

    token_event(z_set, hd, 0, 0, from_z)
    token_event(y_set, hd, 4, 1, ((6, {"head": mate}),))

    @pl.when(at_end)
    def _():
        stored_block(second_end)

    token_event(z_set, hd, 0, 1, (from_z[0], from_z[2]))
    for part_of in range(2):
        token_copy(own_set, across, 5, part_of, {"groups": 1 - y}).start()

    @pl.when(at_end)
    def _():
        stored_block(n - 1 - z)

    @pl.when(inside)
    def _():
        for u in range(units):
            send_weight(3, u)

    fan_second(z)

    @pl.when(at_end)
    def _():
        fan_second(partner)
        fan_second(second_end)

    @pl.when(inside)
    def _():
        fan_second(inner)
        fan_second(outward)
        for u in range(units):
            send_weight(2, u)

    token_copy(z_set, hd, 1, 1, {"head": across}).start()
    for part_of in range(2):
        token_event(d_set, hd, 8, part_of, ((9, {"head": across}), (10, {"head": mate})))
    fan_second(jnp.where(at_end, n - 1 - z, n - 1 - outward))
    step = stored_rows
    total_rows = n * step
    limit = valid_ref[0]
    new_count = n * tiles
    factor = 1.0 / math.sqrt(HEAD_DIM)
    head_count = cols // HEAD_DIM

    def multiplicity(first, second, offset):
        middle = (first % DILATION_SECOND == offset % DILATION_SECOND) & (
            second % DILATION_SECOND == offset % DILATION_SECOND
        )
        distant = (first % DILATION_THIRD == offset % DILATION_THIRD) & (
            second % DILATION_THIRD == offset % DILATION_THIRD
        )
        return 1.0 + jnp.where(middle, 1.0, 0.0) + jnp.where(distant, 1.0, 0.0)

    def sequence_step(t):
        at = pl.ds(t * step, step)
        per = step // LANES
        order = jnp.concatenate([order_ref[pl.ds(t * per + i, 1), :] for i in range(per)], axis=1)
        label = lax.broadcasted_iota(jnp.int32, (step, step), 0)
        label = jnp.where(label < stored_count, label + tiles, -n * step)
        picks = jnp.concatenate(
            [jnp.where(order == label + b * step, 1.0, 0.0).astype(jnp.bfloat16) for b in range(n)],
            axis=0,
        )
        label = lax.broadcasted_iota(jnp.int32, (LANES, step), 0)
        wanted = jnp.where(label < new_count, label // tiles * step + label % tiles, -1)
        found = jnp.where(order == wanted, 1.0, 0.0)
        fresh[t] = found.astype(jnp.bfloat16)
        lane = lax.broadcasted_iota(jnp.int32, (1, step), 1) + t * step
        keep_cols[:, t * step : (t + 1) * step] = jnp.where(
            lane < limit, 1.0 - jnp.sum(found, axis=0, keepdims=True), 0.0
        )
        row = lax.broadcasted_iota(jnp.int32, (step, 1), 0) + t * step
        keep_rows[at, :] = jnp.where(
            row < limit, 1.0 - jnp.sum(found.T, axis=1, keepdims=True), 0.0
        )
        stored = jnp.concatenate(
            [jnp.concatenate([pre_out[b, j] for b in range(n)], axis=1) for j in range(heads)],
            axis=0,
        )
        values = jnp.dot(stored, picks, preferred_element_type=jnp.float32)
        sequence[t] = values.astype(jnp.bfloat16).reshape(heads, cols, step)
        centered = values - jnp.sum(values, axis=0, keepdims=True) / features
        variance = jnp.sum(centered * centered, axis=0, keepdims=True) / features
        normal = (centered * lax.rsqrt(variance + layer_eps) * slide_col[...]).astype(jnp.bfloat16)
        result = jnp.dot(
            qkv_ref[...].reshape(3 * cols, features), normal, preferred_element_type=jnp.float32
        ).astype(jnp.bfloat16)
        queries[t] = result[:cols]
        key_rows[at, :] = result[cols : 2 * cols].T
        value_cols[:, t * step : (t + 1) * step] = result[2 * cols :]

    def attend_stored():
        query = queries[z]
        row_head = lax.broadcasted_iota(jnp.int32, (cols, 1), 0) // HEAD_DIM
        key_at = lax.broadcasted_iota(jnp.int32, (total_rows, 1), 0)
        query_at = lax.broadcasted_iota(jnp.int32, (1, step), 1) + z * step
        for h in range(head_count):
            own = jnp.where(row_head == h, query, jnp.zeros((), jnp.bfloat16))
            scores = jnp.dot(key_rows[...], own, preferred_element_type=jnp.float32) * factor
            scores = jnp.where(keep_rows[...] > 0.0, scores, masked_score)
            peak = jnp.max(scores, axis=0, keepdims=True)
            weights = jnp.exp(scores - peak) * multiplicity(
                key_at, query_at, hd * head_count + h
            )
            at = slice(h * HEAD_DIM, (h + 1) * HEAD_DIM)
            values = jnp.concatenate(
                [value_cols[at, :], jnp.ones((16, total_rows), jnp.bfloat16)], axis=0
            )
            total = jnp.dot(
                values, weights.astype(jnp.bfloat16), preferred_element_type=jnp.float32
            )
            mass = total[HEAD_DIM : HEAD_DIM + 1]
            mix_old[hd, at, :] = (total[:HEAD_DIM] / mass).astype(jnp.bfloat16)
            mix_mass[hd, h * 8 : (h + 1) * 8, :] = jnp.broadcast_to(peak + jnp.log(mass), (8, step))
        mix_query[hd] = query
        for k in range(1, heads):
            for index, buffer in enumerate((mix_query, mix_mass, mix_old)):
                send(
                    buffer.at[hd],
                    buffer.at[hd],
                    send_mix.at[index],
                    recv_mix.at[index],
                    {"head": head_peer(k)},
                )

    loads[0].wait()
    for b in range(n):
        for event, source in ((1, mate), (2, beyond)):
            fan_copy(b, source, event, {"head": mate}).wait_recv()
    for t in range(n):
        sequence_step(t)
        if t == 1:
            embed_copy(across, y, 1, {"head": across}).wait_recv()
            embed_copy(across, y, 2, {"groups": 1 - y}).start()
            embed_copy(across, y, 3, {"head": mate}).start()
        if t in (0, n - 2):
            which, index, event = (z_set, across, 1) if t == 0 else (y_set, across, 5)
            for part_of in range(2):
                token_event(which, index, event, part_of, ((event + 2, {"head": mate}),))
    attend_stored()
    for k in range(1, heads):
        send(
            wcol_parts.at[head_peer(k)],
            wcol_out.at[hd],
            send_aux.at[0],
            recv_aux.at[0],
            {"head": head_peer(k)},
        )
        send(narrow_ref, sub_out.at[hd], send_aux.at[1], recv_aux.at[1], {"head": head_peer(k)})
    for part_of in range(2):
        token_event(d_set, across, 9, part_of, ((11, {"head": mate}),))
    embed_copy(across, 1 - y, 2, {"groups": 1 - y}).wait_recv()
    embed_copy(across, 1 - y, 4, {"head": mate}).start()
    for which, first in ((z_set, 0), (y_set, 4), (d_set, 8)):
        for part_of in range(2):
            token_event(which, mate, first + 2, part_of, ())
            token_event(which, beyond, first + 3, part_of, ())

    whole = wall.at[:, :, :, pl.ds(0, LANES), :]
    pltpu.make_async_copy(whole, whole, local_sem.at[7]).wait()

    def arrived(u):
        r, c = unit(u)
        others = wall.at[r, c, :, pl.ds(0, (n - 1) * LANES), :]
        remote(others, others, send_w.at[0], recv_w.at[u], {"seq": partner}).wait_recv()

    def gathered(r, chosen):
        return jnp.concatenate([wall[r, c, g] for c in chosen for g in range(2)], axis=1)

    def token_block(s, r):
        return jnp.concatenate(
            [
                normed[s, :, :, b * depth + r * LANES : b * depth + (r + 1) * LANES].reshape(
                    rows, LANES
                )
                for b in range(n)
            ],
            axis=1,
        )

    def multiply(r):
        for c in range(blocks_c):
            arrived(r * blocks_c + c)
        w = gathered(r, range(blocks_c))

        @pl.loop(0, 4)
        def _(s):
            value = jnp.dot(token_block(s, r), w, preferred_element_type=jnp.float32)
            if r == 0:
                acc[s] = value
            else:
                acc[s] += value

    def pool(c):
        r = blocks_k - 1
        arrived(r * blocks_c + c)
        w = gathered(r, (c,))

        @pl.loop(0, 4)
        def _(s):
            value = acc[s, :, 2 * c * LANES : 2 * (c + 1) * LANES] + jnp.dot(
                token_block(s, r), w, preferred_element_type=jnp.float32
            )
            gate = value[:, :LANES]
            hidden = (gate / (1.0 + jnp.exp(-gate)) * value[:, LANES:]).astype(jnp.bfloat16)
            hidden = hidden.astype(jnp.float32)
            for tile in range(tiles):
                pool_mine[s // 2, c, pl.ds(s % 2 * tiles + tile, 1), :] = (
                    jnp.sum(hidden[tile * patch : (tile + 1) * patch], axis=0, keepdims=True)
                    / patch
                )

        place = y * n + z
        pooled[place, c] = pool_mine[y, c]
        for k in range(n):
            for other in range(2):
                if k or other:
                    yy = 1 - y if other else y
                    send(
                        pool_mine.at[yy, c],
                        pooled.at[place, c],
                        send_pool.at[c],
                        recv_pool.at[c],
                        {"groups": yy, "seq": seq_peer(k)},
                    )

    for r in range(blocks_k - 1):
        multiply(r)
    for c in range(blocks_c):
        pool(c)

    seen = means.at[pl.ds(0, n - 1)]
    remote(seen, seen, send_mean.at[0], recv_mean.at[0], {"seq": partner}).wait_recv()
    for c in range(blocks_c):
        slot = pooled.at[pl.ds(0, 2 * n - 1), c]
        remote(slot, slot, send_pool.at[c], recv_pool.at[c], {"seq": partner}).wait_recv()
    loads[1].wait()
    everyone = jnp.concatenate(
        [
            jnp.concatenate(
                [
                    pooled[yy * n + b + m, c]
                    for m in range(2)
                    for yy in range(2)
                    for c in range(blocks_c)
                ],
                axis=1,
            )
            for b in range(0, n, 2)
        ],
        axis=0,
    )
    high = everyone.astype(jnp.bfloat16)
    rest = everyone - high.astype(jnp.float32)
    middle = rest.astype(jnp.bfloat16)
    low = (rest - middle.astype(jnp.float32)).astype(jnp.bfloat16)
    local_part = jnp.zeros((n * tiles, down_ref.shape[1]), jnp.float32)
    for piece in (low, middle, high):
        local_part += jnp.dot(piece, down_ref[...], preferred_element_type=jnp.float32)
    here = z * heads + hd
    parts[here] = local_part.astype(jnp.bfloat16)
    for k in range(n):
        for j in range(heads):
            if k or j:
                send(
                    parts.at[here],
                    parts.at[here],
                    send_part.at[0],
                    recv_part.at[0],
                    {"seq": seq_peer(k), "head": head_peer(j)},
                )
    for buffer, receives in ((wcol_out, recv_aux.at[0]), (sub_out, recv_aux.at[1])):
        slot = buffer.at[pl.ds(0, heads - 1)]
        remote(slot, slot, send_aux.at[0], receives, {"head": mate}).wait_recv()
    for j in range(heads):
        sub_col[pl.ds(j * cols, cols), :] = column(sub_out[j, 1:2])
    slot = parts.at[pl.ds(0, n * heads - 1)]
    remote(slot, slot, send_part.at[0], recv_part.at[0], {"seq": partner}).wait_recv()
    remote(own_embed, own_embed, send_new.at[0], recv_new.at[0], {"head": mate}).wait_recv()
    for which, event in ((y, 3), (1 - y, 4)):
        embed_copy(beyond, which, event, {"head": mate}).wait_recv()
    summed = jnp.concatenate(
        [
            sum(parts[b * heads + j].astype(jnp.float32) for j in range(heads))
            for b in range(n)
        ],
        axis=1,
    )
    average = jnp.concatenate([means[b] for b in range(n)], axis=0)
    feature = normalize(
        average + scale_ref[...].reshape(1, width) * summed, fc_ref[...].reshape(1, width)
    ).astype(jnp.bfloat16)
    table = embed_ref[...].reshape(heads * cols, width)
    shift = jnp.concatenate([sub_out[j, 0:1] for j in range(heads)], axis=1)
    fresh_values = (dot_rows(feature, table) + shift).astype(jnp.bfloat16)
    for j in range(heads):
        new_out[j] = fresh_values[:, j * cols : (j + 1) * cols]
    fresh_values = fresh_values.astype(jnp.float32)

    def peers(buffer, receives):
        slot = buffer.at[pl.ds(0, heads - 1)]
        remote(slot, slot, send_aux.at[0], receives, {"head": mate}).wait_recv()

    normal = normalize(fresh_values, slide_ref[...].reshape(1, features)).astype(jnp.bfloat16)
    new_query, new_key, new_value = [
        dot_rows(normal, qkv_ref[g]).astype(jnp.bfloat16) for g in range(3)
    ]
    new_kv[hd, 0] = new_key
    new_kv[hd, 1] = new_value
    for k in range(1, heads):
        send(new_kv.at[hd], new_kv.at[hd], send_kv.at[0], recv_kv.at[0], {"head": head_peer(k)})
    lane_head = lax.broadcasted_iota(jnp.int32, (1, cols), 1) // HEAD_DIM
    nothing = jnp.zeros((), jnp.bfloat16)

    def by_head(rows_in):
        return jnp.concatenate(
            [jnp.where(lane_head == h, rows_in, nothing) for h in range(head_count)], axis=0
        )

    key_at = lax.broadcasted_iota(jnp.int32, (new_count, total_rows), 1)
    placed = jnp.concatenate([fresh[t, :new_count].astype(jnp.float32) for t in range(n)], axis=1)
    new_at = jnp.sum(placed * key_at.astype(jnp.float32), axis=1, keepdims=True).astype(jnp.int32)
    other = lax.broadcasted_iota(jnp.int32, (1, LANES), 1)
    new_lane = jnp.sum(
        jnp.where(other == lax.broadcasted_iota(jnp.int32, (new_count, LANES), 0), new_at, 0),
        axis=0,
        keepdims=True,
    )[:, :new_count]

    many = by_head(new_query)
    scores = dot_rows(many, key_rows[...]) * factor
    scores = jnp.where(keep_cols[...] > 0.0, scores, masked_score)
    recent = dot_rows(many, new_key) * factor
    recent = jnp.where(new_lane < limit, recent, masked_score)
    peak = jnp.maximum(
        jnp.max(scores, axis=1, keepdims=True), jnp.max(recent, axis=1, keepdims=True)
    )
    row_at = jnp.concatenate([new_at] * head_count, axis=0)
    offset = hd * head_count + lax.broadcasted_iota(
        jnp.int32, (head_count * new_count, 1), 0
    ) // new_count
    weights = jnp.exp(scores - peak) * multiplicity(key_at[:1], row_at, offset)
    recent = jnp.exp(recent - peak) * multiplicity(new_lane, row_at, offset)
    mass = jnp.sum(weights, axis=1, keepdims=True) + jnp.sum(recent, axis=1, keepdims=True)
    attended = (
        dot_rows(weights.astype(jnp.bfloat16), value_cols[...])
        + jnp.dot(recent.astype(jnp.bfloat16), new_value, preferred_element_type=jnp.float32)
    ) / mass
    new_mix[hd] = sum(
        jnp.where(lane_head == h, attended[h * new_count : (h + 1) * new_count], 0.0)
        for h in range(head_count)
    ).astype(jnp.bfloat16)
    for k in range(1, heads):
        send(new_mix.at[hd], new_mix.at[hd], send_kv.at[1], recv_kv.at[1], {"head": head_peer(k)})

    for index, buffer in enumerate((mix_query, mix_mass, mix_old)):
        peers(buffer, recv_mix.at[index])
    peers(new_kv, recv_kv.at[0])
    query_at = lax.broadcasted_iota(jnp.int32, (1, step), 1) + z * step
    here_fresh = fresh[z, :new_count]
    known = 1.0 - jnp.sum(here_fresh.astype(jnp.float32), axis=0, keepdims=True)
    known = jnp.where(query_at < limit, known, 0.0)
    betas, alphas = [], []
    for j in range(heads):
        scores = (
            jnp.dot(by_head(new_kv[j, 0]), mix_query[j], preferred_element_type=jnp.float32)
            * factor
        )
        scores = jnp.where(row_at < limit, scores, masked_score)
        offset = j * head_count + lax.broadcasted_iota(
            jnp.int32, (head_count * new_count, 1), 0
        ) // new_count
        grouped = (head_count, new_count, step)
        scores = scores.reshape(grouped)
        stored_mass = mix_mass[j].reshape(grouped)
        ceiling = jnp.maximum(jnp.max(scores, axis=1, keepdims=True), stored_mass)
        weights = jnp.exp(scores - ceiling) * multiplicity(row_at, query_at, offset).reshape(grouped)
        old = jnp.exp(stored_mass - ceiling)
        inverse = known / (old + jnp.sum(weights, axis=1, keepdims=True))
        betas.append((weights * inverse).reshape(head_count * new_count, step))
        alphas.append(old * inverse)

    peers(new_mix, recv_kv.at[1])
    inside_limit = jnp.where(query_at < limit, here_fresh.astype(jnp.float32), 0.0)

    def contract(left, right):
        return lax.dot_general(
            left, right, (((0,), (0,)), ((), ())), preferred_element_type=jnp.float32
        )

    pieces = []
    for j in range(heads):
        left = jnp.concatenate([by_head(new_kv[j, 1]), new_mix[j]], axis=0)
        right = jnp.concatenate([betas[j], inside_limit], axis=0).astype(jnp.bfloat16)
        share_of = jnp.concatenate(
            [
                mix_old[j, h * HEAD_DIM : (h + 1) * HEAD_DIM, :].astype(jnp.float32)
                * alphas[j][h, :1]
                for h in range(head_count)
            ],
            axis=0,
        )
        pieces.append(share_of + contract(left, right))
    mean = sum(jnp.sum(p, axis=0, keepdims=True) for p in pieces) / features
    square = sum(jnp.sum(p * p, axis=0, keepdims=True) for p in pieces) / features
    scaling = lax.rsqrt(square - mean * mean + layer_eps)
    branch = sequence[z, hd].astype(jnp.float32) + contract(new_out[hd], here_fresh)
    for j in range(heads):
        gain = sub_col[pl.ds(j * cols, cols), :]
        settled = ((pieces[j] - mean) * scaling * gain).astype(jnp.bfloat16)
        branch += jnp.dot(wcol_out[j], settled, preferred_element_type=jnp.float32)
    out_ref[...] = branch

    def drain(slot, sends):
        remote(slot, slot, sends, recv_new.at[0], {"head": mate}).wait_send()

    drain(normed.at[pl.ds(0, 3)], send_tok.at[0])
    drain(wall.at[:, :, :, pl.ds(0, (n - 1) * LANES), :], send_w.at[0])
    drain(pre_out.at[0, pl.ds(0, 2)], send_pre.at[0])

    @pl.when(inside)
    def _():
        drain(pre_out.at[0, pl.ds(0, 2)], send_pre.at[1])

    drain(pre_out.at[pl.ds(0, 3)], send_fan.at[0])
    drain(wcol_out.at[pl.ds(0, heads - 1)], send_aux.at[0])
    drain(sub_out.at[pl.ds(0, heads - 1)], send_aux.at[1])
    for c in range(blocks_c):
        drain(pooled.at[pl.ds(0, 2 * n - 1), c], send_pool.at[c])
    drain(means.at[pl.ds(0, n - 1)], send_mean.at[0])
    drain(parts.at[pl.ds(0, n * heads - 1)], send_part.at[0])
    drain(own_embed, send_new.at[0])
    drain(embed_ref.at[pl.ds(0, 2)], send_new.at[1])
    for index, buffer in enumerate((mix_query, mix_mass, mix_old)):
        drain(buffer.at[pl.ds(0, heads - 1)], send_mix.at[index])
    drain(new_kv.at[pl.ds(0, heads - 1)], send_kv.at[0])
    drain(new_mix.at[pl.ds(0, heads - 1)], send_kv.at[1])


def near_body(
    tile_tokens,
    tile_gain,
    w_gate_up,
    w_down,
    layer_scale,
    fc_gain,
    w_embed,
    embed_bias,
    pre_emb,
    tile_order,
    valid_count,
    slide_gain,
    w_qkv,
    sub_gain,
    w_out,
):
    n = lax.axis_size("seq")
    heads = lax.axis_size("head")
    tiles, patch, width = tile_tokens.shape
    depth, hidden_width = w_gate_up.shape[1:]
    rows = tiles * patch
    cols = w_embed.shape[1]
    head_count = cols // HEAD_DIM
    total_rows = tile_order.shape[0]
    block_rows = total_rows // n
    vmem = pl.BlockSpec(memory_space=pltpu.VMEM)
    anywhere = pl.BlockSpec(memory_space=pl.ANY)
    dma = pltpu.SemaphoreType.DMA
    f32, bf16 = jnp.float32, jnp.bfloat16
    quarter = rows // heads
    blocks_k = depth // LANES
    blocks_c = hidden_width // 4 // LANES
    out = pl.pallas_call(
        functools.partial(encode_kernel, tiles),
        out_shape=pltpu.VMEM((cols, block_rows), f32),
        in_specs=[pl.BlockSpec(memory_space=pltpu.SMEM)] + [anywhere] * 14,
        out_specs=vmem,
        scratch_shapes=[
            pltpu.VMEM((width,), f32),
            pltpu.VMEM((width,), f32),
            pltpu.VMEM((width,), f32),
            pltpu.VMEM((cols, block_rows - tiles), bf16),
            pltpu.VMEM((cols, heads * cols), bf16),
            pltpu.VMEM((cols,), f32),
            pltpu.VMEM((cols,), f32),
            pltpu.VMEM((total_rows // LANES, LANES), jnp.int32),
            pltpu.VMEM((heads * cols,), f32),
            pltpu.VMEM((rows, width), bf16),
            pltpu.VMEM(w_down.shape, bf16),
            pltpu.VMEM((heads, cols, width), bf16),
            pltpu.VMEM((3, cols, heads * cols), bf16),
            pltpu.VMEM((heads, cols, cols), bf16),
            pltpu.VMEM((2, cols), f32),
            pltpu.VMEM((cols, block_rows), bf16),
            pltpu.VMEM((n, heads, cols, block_rows), bf16),
            pltpu.VMEM((heads, n * tiles, cols), bf16),
            pltpu.VMEM((heads, cols, cols), bf16),
            pltpu.VMEM((heads, 2, cols), f32),
            pltpu.VMEM((n, heads, cols, block_rows), bf16),
            pltpu.VMEM((n, cols, block_rows), bf16),
            pltpu.VMEM((total_rows, cols), bf16),
            pltpu.VMEM((cols, total_rows), bf16),
            pltpu.VMEM((n, LANES, block_rows), bf16),
            pltpu.VMEM((total_rows, 1), f32),
            pltpu.VMEM((1, total_rows), f32),
            pltpu.VMEM((heads * cols, 1), f32),
            pltpu.VMEM((heads * cols, 1), f32),
            pltpu.VMEM((heads, cols, block_rows), bf16),
            pltpu.VMEM((heads, cols, block_rows), bf16),
            pltpu.VMEM((heads, head_count * 8, block_rows), f32),
            pltpu.VMEM((heads, 2, n * tiles, cols), bf16),
            pltpu.VMEM((heads, n * tiles, cols), bf16),
            pltpu.VMEM((4, heads, quarter, width), bf16),
            pltpu.VMEM((blocks_k, blocks_c, 2, n * LANES, LANES), bf16),
            pltpu.VMEM((4, rows, blocks_c * 2 * LANES), f32),
            pltpu.VMEM((2, blocks_c, 2 * tiles, LANES), f32),
            pltpu.VMEM((2 * n, blocks_c, 2 * tiles, LANES), f32),
            pltpu.VMEM((heads, 1, width), f32),
            pltpu.VMEM((n, tiles, width), f32),
            pltpu.VMEM((n * heads, n * tiles, w_down.shape[1]), bf16),
            dma((17,)),
            dma((1,)),
            dma((12, 2)),
            dma((1,)),
            dma((blocks_k * blocks_c,)),
            dma((2,)),
            dma((n,)),
            dma((1,)),
            dma((3, n)),
            dma((2,)),
            dma((2,)),
            dma((blocks_c,)),
            dma((blocks_c,)),
            dma((1,)),
            dma((1,)),
            dma((1,)),
            dma((1,)),
            dma((2,)),
            dma((5,)),
            dma((3,)),
            dma((3,)),
            dma((2,)),
            dma((2,)),
        ],
        compiler_params=pltpu.CompilerParams(
            collective_id=0, has_side_effects=True, vmem_limit_bytes=58 * 1024 * 1024
        ),
    )(
        valid_count,
        tile_tokens.reshape(rows, width),
        tile_gain,
        layer_scale,
        fc_gain,
        w_gate_up,
        w_down,
        w_embed.T,
        pre_emb.T,
        w_out,
        embed_bias,
        sub_gain,
        tile_order.reshape(total_rows // LANES, LANES),
        slide_gain,
        w_qkv.swapaxes(1, 2),
    )
    return out.T


def body(*args):
    total_rows = args[9].shape[0]
    mesh_fits = all(lax.axis_size(a) == k for a, k in (("groups", 2), ("seq", 4), ("head", 4)))
    if total_rows <= SPAN0 and mesh_fits:
        return near_body(*args)
    return general_body(*args)


def solution(mesh):
    placed = (
        P(("groups", "seq"), None, None),
        P(),
        P(None, "seq", "head"),
        P("head", "seq"),
        P(),
        P(),
        P(None, "head"),
        P("head"),
        P(("groups", "seq"), "head"),
        P("groups"),
        P("groups"),
        P(),
        P(None, None, "head"),
        P("head"),
        P("head", None),
    )
    return jax.shard_map(
        body, mesh=mesh, in_specs=placed, out_specs=P(("groups", "seq"), "head"), check_vma=False
    )
```

```python
import functools
import math

import jax
import jax.numpy as jnp
from jax import lax
from jax.experimental import pallas as pl
from jax.experimental.pallas import tpu as pltpu
from jax.sharding import PartitionSpec as P

DS = 768
HEAD_DIM = 48
SPAN0 = 1024
SPAN1 = 4096
DILATION_SECOND = 4
DILATION_THIRD = 16


layer_eps = 1e-05
masked_score = -1e30


def from_partner(value, axis, bit):
    mask = 2**bit
    pairs = [(source, source ^ mask) for source in range(lax.axis_size(axis))]
    return lax.ppermute(value, axis, pairs)


def normalize(values, gain):
    centered = values - jnp.mean(values, axis=-1, keepdims=True)
    variance = jnp.mean(centered * centered, axis=-1, keepdims=True)
    return centered * lax.rsqrt(variance + layer_eps) * gain


def select_rows(stacked, dilation, offsets):
    group_count, row_count, row_width = stacked.shape
    head_count = offsets.shape[0]
    arranged = stacked.reshape(
        group_count, row_count // dilation, dilation, head_count, row_width // head_count
    )
    choose = jnp.arange(dilation, dtype=jnp.int32)[:, None] == offsets[None, :]
    chosen = jnp.sum(
        jnp.where(choose[None, None, :, :, None], arranged, jnp.zeros((), stacked.dtype)), axis=2
    )
    return chosen.reshape(group_count, row_count // dilation, row_width)


def scatter_rows(attended, log_mass, dilation, offsets):
    query_count, head_count, head_size = attended.shape
    choose = jnp.arange(dilation, dtype=jnp.int32)[:, None] == offsets[None, :]
    spread_out = jnp.where(choose[None, :, :, None], attended[:, None, :, :], 0.0).reshape(
        query_count * dilation, head_count, head_size
    )
    spread_mass = jnp.where(choose[None, :, :], log_mass[:, None, :], masked_score).reshape(
        query_count * dilation, head_count
    )
    selected = jnp.broadcast_to(choose[None, :, :], (query_count, dilation, head_count)).reshape(
        query_count * dilation, head_count
    )
    return (spread_out, spread_mass, selected)


def attend(query_rows, key_rows, value_rows, positions, valid_limit, head_count):
    head_size = query_rows.shape[1] // head_count
    query_heads = query_rows.reshape(query_rows.shape[0], head_count, head_size)
    key_heads = key_rows.reshape(key_rows.shape[0], head_count, head_size)
    value_heads = value_rows.reshape(value_rows.shape[0], head_count, head_size)
    scores = jnp.einsum(
        "qhe,khe->hqk", query_heads, key_heads, preferred_element_type=jnp.float32
    ) / math.sqrt(head_size)
    scores = jnp.where((positions < valid_limit)[:, None, :], scores, masked_score)
    highest = jnp.max(scores, axis=-1, keepdims=True)
    exponent = jnp.exp(scores - highest)
    mass_sum = jnp.sum(exponent, axis=-1, keepdims=True)
    weights = (exponent / mass_sum).astype(jnp.bfloat16)
    attended = jnp.einsum("hqk,khe->qhe", weights, value_heads, preferred_element_type=jnp.float32)
    return (attended, (highest[..., 0] + jnp.log(mass_sum[..., 0])).T)


def general_body(
    tile_tokens,
    tile_gain,
    w_gate_up,
    w_down,
    layer_scale,
    fc_gain,
    w_embed,
    embed_bias,
    pre_emb,
    tile_order,
    valid_count,
    slide_gain,
    w_qkv,
    sub_gain,
    w_out,
):
    new_count, patch_count, tile_width = tile_tokens.shape
    token_rows = tile_tokens.reshape(new_count * patch_count, tile_width)
    normed = normalize(token_rows.astype(jnp.float32), tile_gain).astype(jnp.bfloat16)
    hidden_width = w_gate_up.shape[2]
    gate_up = jnp.einsum(
        "rk,gkf->grf",
        normed,
        lax.all_gather(w_gate_up, "seq", axis=1, tiled=True),
        preferred_element_type=jnp.float32,
    )
    hidden = (jax.nn.silu(gate_up[0]) * gate_up[1]).astype(jnp.bfloat16)
    pooled_hidden = jnp.mean(
        hidden.reshape(new_count, patch_count, hidden_width), axis=1, dtype=jnp.float32
    )
    everyone = lax.all_gather(pooled_hidden, "seq", axis=0, tiled=True)
    local_part = jnp.dot(everyone, w_down.astype(jnp.float32), precision=lax.Precision.HIGHEST)
    pooled_part = lax.all_to_all(local_part, "seq", split_axis=0, concat_axis=1, tiled=True)
    summed = lax.psum(pooled_part, "head")
    pooled = jnp.mean(tile_tokens, axis=1, dtype=jnp.float32) + layer_scale * summed
    feature = normalize(pooled, fc_gain).astype(jnp.bfloat16)
    new_rows = (jnp.dot(feature, w_embed, preferred_element_type=jnp.float32) + embed_bias).astype(
        jnp.bfloat16
    )
    stored = jnp.concatenate([new_rows, pre_emb], axis=0)
    block_rows = stored.shape[0]
    total_rows = tile_order.shape[0]
    peer_rows = block_rows // lax.axis_size("seq")
    device = lax.axis_index("seq")
    local_index = jnp.arange(block_rows, dtype=jnp.int32)
    inverse = (
        jnp.zeros((total_rows,), jnp.int32)
        .at[tile_order]
        .set(jnp.arange(total_rows, dtype=jnp.int32))
    )
    placed = lax.dynamic_slice_in_dim(inverse, device * block_rows, block_rows)
    target = placed // block_rows
    before = (target[:, None] == target[None, :]) & (placed[None, :] < placed[:, None])
    slot_index = target * peer_rows + jnp.sum(before, axis=1, dtype=jnp.int32)
    routing = (slot_index[None, :] == local_index[:, None]).astype(jnp.bfloat16)
    outgoing = jnp.dot(routing, stored, preferred_element_type=jnp.float32).astype(jnp.bfloat16)
    incoming = lax.all_to_all(outgoing, "seq", split_axis=0, concat_axis=0, tiled=True)
    wanted = lax.dynamic_slice_in_dim(tile_order, device * block_rows, block_rows)
    source = wanted // block_rows
    earlier = (source[:, None] == source[None, :]) & (local_index[None, :] < local_index[:, None])
    arrival = source * peer_rows + jnp.sum(earlier, axis=1, dtype=jnp.int32)
    own_part = jnp.take(incoming, arrival, axis=0)
    sequence = lax.all_gather(own_part, "head", axis=1, tiled=True)
    slide_normed = normalize(sequence.astype(jnp.float32), slide_gain).astype(jnp.bfloat16)
    projected_rows = jnp.einsum(
        "rd,gdc->grc", slide_normed, w_qkv, preferred_element_type=jnp.float32
    ).astype(jnp.bfloat16)
    cols_here = projected_rows.shape[2]
    head_count = cols_here // HEAD_DIM
    head_indices = lax.axis_index("head") * head_count + jnp.arange(head_count, dtype=jnp.int32)
    valid_limit = valid_count[0]
    row_index = device * block_rows + local_index
    near_devices = min(SPAN0, total_rows) // block_rows
    near_rows = projected_rows[1:]
    for bit_index in range(near_devices.bit_length() - 1):
        partner = from_partner(near_rows, "seq", bit_index)
        upper_half = device // (1 << bit_index) % 2 == 1
        near_rows = jnp.where(
            upper_half,
            jnp.concatenate([partner, near_rows], 1),
            jnp.concatenate([near_rows, partner], 1),
        )
    near_start = device // near_devices * near_devices * block_rows
    near_pos = jnp.broadcast_to(
        near_start + jnp.arange(near_rows.shape[1], dtype=jnp.int32),
        (head_count, near_rows.shape[1]),
    )
    near_out, near_mass = attend(
        projected_rows[0], near_rows[0], near_rows[1], near_pos, valid_limit, head_count
    )
    near_sel = jnp.ones((block_rows, head_count), dtype=bool)
    middle_level_offsets = head_indices % DILATION_SECOND
    middle_level = select_rows(projected_rows, DILATION_SECOND, middle_level_offsets)
    middle_devices = min(SPAN1, total_rows) // block_rows
    middle_key_value = middle_level[1:]
    every_row = lax.all_gather(middle_key_value, "seq", axis=1, tiled=True)
    group_rows = middle_devices * middle_key_value.shape[1]
    middle_key_value = lax.dynamic_slice_in_dim(
        every_row, device // middle_devices * group_rows, group_rows, 1
    )
    middle_start = device // middle_devices * middle_devices * block_rows
    middle_pos = (
        middle_start
        + middle_level_offsets[:, None]
        + DILATION_SECOND * jnp.arange(middle_key_value.shape[1], dtype=jnp.int32)[None, :]
    )
    middle_attention, middle_log_sum = attend(
        middle_level[0],
        middle_key_value[0],
        middle_key_value[1],
        middle_pos,
        valid_limit,
        head_count,
    )
    middle_output, middle_level_mass, middle_selected = scatter_rows(
        middle_attention, middle_log_sum, DILATION_SECOND, middle_level_offsets
    )
    distant_offsets = head_indices % DILATION_THIRD
    distant_local_rows = select_rows(projected_rows, DILATION_THIRD, distant_offsets)
    distant_key_value = lax.all_gather(distant_local_rows[1:], "seq", axis=1, tiled=True)
    distant_positions = (
        distant_offsets[:, None]
        + DILATION_THIRD * jnp.arange(distant_key_value.shape[1], dtype=jnp.int32)[None, :]
    )
    distant_attention, distant_log_sum = attend(
        distant_local_rows[0],
        distant_key_value[0],
        distant_key_value[1],
        distant_positions,
        valid_limit,
        head_count,
    )
    distant_output, distant_mass, distant_selected = scatter_rows(
        distant_attention, distant_log_sum, DILATION_THIRD, distant_offsets
    )
    outputs = jnp.stack([near_out, middle_output, distant_output])
    masses = jnp.stack([near_mass, middle_level_mass, distant_mass])
    selects = jnp.stack([near_sel, middle_selected, distant_selected])
    ceiling = jnp.max(masses, axis=0)
    shares = jnp.where(selects, jnp.exp(masses - ceiling), 0.0)
    combined = jnp.sum(shares[..., None] * outputs, axis=0) / jnp.sum(shares, axis=0)[..., None]
    combined = jnp.where((row_index < valid_limit)[:, None, None], combined, 0.0).reshape(
        block_rows, cols_here
    )
    row_total, row_square = lax.psum(
        (jnp.sum(combined, axis=1), jnp.sum(combined * combined, axis=1)), "head"
    )
    mean_value = row_total / DS
    mean_square = row_square / DS
    scaling = lax.rsqrt(mean_square - mean_value * mean_value + layer_eps)
    settled = ((combined - mean_value[:, None]) * scaling[:, None] * sub_gain).astype(jnp.bfloat16)
    partial_rows = jnp.dot(settled, w_out, preferred_element_type=jnp.float32)
    branch_sum = lax.psum_scatter(partial_rows, "head", scatter_dimension=1, tiled=True)
    return own_part.astype(jnp.float32) + branch_sum


MESH = pl.DeviceIdType.MESH
LANES = 128


def remote(src, dst, send_sem, recv_sem, device):
    return pltpu.make_async_remote_copy(
        src_ref=src,
        dst_ref=dst,
        send_sem=send_sem,
        recv_sem=recv_sem,
        device_id=device,
        device_id_type=MESH,
    )


def dot_rows(left, right):
    return lax.dot_general(
        left, right, (((1,), (1,)), ((), ())), preferred_element_type=jnp.float32
    )


def encode_kernel(
    tiles,
    valid_ref,
    tok_hbm,
    gain_hbm,
    scale_hbm,
    fc_hbm,
    w_hbm,
    down_hbm,
    embed_hbm,
    pre_hbm,
    wcol_hbm,
    bias_hbm,
    sub_hbm,
    order_hbm,
    slide_hbm,
    qkv_hbm,
    out_ref,
    gain_ref,
    scale_ref,
    fc_ref,
    pre_ref,
    wcol_ref,
    bias_ref,
    sub_ref,
    order_ref,
    slide_ref,
    tok_ref,
    down_ref,
    embed_ref,
    qkv_ref,
    wcol_parts,
    narrow_ref,
    pre_own,
    pre_out,
    new_out,
    wcol_out,
    sub_out,
    sequence,
    queries,
    key_rows,
    value_cols,
    fresh,
    keep_rows,
    keep_cols,
    slide_col,
    sub_col,
    mix_old,
    mix_query,
    mix_mass,
    new_kv,
    new_mix,
    normed,
    wall,
    acc,
    pool_parts,
    pool_mine,
    pooled,
    sums,
    means,
    parts,
    local_sem,
    send_tok,
    recv_tok,
    recv_mate,
    send_w,
    recv_w,
    send_pre,
    recv_pre,
    send_fan,
    recv_fan,
    send_aux,
    recv_aux,
    send_pool,
    recv_pool,
    send_mean,
    recv_mean,
    send_part,
    recv_part,
    send_new,
    recv_new,
    send_mix,
    recv_mix,
    send_kv,
    recv_kv,
):
    n = lax.axis_size("seq")
    heads = lax.axis_size("head")
    z = lax.axis_index("seq")
    hd = lax.axis_index("head")
    y = lax.axis_index("groups")
    rows, width = tok_hbm.shape
    patch = rows // tiles
    depth, hidden_width = w_hbm.shape[1:]
    quarter = rows // heads
    share = hidden_width // 4
    blocks_k = depth // LANES
    blocks_c = share // LANES
    narrow = wcol_hbm.shape[0]

    part = lax.rem(z, 2)
    pair = z // 2
    partner = z + 1 - 2 * part
    at_end = (z == 0) | (z == n - 1)
    inside = jnp.logical_not(at_end)
    inner = n - 1 - z
    outward = jnp.where(z < 2, 0, n - 1)
    toward = jnp.where(z < 2, 1, n - 1)
    across = lax.rem(hd + 2, heads)
    mate = hd + 1 - 2 * lax.rem(hd, 2)
    beyond = lax.rem(mate + 2, heads)

    def seq_peer(k):
        return lax.rem(z + k, n)

    def ahead(k):
        return lax.rem(z + k * toward, n)

    def head_peer(k):
        return lax.rem(hd + k, heads)

    def head_source(k):
        return lax.rem(hd + heads - k, heads)

    def quarter_rows(index):
        return pl.ds(pl.multiple_of(index * quarter, quarter), quarter)

    def unit(u):
        return u // blocks_c, u % blocks_c

    def weight_block(owner, u):
        r, c = unit(u)
        place = (lax.rem(owner, 2) * 2 + y) * share + c * LANES
        return w_hbm.at[
            :, pl.ds(r * LANES, LANES), pl.ds(pl.multiple_of(place, LANES), LANES)
        ]

    def wall_block(source, u):
        r, c = unit(u)
        return wall.at[r, c, :, pl.ds(pl.multiple_of(source * LANES, LANES), LANES), :]

    units = blocks_k * blocks_c
    half = quarter // 2
    first_quarters = (hd, across, mate, beyond)
    token_loads = [
        pltpu.make_async_copy(
            tok_hbm.at[quarter_rows(q)], tok_ref.at[quarter_rows(q)], local_sem.at[i]
        )
        for i, q in enumerate(first_quarters)
    ]
    loads = [
        pltpu.make_async_copy(source, target, local_sem.at[4 + i])
        for i, (source, target) in enumerate(
            ((qkv_hbm, qkv_ref), (down_hbm, down_ref), (embed_hbm, embed_ref.at[hd]))
        )
    ]
    weight_loads = [
        pltpu.make_async_copy(weight_block(z, u), wall_block(z, u), local_sem.at[7])
        for u in range(units)
    ]
    barrier = pltpu.get_barrier_semaphore()
    count = 0
    for k in range(n):
        for j in range(heads):
            if k or j:
                pl.semaphore_signal(
                    barrier,
                    inc=1,
                    device_id={"seq": seq_peer(k), "head": head_peer(j)},
                    device_id_type=MESH,
                )
                count += 1
    for k in range(n):
        pl.semaphore_signal(
            barrier, inc=1, device_id={"groups": 1 - y, "seq": seq_peer(k)}, device_id_type=MESH
        )
        count += 1
    small_loads = [
        pltpu.make_async_copy(source, target, local_sem.at[8 + i])
        for i, (source, target) in enumerate(
            (
                (pre_hbm, pre_ref),
                (gain_hbm, gain_ref),
                (scale_hbm, scale_ref),
                (fc_hbm, fc_ref),
                (wcol_hbm, wcol_ref),
                (bias_hbm, bias_ref),
                (sub_hbm, sub_ref),
                (order_hbm, order_ref),
                (slide_hbm, slide_ref),
            )
        )
    ]
    for load in token_loads[:1] + small_loads + token_loads[1:] + weight_loads + loads:
        load.start()

    block = 64

    def norm_quarter(position):
        index = first_quarters[position]
        token_loads[position].wait()

        def norm_rows(i, total):
            at = pl.ds(pl.multiple_of(index * quarter + i * block, block), block)
            values = tok_ref[at, :].astype(jnp.float32)
            out = normalize(values, gain_ref[...].reshape(1, width)).astype(jnp.bfloat16)
            normed[y * 2 + part, index, pl.ds(pl.multiple_of(i * block, block), block), :] = out
            return total + jnp.sum(values, axis=0, keepdims=True)

        sums[index] = lax.fori_loop(
            0, quarter // block, norm_rows, jnp.zeros((1, width), jnp.float32)
        )

    cols, stored_count = pre_hbm.shape
    stored_rows = stored_count + tiles
    small_loads[0].wait()
    small_loads[1].wait()
    pre_own[...] = jnp.concatenate(
        [pre_ref[...], jnp.zeros((cols, tiles), jnp.bfloat16)], axis=1
    )

    @pl.when(z < 2)
    def _():
        norm_quarter(0)

    pl.semaphore_wait(barrier, count)

    def send(source, target, sends, receives, device):
        remote(source, target, sends, receives, device).start()

    def send_weight(k, u):
        target = ahead(k)
        send(
            weight_block(target, u), wall_block(z, u), send_w.at[0], recv_w.at[u], {"seq": target}
        )

    def end_weights(r):
        for c in range(blocks_c):
            send_weight(1, r * blocks_c + c)
            send_weight(3, r * blocks_c + c)

    def paced_weights(r):
        @pl.when(at_end)
        def _():
            end_weights(r)

        @pl.when(inside)
        def _():
            for c in range(blocks_c):
                send_weight(2, r * blocks_c + c)

    own_set = y * 2 + part
    z_set = y * 2 + 1 - part
    y_set = (1 - y) * 2 + part
    d_set = (1 - y) * 2 + 1 - part

    def token_copy(which, index, event, part_of, device):
        slot = normed.at[which, index, pl.ds(part_of * half, half)]
        receives = recv_mate.at[0] if event % 4 > 1 else recv_tok.at[event // 4 * 2 + event % 4, part_of]
        return remote(slot, slot, send_tok.at[0], receives, device)

    def fan_copy(block_index, share_index, event, device):
        slot = pre_out.at[block_index, share_index]
        receives = recv_mate.at[1] if event else recv_fan.at[block_index]
        return remote(slot, slot, send_fan.at[0], receives, device)

    for index in range(2):
        target = jnp.where(
            at_end,
            jnp.where(z == 0, 1 + index, n - 2 - index),
            outward if index == 0 else inner,
        )
        send(pre_own, pre_out.at[z, hd], send_pre.at[0], recv_pre.at[z], {"seq": target})

    @pl.when(z >= 2)
    def _():
        norm_quarter(0)

    token_copy(own_set, hd, 0, 0, {"seq": partner}).start()
    for part_of in range(2):
        token_copy(own_set, hd, 4, part_of, {"groups": 1 - y}).start()

    @pl.when(at_end)
    def _():
        token_copy(own_set, hd, 0, 1, {"seq": partner}).start()

    @pl.when(at_end)
    def _():
        for u in range(units):
            send_weight(2, u)
        end_weights(0)

    @pl.when(inside)
    def _():
        for u in range(units):
            send_weight(1, u)

    cols_half = cols // 2

    def embed_half(owner, which):
        return embed_ref.at[
            owner, pl.ds(pl.multiple_of(which * cols_half, cols_half), cols_half)
        ]

    def embed_copy(owner, which, event, device):
        slot = embed_half(owner, which)
        return remote(slot, slot, send_new.at[1], recv_new.at[event], device)

    loads[2].wait()
    own_embed = embed_ref.at[hd]
    send(own_embed, own_embed, send_new.at[0], recv_new.at[0], {"head": mate})
    embed_copy(hd, y, 1, {"head": across}).start()
    pre_out[z, hd] = pre_own[...]
    norm_quarter(1)

    def fan_first(b):
        fan_copy(b, hd, 0, {"head": across}).start()
        fan_copy(b, hd, 1, {"head": mate}).start()

    def fan_second(b):
        fan_copy(b, across, 0, {"head": across}).wait_recv()
        fan_copy(b, across, 2, {"head": mate}).start()

    def stored_block(b, forward=False):
        slot = pre_out.at[b, hd]
        remote(slot, slot, send_pre.at[0], recv_pre.at[b], {"seq": partner}).wait_recv()
        if forward:
            send(slot, slot, send_pre.at[1], recv_pre.at[b], {"seq": outward})
        fan_first(b)

    fan_first(z)
    second_end = jnp.where(z == 0, 2, n - 3)

    @pl.when(at_end)
    def _():
        stored_block(partner)

    @pl.when(inside)
    def _():
        stored_block(inner, True)
        token_copy(own_set, hd, 0, 1, {"seq": partner}).start()
        stored_block(outward)

    norm_quarter(2)
    norm_quarter(3)
    for tile in range(tiles):
        per = heads // tiles
        means[z, pl.ds(tile, 1), :] = (
            sum(sums[tile * per + i] for i in range(per)) / patch
        )
    for k in range(1, n):
        send(means.at[z], means.at[z], send_mean.at[0], recv_mean.at[0], {"seq": seq_peer(k)})
    for load in small_loads[2:]:
        load.wait()
    narrow_ref[pl.ds(0, 1), :] = bias_ref[...].reshape(1, narrow)
    narrow_ref[pl.ds(1, 1), :] = sub_ref[...].reshape(1, narrow)
    for j in range(heads):
        wcol_parts[j] = wcol_ref[:, j * narrow : (j + 1) * narrow].T
    wcol_out[hd] = wcol_parts[hd]
    sub_out[hd] = narrow_ref[...]

    def column(row):
        size = row.shape[1]
        same = lax.broadcasted_iota(jnp.int32, (size, size), 0) == lax.broadcasted_iota(
            jnp.int32, (size, size), 1
        )
        return jnp.sum(jnp.where(same, row, 0.0), axis=1, keepdims=True)

    features = heads * cols
    for start in range(0, features, LANES):
        at = pl.ds(start, LANES)
        slide_col[at, :] = column(slide_ref[...].reshape(1, features)[:, start : start + LANES])

    def token_event(which, index, event, part_of, forwards):
        token_copy(which, index, event, part_of, {"head": mate}).wait_recv()
        for to, device in forwards:
            token_copy(which, index, to, part_of, device).start()

    from_z = ((8, {"groups": 1 - y}), (1, {"head": across}), (2, {"head": mate}))
    token_event(y_set, hd, 4, 0, ((6, {"head": mate}),))

    @pl.when(inside)
    def _():
        stored_block(n - 1 - outward, True)

    token_event(z_set, hd, 0, 0, from_z)
    token_event(y_set, hd, 4, 1, ((6, {"head": mate}),))

    @pl.when(at_end)
    def _():
        stored_block(second_end)

    token_event(z_set, hd, 0, 1, (from_z[0], from_z[2]))
    for part_of in range(2):
        token_copy(own_set, across, 5, part_of, {"groups": 1 - y}).start()

    @pl.when(at_end)
    def _():
        stored_block(n - 1 - z)

    @pl.when(inside)
    def _():
        for u in range(units):
            send_weight(3, u)

    fan_second(z)

    @pl.when(at_end)
    def _():
        fan_second(partner)
        fan_second(second_end)

    @pl.when(inside)
    def _():
        fan_second(inner)
        fan_second(outward)
        for c in range(blocks_c):
            send_weight(2, c)

    token_copy(z_set, hd, 1, 1, {"head": across}).start()
    for part_of in range(2):
        token_event(d_set, hd, 8, part_of, ((9, {"head": across}), (10, {"head": mate})))
    paced_weights(1)
    fan_second(jnp.where(at_end, n - 1 - z, n - 1 - outward))
    step = stored_rows
    total_rows = n * step
    limit = valid_ref[0]
    new_count = n * tiles
    factor = 1.0 / math.sqrt(HEAD_DIM)
    head_count = cols // HEAD_DIM

    def multiplicity(first, second, offset):
        middle = (first % DILATION_SECOND == offset % DILATION_SECOND) & (
            second % DILATION_SECOND == offset % DILATION_SECOND
        )
        distant = (first % DILATION_THIRD == offset % DILATION_THIRD) & (
            second % DILATION_THIRD == offset % DILATION_THIRD
        )
        return 1.0 + jnp.where(middle, 1.0, 0.0) + jnp.where(distant, 1.0, 0.0)

    def sequence_step(t):
        at = pl.ds(t * step, step)
        per = step // LANES
        order = jnp.concatenate([order_ref[pl.ds(t * per + i, 1), :] for i in range(per)], axis=1)
        label = lax.broadcasted_iota(jnp.int32, (step, step), 0)
        label = jnp.where(label < stored_count, label + tiles, -n * step)
        picks = jnp.concatenate(
            [jnp.where(order == label + b * step, 1.0, 0.0).astype(jnp.bfloat16) for b in range(n)],
            axis=0,
        )
        label = lax.broadcasted_iota(jnp.int32, (LANES, step), 0)
        wanted = jnp.where(label < new_count, label // tiles * step + label % tiles, -1)
        found = jnp.where(order == wanted, 1.0, 0.0)
        fresh[t] = found.astype(jnp.bfloat16)
        lane = lax.broadcasted_iota(jnp.int32, (1, step), 1) + t * step
        keep_cols[:, t * step : (t + 1) * step] = jnp.where(
            lane < limit, 1.0 - jnp.sum(found, axis=0, keepdims=True), 0.0
        )
        row = lax.broadcasted_iota(jnp.int32, (step, 1), 0) + t * step
        keep_rows[at, :] = jnp.where(
            row < limit, 1.0 - jnp.sum(found.T, axis=1, keepdims=True), 0.0
        )
        stored = jnp.concatenate(
            [jnp.concatenate([pre_out[b, j] for b in range(n)], axis=1) for j in range(heads)],
            axis=0,
        )
        values = jnp.dot(stored, picks, preferred_element_type=jnp.float32)
        sequence[t] = values.astype(jnp.bfloat16).reshape(heads, cols, step)
        centered = values - jnp.sum(values, axis=0, keepdims=True) / features
        variance = jnp.sum(centered * centered, axis=0, keepdims=True) / features
        normal = (centered * lax.rsqrt(variance + layer_eps) * slide_col[...]).astype(jnp.bfloat16)
        result = jnp.dot(
            qkv_ref[...].reshape(3 * cols, features), normal, preferred_element_type=jnp.float32
        ).astype(jnp.bfloat16)
        queries[t] = result[:cols]
        key_rows[at, :] = result[cols : 2 * cols].T
        value_cols[:, t * step : (t + 1) * step] = result[2 * cols :]

    def attend_stored():
        query = queries[z]
        row_head = lax.broadcasted_iota(jnp.int32, (cols, 1), 0) // HEAD_DIM
        key_at = lax.broadcasted_iota(jnp.int32, (total_rows, 1), 0)
        query_at = lax.broadcasted_iota(jnp.int32, (1, step), 1) + z * step
        for h in range(head_count):
            own = jnp.where(row_head == h, query, jnp.zeros((), jnp.bfloat16))
            scores = jnp.dot(key_rows[...], own, preferred_element_type=jnp.float32) * factor
            scores = jnp.where(keep_rows[...] > 0.0, scores, masked_score)
            peak = jnp.max(scores, axis=0, keepdims=True)
            weights = jnp.exp(scores - peak) * multiplicity(
                key_at, query_at, hd * head_count + h
            )
            at = slice(h * HEAD_DIM, (h + 1) * HEAD_DIM)
            values = jnp.concatenate(
                [value_cols[at, :], jnp.ones((16, total_rows), jnp.bfloat16)], axis=0
            )
            total = jnp.dot(
                values, weights.astype(jnp.bfloat16), preferred_element_type=jnp.float32
            )
            mass = total[HEAD_DIM : HEAD_DIM + 1]
            mix_old[hd, at, :] = (total[:HEAD_DIM] / mass).astype(jnp.bfloat16)
            mix_mass[hd, h * 8 : (h + 1) * 8, :] = jnp.broadcast_to(peak + jnp.log(mass), (8, step))
        mix_query[hd] = query
        for k in range(1, heads):
            for index, buffer in enumerate((mix_query, mix_mass, mix_old)):
                send(
                    buffer.at[hd],
                    buffer.at[hd],
                    send_mix.at[index],
                    recv_mix.at[index],
                    {"head": head_peer(k)},
                )

    loads[0].wait()
    slot = pre_out.at[:, pl.ds(0, 2)]
    remote(slot, slot, send_fan.at[0], recv_mate.at[1], {"head": mate}).wait_recv()
    for t in range(n):
        sequence_step(t)
        if t == 1:
            for r in range(2, blocks_k):
                paced_weights(r)
            embed_copy(across, y, 1, {"head": across}).wait_recv()
            embed_copy(across, y, 2, {"groups": 1 - y}).start()
            embed_copy(across, y, 3, {"head": mate}).start()
        if t in (0, n - 2):
            which, index, event = (z_set, across, 1) if t == 0 else (y_set, across, 5)
            for part_of in range(2):
                token_event(which, index, event, part_of, ((event + 2, {"head": mate}),))
    for k in range(1, heads):
        send(
            wcol_parts.at[head_peer(k)],
            wcol_out.at[hd],
            send_aux.at[0],
            recv_aux.at[0],
            {"head": head_peer(k)},
        )
        send(narrow_ref, sub_out.at[hd], send_aux.at[1], recv_aux.at[1], {"head": head_peer(k)})
    attend_stored()
    for part_of in range(2):
        token_event(d_set, across, 9, part_of, ((11, {"head": mate}),))
    embed_copy(across, 1 - y, 2, {"groups": 1 - y}).wait_recv()
    embed_copy(across, 1 - y, 4, {"head": mate}).start()
    slot = normed.at[pl.ds(0, 3), pl.ds(0, 2)]
    remote(slot, slot, send_tok.at[0], recv_mate.at[0], {"head": mate}).wait_recv()
    whole = wall.at[:, :, :, pl.ds(0, LANES), :]
    pltpu.make_async_copy(whole, whole, local_sem.at[7]).wait()

    def arrived(u):
        r, c = unit(u)
        others = wall.at[r, c, :, pl.ds(0, (n - 1) * LANES), :]
        remote(others, others, send_w.at[0], recv_w.at[u], {"seq": partner}).wait_recv()

    def gathered(r, chosen):
        return jnp.concatenate([wall[r, c, g] for c in chosen for g in range(2)], axis=1)

    def token_block(s, r):
        return jnp.concatenate(
            [
                normed[s, :, :, b * depth + r * LANES : b * depth + (r + 1) * LANES].reshape(
                    rows, LANES
                )
                for b in range(n)
            ],
            axis=1,
        )

    def multiply(r):
        for c in range(blocks_c):
            arrived(r * blocks_c + c)
        w = gathered(r, range(blocks_c))

        @pl.loop(0, 4)
        def _(s):
            value = jnp.dot(token_block(s, r), w, preferred_element_type=jnp.float32)
            if r == 0:
                acc[s] = value
            else:
                acc[s] += value

    def pool():
        r = blocks_k - 1
        for c in range(blocks_c):
            arrived(r * blocks_c + c)
        w = gathered(r, range(blocks_c))

        @pl.loop(0, 4)
        def _(s):
            value = acc[s] + jnp.dot(token_block(s, r), w, preferred_element_type=jnp.float32)
            for c in range(blocks_c):
                gate = value[:, 2 * c * LANES : (2 * c + 1) * LANES]
                raised = value[:, (2 * c + 1) * LANES : (2 * c + 2) * LANES]
                hidden = (gate / (1.0 + jnp.exp(-gate)) * raised).astype(jnp.bfloat16)
                hidden = hidden.astype(jnp.float32)
                for tile in range(tiles):
                    pool_parts[s // 2, c, pl.ds(s % 2 * tiles + tile, 1), :] = (
                        jnp.sum(hidden[tile * patch : (tile + 1) * patch], axis=0, keepdims=True)
                        / patch
                    )

        for yy in range(2):
            pool_mine[yy] = jnp.concatenate([pool_parts[yy, c] for c in range(blocks_c)], axis=1)
        place = y * n + z
        pooled[place] = pool_mine[y]
        for k in reversed(range(n)):
            for other in range(2):
                if k or other:
                    yy = 1 - y if other else y
                    send(
                        pool_mine.at[yy],
                        pooled.at[place],
                        send_pool.at[0],
                        recv_pool.at[0],
                        {"groups": yy, "seq": ahead(k)},
                    )

    for r in range(blocks_k - 1):
        multiply(r)
    pool()

    seen = means.at[pl.ds(0, n - 1)]
    remote(seen, seen, send_mean.at[0], recv_mean.at[0], {"seq": partner}).wait_recv()
    slot = pooled.at[pl.ds(0, 2 * n - 1)]
    remote(slot, slot, send_pool.at[0], recv_pool.at[0], {"seq": partner}).wait_recv()
    loads[1].wait()
    everyone = jnp.concatenate(
        [
            jnp.concatenate(
                [pooled[yy * n + b + m] for m in range(2) for yy in range(2)],
                axis=1,
            )
            for b in range(0, n, 2)
        ],
        axis=0,
    )
    high = everyone.astype(jnp.bfloat16)
    rest = everyone - high.astype(jnp.float32)
    middle = rest.astype(jnp.bfloat16)
    low = (rest - middle.astype(jnp.float32)).astype(jnp.bfloat16)
    product = jnp.dot(
        jnp.concatenate([low, middle, high], axis=0),
        down_ref[...],
        preferred_element_type=jnp.float32,
    )
    local_part = sum(product[i * n * tiles : (i + 1) * n * tiles] for i in range(3))
    here = z * heads + hd
    parts[here] = local_part.astype(jnp.bfloat16)
    for k in reversed(range(n)):
        for j in reversed(range(heads)):
            if k or j:
                send(
                    parts.at[here],
                    parts.at[here],
                    send_part.at[0],
                    recv_part.at[0],
                    {"seq": ahead(k), "head": head_peer(j)},
                )
    for buffer, receives in ((wcol_out, recv_aux.at[0]), (sub_out, recv_aux.at[1])):
        slot = buffer.at[pl.ds(0, heads - 1)]
        remote(slot, slot, send_aux.at[0], receives, {"head": mate}).wait_recv()
    for j in range(heads):
        sub_col[pl.ds(j * cols, cols), :] = column(sub_out[j, 1:2])
    slot = parts.at[pl.ds(0, n * heads - 1)]
    remote(slot, slot, send_part.at[0], recv_part.at[0], {"seq": partner}).wait_recv()
    remote(own_embed, own_embed, send_new.at[0], recv_new.at[0], {"head": mate}).wait_recv()
    for which, event in ((y, 3), (1 - y, 4)):
        embed_copy(beyond, which, event, {"head": mate}).wait_recv()
    summed = jnp.concatenate(
        [
            sum(parts[b * heads + j].astype(jnp.float32) for j in range(heads))
            for b in range(n)
        ],
        axis=1,
    )
    average = jnp.concatenate([means[b] for b in range(n)], axis=0)
    feature = normalize(
        average + scale_ref[...].reshape(1, width) * summed, fc_ref[...].reshape(1, width)
    ).astype(jnp.bfloat16)
    table = embed_ref[...].reshape(heads * cols, width)
    shift = jnp.concatenate([sub_out[j, 0:1] for j in range(heads)], axis=1)
    fresh_values = (dot_rows(feature, table) + shift).astype(jnp.bfloat16)
    for j in range(heads):
        new_out[j] = fresh_values[:, j * cols : (j + 1) * cols]
    fresh_values = fresh_values.astype(jnp.float32)

    def peers(buffer, receives):
        slot = buffer.at[pl.ds(0, heads - 1)]
        remote(slot, slot, send_aux.at[0], receives, {"head": mate}).wait_recv()

    normal = normalize(fresh_values, slide_ref[...].reshape(1, features)).astype(jnp.bfloat16)
    new_query, new_key, new_value = [
        dot_rows(normal, qkv_ref[g]).astype(jnp.bfloat16) for g in range(3)
    ]
    new_kv[hd, 0] = new_key
    new_kv[hd, 1] = new_value
    for k in range(1, heads):
        send(new_kv.at[hd], new_kv.at[hd], send_kv.at[0], recv_kv.at[0], {"head": head_peer(k)})
    lane_head = lax.broadcasted_iota(jnp.int32, (1, cols), 1) // HEAD_DIM
    nothing = jnp.zeros((), jnp.bfloat16)

    def by_head(rows_in):
        return jnp.concatenate(
            [jnp.where(lane_head == h, rows_in, nothing) for h in range(head_count)], axis=0
        )

    key_at = lax.broadcasted_iota(jnp.int32, (new_count, total_rows), 1)
    placed = jnp.concatenate([fresh[t, :new_count].astype(jnp.float32) for t in range(n)], axis=1)
    new_at = jnp.sum(placed * key_at.astype(jnp.float32), axis=1, keepdims=True).astype(jnp.int32)
    other = lax.broadcasted_iota(jnp.int32, (1, LANES), 1)
    new_lane = jnp.sum(
        jnp.where(other == lax.broadcasted_iota(jnp.int32, (new_count, LANES), 0), new_at, 0),
        axis=0,
        keepdims=True,
    )[:, :new_count]

    many = by_head(new_query)
    scores = dot_rows(many, key_rows[...]) * factor
    scores = jnp.where(keep_cols[...] > 0.0, scores, masked_score)
    recent = dot_rows(many, new_key) * factor
    recent = jnp.where(new_lane < limit, recent, masked_score)
    peak = jnp.maximum(
        jnp.max(scores, axis=1, keepdims=True), jnp.max(recent, axis=1, keepdims=True)
    )
    row_at = jnp.concatenate([new_at] * head_count, axis=0)
    offset = hd * head_count + lax.broadcasted_iota(
        jnp.int32, (head_count * new_count, 1), 0
    ) // new_count
    weights = jnp.exp(scores - peak) * multiplicity(key_at[:1], row_at, offset)
    recent = jnp.exp(recent - peak) * multiplicity(new_lane, row_at, offset)
    mass = jnp.sum(weights, axis=1, keepdims=True) + jnp.sum(recent, axis=1, keepdims=True)
    attended = (
        dot_rows(weights.astype(jnp.bfloat16), value_cols[...])
        + jnp.dot(recent.astype(jnp.bfloat16), new_value, preferred_element_type=jnp.float32)
    ) / mass
    new_mix[hd] = sum(
        jnp.where(lane_head == h, attended[h * new_count : (h + 1) * new_count], 0.0)
        for h in range(head_count)
    ).astype(jnp.bfloat16)
    for k in range(1, heads):
        send(new_mix.at[hd], new_mix.at[hd], send_kv.at[1], recv_kv.at[1], {"head": head_peer(k)})

    for index, buffer in enumerate((mix_query, mix_mass, mix_old)):
        peers(buffer, recv_mix.at[index])
    peers(new_kv, recv_kv.at[0])
    query_at = lax.broadcasted_iota(jnp.int32, (1, step), 1) + z * step
    here_fresh = fresh[z, :new_count]
    known = 1.0 - jnp.sum(here_fresh.astype(jnp.float32), axis=0, keepdims=True)
    known = jnp.where(query_at < limit, known, 0.0)
    betas, alphas = [], []
    for j in range(heads):
        scores = (
            jnp.dot(by_head(new_kv[j, 0]), mix_query[j], preferred_element_type=jnp.float32)
            * factor
        )
        scores = jnp.where(row_at < limit, scores, masked_score)
        offset = j * head_count + lax.broadcasted_iota(
            jnp.int32, (head_count * new_count, 1), 0
        ) // new_count
        grouped = (head_count, new_count, step)
        scores = scores.reshape(grouped)
        stored_mass = mix_mass[j].reshape(grouped)
        ceiling = jnp.maximum(jnp.max(scores, axis=1, keepdims=True), stored_mass)
        weights = jnp.exp(scores - ceiling) * multiplicity(row_at, query_at, offset).reshape(grouped)
        old = jnp.exp(stored_mass - ceiling)
        inverse = known / (old + jnp.sum(weights, axis=1, keepdims=True))
        betas.append((weights * inverse).reshape(head_count * new_count, step))
        alphas.append(old * inverse)

    inside_limit = jnp.where(query_at < limit, here_fresh.astype(jnp.float32), 0.0).astype(
        jnp.bfloat16
    )

    def contract(left, right):
        return lax.dot_general(
            left, right, (((0,), (0,)), ((), ())), preferred_element_type=jnp.float32
        )

    pieces = []
    for j in range(heads):
        share_of = jnp.concatenate(
            [
                mix_old[j, h * HEAD_DIM : (h + 1) * HEAD_DIM, :].astype(jnp.float32)
                * alphas[j][h, :1]
                for h in range(head_count)
            ],
            axis=0,
        )
        pieces.append(share_of + contract(by_head(new_kv[j, 1]), betas[j].astype(jnp.bfloat16)))
    branch = sequence[z, hd].astype(jnp.float32) + contract(new_out[hd], here_fresh)
    peers(new_mix, recv_kv.at[1])
    pieces = [piece + contract(new_mix[j], inside_limit) for j, piece in enumerate(pieces)]
    mean = sum(jnp.sum(p, axis=0, keepdims=True) for p in pieces) / features
    square = sum(jnp.sum(p * p, axis=0, keepdims=True) for p in pieces) / features
    scaling = lax.rsqrt(square - mean * mean + layer_eps)
    for j in range(heads):
        gain = sub_col[pl.ds(j * cols, cols), :]
        settled = ((pieces[j] - mean) * scaling * gain).astype(jnp.bfloat16)
        branch += jnp.dot(wcol_out[j], settled, preferred_element_type=jnp.float32)
    out_ref[...] = branch

    def drain(slot, sends):
        remote(slot, slot, sends, recv_new.at[0], {"head": mate}).wait_send()

    drain(normed.at[pl.ds(0, 3)], send_tok.at[0])
    drain(wall.at[:, :, :, pl.ds(0, (n - 1) * LANES), :], send_w.at[0])
    drain(pre_out.at[0, pl.ds(0, 2)], send_pre.at[0])

    @pl.when(inside)
    def _():
        drain(pre_out.at[0, pl.ds(0, 2)], send_pre.at[1])

    drain(pre_out.at[pl.ds(0, 3)], send_fan.at[0])
    drain(wcol_out.at[pl.ds(0, heads - 1)], send_aux.at[0])
    drain(sub_out.at[pl.ds(0, heads - 1)], send_aux.at[1])
    drain(pooled.at[pl.ds(0, 2 * n - 1)], send_pool.at[0])
    drain(means.at[pl.ds(0, n - 1)], send_mean.at[0])
    drain(parts.at[pl.ds(0, n * heads - 1)], send_part.at[0])
    drain(own_embed, send_new.at[0])
    drain(embed_ref.at[pl.ds(0, 2)], send_new.at[1])
    for index, buffer in enumerate((mix_query, mix_mass, mix_old)):
        drain(buffer.at[pl.ds(0, heads - 1)], send_mix.at[index])
    drain(new_kv.at[pl.ds(0, heads - 1)], send_kv.at[0])
    drain(new_mix.at[pl.ds(0, heads - 1)], send_kv.at[1])


def near_body(
    tile_tokens,
    tile_gain,
    w_gate_up,
    w_down,
    layer_scale,
    fc_gain,
    w_embed,
    embed_bias,
    pre_emb,
    tile_order,
    valid_count,
    slide_gain,
    w_qkv,
    sub_gain,
    w_out,
):
    n = lax.axis_size("seq")
    heads = lax.axis_size("head")
    tiles, patch, width = tile_tokens.shape
    depth, hidden_width = w_gate_up.shape[1:]
    rows = tiles * patch
    cols = w_embed.shape[1]
    head_count = cols // HEAD_DIM
    total_rows = tile_order.shape[0]
    block_rows = total_rows // n
    vmem = pl.BlockSpec(memory_space=pltpu.VMEM)
    anywhere = pl.BlockSpec(memory_space=pl.ANY)
    dma = pltpu.SemaphoreType.DMA
    f32, bf16 = jnp.float32, jnp.bfloat16
    quarter = rows // heads
    blocks_k = depth // LANES
    blocks_c = hidden_width // 4 // LANES
    out = pl.pallas_call(
        functools.partial(encode_kernel, tiles),
        out_shape=pltpu.VMEM((cols, block_rows), f32),
        in_specs=[pl.BlockSpec(memory_space=pltpu.SMEM)] + [anywhere] * 14,
        out_specs=vmem,
        scratch_shapes=[
            pltpu.VMEM((width,), f32),
            pltpu.VMEM((width,), f32),
            pltpu.VMEM((width,), f32),
            pltpu.VMEM((cols, block_rows - tiles), bf16),
            pltpu.VMEM((cols, heads * cols), bf16),
            pltpu.VMEM((cols,), f32),
            pltpu.VMEM((cols,), f32),
            pltpu.VMEM((total_rows // LANES, LANES), jnp.int32),
            pltpu.VMEM((heads * cols,), f32),
            pltpu.VMEM((rows, width), bf16),
            pltpu.VMEM(w_down.shape, bf16),
            pltpu.VMEM((heads, cols, width), bf16),
            pltpu.VMEM((3, cols, heads * cols), bf16),
            pltpu.VMEM((heads, cols, cols), bf16),
            pltpu.VMEM((2, cols), f32),
            pltpu.VMEM((cols, block_rows), bf16),
            pltpu.VMEM((n, heads, cols, block_rows), bf16),
            pltpu.VMEM((heads, n * tiles, cols), bf16),
            pltpu.VMEM((heads, cols, cols), bf16),
            pltpu.VMEM((heads, 2, cols), f32),
            pltpu.VMEM((n, heads, cols, block_rows), bf16),
            pltpu.VMEM((n, cols, block_rows), bf16),
            pltpu.VMEM((total_rows, cols), bf16),
            pltpu.VMEM((cols, total_rows), bf16),
            pltpu.VMEM((n, LANES, block_rows), bf16),
            pltpu.VMEM((total_rows, 1), f32),
            pltpu.VMEM((1, total_rows), f32),
            pltpu.VMEM((heads * cols, 1), f32),
            pltpu.VMEM((heads * cols, 1), f32),
            pltpu.VMEM((heads, cols, block_rows), bf16),
            pltpu.VMEM((heads, cols, block_rows), bf16),
            pltpu.VMEM((heads, head_count * 8, block_rows), f32),
            pltpu.VMEM((heads, 2, n * tiles, cols), bf16),
            pltpu.VMEM((heads, n * tiles, cols), bf16),
            pltpu.VMEM((4, heads, quarter, width), bf16),
            pltpu.VMEM((blocks_k, blocks_c, 2, n * LANES, LANES), bf16),
            pltpu.VMEM((4, rows, blocks_c * 2 * LANES), f32),
            pltpu.VMEM((2, blocks_c, 2 * tiles, LANES), f32),
            pltpu.VMEM((2, 2 * tiles, blocks_c * LANES), f32),
            pltpu.VMEM((2 * n, 2 * tiles, blocks_c * LANES), f32),
            pltpu.VMEM((heads, 1, width), f32),
            pltpu.VMEM((n, tiles, width), f32),
            pltpu.VMEM((n * heads, n * tiles, w_down.shape[1]), bf16),
            dma((17,)),
            dma((1,)),
            dma((6, 2)),
            dma((2,)),
            dma((1,)),
            dma((blocks_k * blocks_c,)),
            dma((2,)),
            dma((n,)),
            dma((1,)),
            dma((n,)),
            dma((2,)),
            dma((2,)),
            dma((1,)),
            dma((1,)),
            dma((1,)),
            dma((1,)),
            dma((1,)),
            dma((1,)),
            dma((2,)),
            dma((5,)),
            dma((3,)),
            dma((3,)),
            dma((2,)),
            dma((2,)),
        ],
        compiler_params=pltpu.CompilerParams(
            collective_id=0, has_side_effects=True, vmem_limit_bytes=58 * 1024 * 1024
        ),
    )(
        valid_count,
        tile_tokens.reshape(rows, width),
        tile_gain,
        layer_scale,
        fc_gain,
        w_gate_up,
        w_down,
        w_embed.T,
        pre_emb.T,
        w_out,
        embed_bias,
        sub_gain,
        tile_order.reshape(total_rows // LANES, LANES),
        slide_gain,
        w_qkv.swapaxes(1, 2),
    )
    return out.T


def body(*args):
    total_rows = args[9].shape[0]
    mesh_fits = all(lax.axis_size(a) == k for a, k in (("groups", 2), ("seq", 4), ("head", 4)))
    if total_rows <= SPAN0 and mesh_fits:
        return near_body(*args)
    return general_body(*args)


def solution(mesh):
    placed = (
        P(("groups", "seq"), None, None),
        P(),
        P(None, "seq", "head"),
        P("head", "seq"),
        P(),
        P(),
        P(None, "head"),
        P("head"),
        P(("groups", "seq"), "head"),
        P("groups"),
        P("groups"),
        P(),
        P(None, None, "head"),
        P("head"),
        P("head", None),
    )
    return jax.shard_map(
        body, mesh=mesh, in_specs=placed, out_specs=P(("groups", "seq"), "head"), check_vma=False
    )
```

```python
import functools
import math

import jax
import jax.numpy as jnp
from jax import lax
from jax.experimental import pallas as pl
from jax.experimental.pallas import tpu as pltpu
from jax.sharding import PartitionSpec as P

DS = 768
HEAD_DIM = 48
SPAN0 = 1024
SPAN1 = 4096
DILATION_SECOND = 4
DILATION_THIRD = 16


layer_eps = 1e-05
masked_score = -1e30


def from_partner(value, axis, bit):
    mask = 2**bit
    pairs = [(source, source ^ mask) for source in range(lax.axis_size(axis))]
    return lax.ppermute(value, axis, pairs)


def normalize(values, gain):
    centered = values - jnp.mean(values, axis=-1, keepdims=True)
    variance = jnp.mean(centered * centered, axis=-1, keepdims=True)
    return centered * lax.rsqrt(variance + layer_eps) * gain


def select_rows(stacked, dilation, offsets):
    group_count, row_count, row_width = stacked.shape
    head_count = offsets.shape[0]
    arranged = stacked.reshape(
        group_count, row_count // dilation, dilation, head_count, row_width // head_count
    )
    choose = jnp.arange(dilation, dtype=jnp.int32)[:, None] == offsets[None, :]
    chosen = jnp.sum(
        jnp.where(choose[None, None, :, :, None], arranged, jnp.zeros((), stacked.dtype)), axis=2
    )
    return chosen.reshape(group_count, row_count // dilation, row_width)


def scatter_rows(attended, log_mass, dilation, offsets):
    query_count, head_count, head_size = attended.shape
    choose = jnp.arange(dilation, dtype=jnp.int32)[:, None] == offsets[None, :]
    spread_out = jnp.where(choose[None, :, :, None], attended[:, None, :, :], 0.0).reshape(
        query_count * dilation, head_count, head_size
    )
    spread_mass = jnp.where(choose[None, :, :], log_mass[:, None, :], masked_score).reshape(
        query_count * dilation, head_count
    )
    selected = jnp.broadcast_to(choose[None, :, :], (query_count, dilation, head_count)).reshape(
        query_count * dilation, head_count
    )
    return (spread_out, spread_mass, selected)


def attend(query_rows, key_rows, value_rows, positions, valid_limit, head_count):
    head_size = query_rows.shape[1] // head_count
    query_heads = query_rows.reshape(query_rows.shape[0], head_count, head_size)
    key_heads = key_rows.reshape(key_rows.shape[0], head_count, head_size)
    value_heads = value_rows.reshape(value_rows.shape[0], head_count, head_size)
    scores = jnp.einsum(
        "qhe,khe->hqk", query_heads, key_heads, preferred_element_type=jnp.float32
    ) / math.sqrt(head_size)
    scores = jnp.where((positions < valid_limit)[:, None, :], scores, masked_score)
    highest = jnp.max(scores, axis=-1, keepdims=True)
    exponent = jnp.exp(scores - highest)
    mass_sum = jnp.sum(exponent, axis=-1, keepdims=True)
    weights = (exponent / mass_sum).astype(jnp.bfloat16)
    attended = jnp.einsum("hqk,khe->qhe", weights, value_heads, preferred_element_type=jnp.float32)
    return (attended, (highest[..., 0] + jnp.log(mass_sum[..., 0])).T)


def general_body(
    tile_tokens,
    tile_gain,
    w_gate_up,
    w_down,
    layer_scale,
    fc_gain,
    w_embed,
    embed_bias,
    pre_emb,
    tile_order,
    valid_count,
    slide_gain,
    w_qkv,
    sub_gain,
    w_out,
):
    new_count, patch_count, tile_width = tile_tokens.shape
    token_rows = tile_tokens.reshape(new_count * patch_count, tile_width)
    normed = normalize(token_rows.astype(jnp.float32), tile_gain).astype(jnp.bfloat16)
    hidden_width = w_gate_up.shape[2]
    gate_up = jnp.einsum(
        "rk,gkf->grf",
        normed,
        lax.all_gather(w_gate_up, "seq", axis=1, tiled=True),
        preferred_element_type=jnp.float32,
    )
    hidden = (jax.nn.silu(gate_up[0]) * gate_up[1]).astype(jnp.bfloat16)
    pooled_hidden = jnp.mean(
        hidden.reshape(new_count, patch_count, hidden_width), axis=1, dtype=jnp.float32
    )
    everyone = lax.all_gather(pooled_hidden, "seq", axis=0, tiled=True)
    local_part = jnp.dot(everyone, w_down.astype(jnp.float32), precision=lax.Precision.HIGHEST)
    pooled_part = lax.all_to_all(local_part, "seq", split_axis=0, concat_axis=1, tiled=True)
    summed = lax.psum(pooled_part, "head")
    pooled = jnp.mean(tile_tokens, axis=1, dtype=jnp.float32) + layer_scale * summed
    feature = normalize(pooled, fc_gain).astype(jnp.bfloat16)
    new_rows = (jnp.dot(feature, w_embed, preferred_element_type=jnp.float32) + embed_bias).astype(
        jnp.bfloat16
    )
    stored = jnp.concatenate([new_rows, pre_emb], axis=0)
    block_rows = stored.shape[0]
    total_rows = tile_order.shape[0]
    peer_rows = block_rows // lax.axis_size("seq")
    device = lax.axis_index("seq")
    local_index = jnp.arange(block_rows, dtype=jnp.int32)
    inverse = (
        jnp.zeros((total_rows,), jnp.int32)
        .at[tile_order]
        .set(jnp.arange(total_rows, dtype=jnp.int32))
    )
    placed = lax.dynamic_slice_in_dim(inverse, device * block_rows, block_rows)
    target = placed // block_rows
    before = (target[:, None] == target[None, :]) & (placed[None, :] < placed[:, None])
    slot_index = target * peer_rows + jnp.sum(before, axis=1, dtype=jnp.int32)
    routing = (slot_index[None, :] == local_index[:, None]).astype(jnp.bfloat16)
    outgoing = jnp.dot(routing, stored, preferred_element_type=jnp.float32).astype(jnp.bfloat16)
    incoming = lax.all_to_all(outgoing, "seq", split_axis=0, concat_axis=0, tiled=True)
    wanted = lax.dynamic_slice_in_dim(tile_order, device * block_rows, block_rows)
    source = wanted // block_rows
    earlier = (source[:, None] == source[None, :]) & (local_index[None, :] < local_index[:, None])
    arrival = source * peer_rows + jnp.sum(earlier, axis=1, dtype=jnp.int32)
    own_part = jnp.take(incoming, arrival, axis=0)
    sequence = lax.all_gather(own_part, "head", axis=1, tiled=True)
    slide_normed = normalize(sequence.astype(jnp.float32), slide_gain).astype(jnp.bfloat16)
    projected_rows = jnp.einsum(
        "rd,gdc->grc", slide_normed, w_qkv, preferred_element_type=jnp.float32
    ).astype(jnp.bfloat16)
    cols_here = projected_rows.shape[2]
    head_count = cols_here // HEAD_DIM
    head_indices = lax.axis_index("head") * head_count + jnp.arange(head_count, dtype=jnp.int32)
    valid_limit = valid_count[0]
    row_index = device * block_rows + local_index
    near_devices = min(SPAN0, total_rows) // block_rows
    near_rows = projected_rows[1:]
    for bit_index in range(near_devices.bit_length() - 1):
        partner = from_partner(near_rows, "seq", bit_index)
        upper_half = device // (1 << bit_index) % 2 == 1
        near_rows = jnp.where(
            upper_half,
            jnp.concatenate([partner, near_rows], 1),
            jnp.concatenate([near_rows, partner], 1),
        )
    near_start = device // near_devices * near_devices * block_rows
    near_pos = jnp.broadcast_to(
        near_start + jnp.arange(near_rows.shape[1], dtype=jnp.int32),
        (head_count, near_rows.shape[1]),
    )
    near_out, near_mass = attend(
        projected_rows[0], near_rows[0], near_rows[1], near_pos, valid_limit, head_count
    )
    near_sel = jnp.ones((block_rows, head_count), dtype=bool)
    middle_level_offsets = head_indices % DILATION_SECOND
    middle_level = select_rows(projected_rows, DILATION_SECOND, middle_level_offsets)
    middle_devices = min(SPAN1, total_rows) // block_rows
    middle_key_value = middle_level[1:]
    every_row = lax.all_gather(middle_key_value, "seq", axis=1, tiled=True)
    group_rows = middle_devices * middle_key_value.shape[1]
    middle_key_value = lax.dynamic_slice_in_dim(
        every_row, device // middle_devices * group_rows, group_rows, 1
    )
    middle_start = device // middle_devices * middle_devices * block_rows
    middle_pos = (
        middle_start
        + middle_level_offsets[:, None]
        + DILATION_SECOND * jnp.arange(middle_key_value.shape[1], dtype=jnp.int32)[None, :]
    )
    middle_attention, middle_log_sum = attend(
        middle_level[0],
        middle_key_value[0],
        middle_key_value[1],
        middle_pos,
        valid_limit,
        head_count,
    )
    middle_output, middle_level_mass, middle_selected = scatter_rows(
        middle_attention, middle_log_sum, DILATION_SECOND, middle_level_offsets
    )
    distant_offsets = head_indices % DILATION_THIRD
    distant_local_rows = select_rows(projected_rows, DILATION_THIRD, distant_offsets)
    distant_key_value = lax.all_gather(distant_local_rows[1:], "seq", axis=1, tiled=True)
    distant_positions = (
        distant_offsets[:, None]
        + DILATION_THIRD * jnp.arange(distant_key_value.shape[1], dtype=jnp.int32)[None, :]
    )
    distant_attention, distant_log_sum = attend(
        distant_local_rows[0],
        distant_key_value[0],
        distant_key_value[1],
        distant_positions,
        valid_limit,
        head_count,
    )
    distant_output, distant_mass, distant_selected = scatter_rows(
        distant_attention, distant_log_sum, DILATION_THIRD, distant_offsets
    )
    outputs = jnp.stack([near_out, middle_output, distant_output])
    masses = jnp.stack([near_mass, middle_level_mass, distant_mass])
    selects = jnp.stack([near_sel, middle_selected, distant_selected])
    ceiling = jnp.max(masses, axis=0)
    shares = jnp.where(selects, jnp.exp(masses - ceiling), 0.0)
    combined = jnp.sum(shares[..., None] * outputs, axis=0) / jnp.sum(shares, axis=0)[..., None]
    combined = jnp.where((row_index < valid_limit)[:, None, None], combined, 0.0).reshape(
        block_rows, cols_here
    )
    row_total, row_square = lax.psum(
        (jnp.sum(combined, axis=1), jnp.sum(combined * combined, axis=1)), "head"
    )
    mean_value = row_total / DS
    mean_square = row_square / DS
    scaling = lax.rsqrt(mean_square - mean_value * mean_value + layer_eps)
    settled = ((combined - mean_value[:, None]) * scaling[:, None] * sub_gain).astype(jnp.bfloat16)
    partial_rows = jnp.dot(settled, w_out, preferred_element_type=jnp.float32)
    branch_sum = lax.psum_scatter(partial_rows, "head", scatter_dimension=1, tiled=True)
    return own_part.astype(jnp.float32) + branch_sum


MESH = pl.DeviceIdType.MESH
LANES = 128


def remote(src, dst, send_sem, recv_sem, device):
    return pltpu.make_async_remote_copy(
        src_ref=src,
        dst_ref=dst,
        send_sem=send_sem,
        recv_sem=recv_sem,
        device_id=device,
        device_id_type=MESH,
    )


def dot_rows(left, right):
    return lax.dot_general(
        left, right, (((1,), (1,)), ((), ())), preferred_element_type=jnp.float32
    )


def encode_kernel(
    tiles,
    valid_ref,
    tok_hbm,
    gain_hbm,
    scale_hbm,
    fc_hbm,
    w_hbm,
    down_hbm,
    embed_hbm,
    pre_hbm,
    wcol_hbm,
    bias_hbm,
    sub_hbm,
    order_hbm,
    slide_hbm,
    qkv_hbm,
    out_ref,
    gain_ref,
    scale_ref,
    fc_ref,
    pre_ref,
    wcol_ref,
    bias_ref,
    sub_ref,
    order_ref,
    slide_ref,
    tok_ref,
    down_ref,
    embed_ref,
    qkv_ref,
    qkv_cols,
    embed_cols,
    wcol_parts,
    narrow_ref,
    pre_own,
    pre_out,
    new_out,
    wcol_out,
    sub_out,
    sequence,
    queries,
    key_rows,
    key_cols,
    value_rows,
    value_cols,
    fresh,
    keep_rows,
    keep_cols,
    slide_col,
    sub_col,
    mix_old,
    mix_query,
    mix_mass,
    new_kv,
    new_mix,
    normed,
    wall,
    acc,
    pool_mine,
    pooled,
    sums,
    means,
    parts,
    local_sem,
    send_tok,
    recv_tok,
    recv_mate,
    send_w,
    recv_w,
    send_pre,
    recv_pre,
    send_fan,
    recv_fan,
    send_aux,
    recv_aux,
    send_pool,
    recv_pool,
    send_mean,
    recv_mean,
    send_part,
    recv_part,
    send_new,
    recv_new,
    send_mix,
    recv_mix,
    send_kv,
    recv_kv,
):
    n = lax.axis_size("seq")
    heads = lax.axis_size("head")
    z = lax.axis_index("seq")
    hd = lax.axis_index("head")
    y = lax.axis_index("groups")
    rows, width = tok_hbm.shape
    patch = rows // tiles
    depth, hidden_width = w_hbm.shape[1:]
    quarter = rows // heads
    share = hidden_width // 4
    blocks_k = depth // LANES
    blocks_c = share // LANES
    narrow = wcol_hbm.shape[0]

    part = lax.rem(z, 2)
    pair = z // 2
    partner = z + 1 - 2 * part
    at_end = (z == 0) | (z == n - 1)
    inside = jnp.logical_not(at_end)
    inner = n - 1 - z
    outward = jnp.where(z < 2, 0, n - 1)
    toward = jnp.where(z < 2, 1, n - 1)
    across = lax.rem(hd + 2, heads)
    mate = hd + 1 - 2 * lax.rem(hd, 2)
    beyond = lax.rem(mate + 2, heads)

    def seq_peer(k):
        return lax.rem(z + k, n)

    def ahead(k):
        return lax.rem(z + k * toward, n)

    def head_peer(k):
        return lax.rem(hd + k, heads)

    def head_source(k):
        return lax.rem(hd + heads - k, heads)

    def quarter_rows(index):
        return pl.ds(pl.multiple_of(index * quarter, quarter), quarter)

    def unit(u):
        return u // blocks_c, u % blocks_c

    def weight_block(owner, u):
        r, c = unit(u)
        place = (lax.rem(owner, 2) * 2 + y) * share + c * LANES
        return w_hbm.at[
            :, pl.ds(r * LANES, LANES), pl.ds(pl.multiple_of(place, LANES), LANES)
        ]

    def wall_block(source, u):
        r, c = unit(u)
        return wall.at[r, c, :, pl.ds(pl.multiple_of(source * LANES, LANES), LANES), :]

    units = blocks_k * blocks_c
    half = quarter // 2
    first_quarters = (hd, across, mate, beyond)
    token_loads = [
        pltpu.make_async_copy(
            tok_hbm.at[quarter_rows(q)], tok_ref.at[quarter_rows(q)], local_sem.at[i]
        )
        for i, q in enumerate(first_quarters)
    ]
    loads = [
        pltpu.make_async_copy(source, target, local_sem.at[4 + i])
        for i, (source, target) in enumerate(
            ((qkv_hbm, qkv_ref), (down_hbm, down_ref), (embed_hbm, embed_ref.at[hd]))
        )
    ]
    weight_loads = [
        pltpu.make_async_copy(weight_block(z, u), wall_block(z, u), local_sem.at[7])
        for u in range(units)
    ]
    barrier = pltpu.get_barrier_semaphore()
    count = 0
    for k in range(n):
        for j in range(heads):
            if k or j:
                pl.semaphore_signal(
                    barrier,
                    inc=1,
                    device_id={"seq": seq_peer(k), "head": head_peer(j)},
                    device_id_type=MESH,
                )
                count += 1
    for k in range(n):
        pl.semaphore_signal(
            barrier, inc=1, device_id={"groups": 1 - y, "seq": seq_peer(k)}, device_id_type=MESH
        )
        count += 1
    small_loads = [
        pltpu.make_async_copy(source, target, local_sem.at[8 + i])
        for i, (source, target) in enumerate(
            (
                (pre_hbm, pre_ref),
                (gain_hbm, gain_ref),
                (scale_hbm, scale_ref),
                (fc_hbm, fc_ref),
                (wcol_hbm, wcol_ref),
                (bias_hbm, bias_ref),
                (sub_hbm, sub_ref),
                (order_hbm, order_ref),
                (slide_hbm, slide_ref),
            )
        )
    ]
    for load in token_loads[:1] + small_loads + token_loads[1:] + weight_loads + loads:
        load.start()

    block = 64

    def norm_quarter(position):
        index = first_quarters[position]
        token_loads[position].wait()

        def norm_rows(i, total):
            at = pl.ds(pl.multiple_of(index * quarter + i * block, block), block)
            values = tok_ref[at, :].astype(jnp.float32)
            out = normalize(values, gain_ref[...].reshape(1, width)).astype(jnp.bfloat16)
            normed[y * 2 + part, index, pl.ds(pl.multiple_of(i * block, block), block), :] = out
            return total + jnp.sum(values, axis=0, keepdims=True)

        sums[index] = lax.fori_loop(
            0, quarter // block, norm_rows, jnp.zeros((1, width), jnp.float32)
        )

    cols, stored_count = pre_hbm.shape
    stored_rows = stored_count + tiles
    small_loads[0].wait()
    small_loads[1].wait()
    pre_own[...] = jnp.concatenate(
        [pre_ref[...], jnp.zeros((cols, tiles), jnp.bfloat16)], axis=1
    )

    @pl.when(z < 2)
    def _():
        norm_quarter(0)

    pl.semaphore_wait(barrier, count)

    def send(source, target, sends, receives, device):
        remote(source, target, sends, receives, device).start()

    def send_weight(k, u):
        target = ahead(k)
        send(
            weight_block(target, u), wall_block(z, u), send_w.at[0], recv_w.at[u], {"seq": target}
        )

    def end_weights(r):
        for c in range(blocks_c):
            send_weight(1, r * blocks_c + c)
            send_weight(3, r * blocks_c + c)

    def paced_weights(r):
        @pl.when(at_end)
        def _():
            end_weights(r)

        @pl.when(inside)
        def _():
            for c in range(blocks_c):
                send_weight(2, r * blocks_c + c)

    own_set = y * 2 + part
    z_set = y * 2 + 1 - part
    y_set = (1 - y) * 2 + part
    d_set = (1 - y) * 2 + 1 - part

    def token_copy(which, index, event, part_of, device):
        slot = normed.at[which, index, pl.ds(part_of * half, half)]
        receives = recv_mate.at[0] if event % 4 > 1 else recv_tok.at[event // 4 * 2 + event % 4, part_of]
        return remote(slot, slot, send_tok.at[0], receives, device)

    def fan_copy(block_index, share_index, event, device):
        slot = pre_out.at[block_index, share_index]
        receives = recv_mate.at[1] if event else recv_fan.at[block_index]
        return remote(slot, slot, send_fan.at[0], receives, device)

    for index in range(2):
        target = jnp.where(
            at_end,
            jnp.where(z == 0, 1 + index, n - 2 - index),
            outward if index == 0 else inner,
        )
        send(pre_own, pre_out.at[z, hd], send_pre.at[0], recv_pre.at[z], {"seq": target})

    @pl.when(z >= 2)
    def _():
        norm_quarter(0)

    token_copy(own_set, hd, 0, 0, {"seq": partner}).start()
    for part_of in range(2):
        token_copy(own_set, hd, 4, part_of, {"groups": 1 - y}).start()

    @pl.when(at_end)
    def _():
        token_copy(own_set, hd, 0, 1, {"seq": partner}).start()

    @pl.when(at_end)
    def _():
        for u in range(units):
            send_weight(2, u)
        end_weights(0)

    @pl.when(inside)
    def _():
        for u in range(units):
            send_weight(1, u)

    cols_half = cols // 2

    def embed_half(owner, which):
        return embed_ref.at[
            owner, pl.ds(pl.multiple_of(which * cols_half, cols_half), cols_half)
        ]

    def embed_copy(owner, which, event, device):
        slot = embed_half(owner, which)
        return remote(slot, slot, send_new.at[1], recv_new.at[event], device)

    loads[2].wait()
    own_embed = embed_ref.at[hd]
    send(own_embed, own_embed, send_new.at[0], recv_new.at[0], {"head": mate})
    embed_copy(hd, y, 1, {"head": across}).start()
    pre_out[z, hd] = pre_own[...]
    norm_quarter(1)

    def fan_first(b):
        fan_copy(b, hd, 0, {"head": across}).start()
        fan_copy(b, hd, 1, {"head": mate}).start()

    def fan_second(b):
        fan_copy(b, across, 0, {"head": across}).wait_recv()
        fan_copy(b, across, 2, {"head": mate}).start()

    def stored_block(b, forward=False):
        slot = pre_out.at[b, hd]
        remote(slot, slot, send_pre.at[0], recv_pre.at[b], {"seq": partner}).wait_recv()
        if forward:
            send(slot, slot, send_pre.at[1], recv_pre.at[b], {"seq": outward})
        fan_first(b)

    fan_first(z)
    second_end = jnp.where(z == 0, 2, n - 3)

    @pl.when(at_end)
    def _():
        stored_block(partner)

    @pl.when(inside)
    def _():
        stored_block(inner, True)
        token_copy(own_set, hd, 0, 1, {"seq": partner}).start()
        stored_block(outward)

    norm_quarter(2)
    norm_quarter(3)
    for tile in range(tiles):
        per = heads // tiles
        means[z, pl.ds(tile, 1), :] = (
            sum(sums[tile * per + i] for i in range(per)) / patch
        )
    for k in range(1, n):
        send(means.at[z], means.at[z], send_mean.at[0], recv_mean.at[0], {"seq": seq_peer(k)})
    for load in small_loads[2:]:
        load.wait()
    narrow_ref[pl.ds(0, 1), :] = bias_ref[...].reshape(1, narrow)
    narrow_ref[pl.ds(1, 1), :] = sub_ref[...].reshape(1, narrow)
    for j in range(heads):
        wcol_parts[j] = wcol_ref[:, j * narrow : (j + 1) * narrow].T
    wcol_out[hd] = wcol_parts[hd]
    sub_out[hd] = narrow_ref[...]

    def column(row):
        size = row.shape[1]
        same = lax.broadcasted_iota(jnp.int32, (size, size), 0) == lax.broadcasted_iota(
            jnp.int32, (size, size), 1
        )
        return jnp.sum(jnp.where(same, row, 0.0), axis=1, keepdims=True)

    loads[0].wait()
    for g in range(3):
        qkv_cols[g] = qkv_ref[g].T
    features = heads * cols
    for start in range(0, features, LANES):
        at = pl.ds(start, LANES)
        slide_col[at, :] = column(slide_ref[...].reshape(1, features)[:, start : start + LANES])

    def token_event(which, index, event, part_of, forwards):
        token_copy(which, index, event, part_of, {"head": mate}).wait_recv()
        for to, device in forwards:
            token_copy(which, index, to, part_of, device).start()

    from_z = ((8, {"groups": 1 - y}), (1, {"head": across}), (2, {"head": mate}))
    token_event(y_set, hd, 4, 0, ((6, {"head": mate}),))

    @pl.when(inside)
    def _():
        stored_block(n - 1 - outward, True)

    token_event(z_set, hd, 0, 0, from_z)
    token_event(y_set, hd, 4, 1, ((6, {"head": mate}),))

    @pl.when(at_end)
    def _():
        stored_block(second_end)

    token_event(z_set, hd, 0, 1, (from_z[0], from_z[2]))
    for part_of in range(2):
        token_copy(own_set, across, 5, part_of, {"groups": 1 - y}).start()

    @pl.when(at_end)
    def _():
        stored_block(n - 1 - z)

    @pl.when(inside)
    def _():
        for u in range(units):
            send_weight(3, u)

    fan_second(z)

    @pl.when(at_end)
    def _():
        fan_second(partner)
        fan_second(second_end)

    @pl.when(inside)
    def _():
        fan_second(inner)
        fan_second(outward)
        for c in range(blocks_c):
            send_weight(2, c)

    token_copy(z_set, hd, 1, 1, {"head": across}).start()
    for part_of in range(2):
        token_event(d_set, hd, 8, part_of, ((9, {"head": across}), (10, {"head": mate})))
    paced_weights(1)
    fan_second(jnp.where(at_end, n - 1 - z, n - 1 - outward))
    step = stored_rows
    total_rows = n * step
    limit = valid_ref[0]
    new_count = n * tiles
    factor = 1.0 / math.sqrt(HEAD_DIM)
    head_count = cols // HEAD_DIM

    def multiplicity(first, second, offset):
        middle = (first % DILATION_SECOND == offset % DILATION_SECOND) & (
            second % DILATION_SECOND == offset % DILATION_SECOND
        )
        distant = (first % DILATION_THIRD == offset % DILATION_THIRD) & (
            second % DILATION_THIRD == offset % DILATION_THIRD
        )
        return 1.0 + jnp.where(middle, 1.0, 0.0) + jnp.where(distant, 1.0, 0.0)

    def sequence_step(t):
        at = pl.ds(t * step, step)
        per = step // LANES
        order = jnp.concatenate([order_ref[pl.ds(t * per + i, 1), :] for i in range(per)], axis=1)
        label = lax.broadcasted_iota(jnp.int32, (step, step), 0)
        label = jnp.where(label < stored_count, label + tiles, -n * step)
        picks = jnp.concatenate(
            [jnp.where(order == label + b * step, 1.0, 0.0).astype(jnp.bfloat16) for b in range(n)],
            axis=0,
        )
        label = lax.broadcasted_iota(jnp.int32, (LANES, step), 0)
        wanted = jnp.where(label < new_count, label // tiles * step + label % tiles, -1)
        found = jnp.where(order == wanted, 1.0, 0.0)
        fresh[t] = found.astype(jnp.bfloat16)
        lane = lax.broadcasted_iota(jnp.int32, (1, step), 1) + t * step
        keep_cols[:, t * step : (t + 1) * step] = jnp.where(
            lane < limit, 1.0 - jnp.sum(found, axis=0, keepdims=True), 0.0
        )
        row = lax.broadcasted_iota(jnp.int32, (step, 1), 0) + t * step
        keep_rows[at, :] = jnp.where(
            row < limit, 1.0 - jnp.sum(found.T, axis=1, keepdims=True), 0.0
        )
        stored = jnp.concatenate(
            [jnp.concatenate([pre_out[b, j] for b in range(n)], axis=1) for j in range(heads)],
            axis=0,
        )
        values = jnp.dot(stored, picks, preferred_element_type=jnp.float32)
        sequence[t] = values.astype(jnp.bfloat16).reshape(heads, cols, step)
        centered = values - jnp.sum(values, axis=0, keepdims=True) / features
        variance = jnp.sum(centered * centered, axis=0, keepdims=True) / features
        normal = (centered * lax.rsqrt(variance + layer_eps) * slide_col[...]).astype(jnp.bfloat16)
        result = jnp.dot(
            qkv_ref[...].reshape(3 * cols, features), normal, preferred_element_type=jnp.float32
        ).astype(jnp.bfloat16)
        queries[t] = result[:cols]
        key_rows[at, :] = result[cols : 2 * cols].T
        key_cols[:, t * step : (t + 1) * step] = result[cols : 2 * cols]
        value_cols[:, t * step : (t + 1) * step] = result[2 * cols :]
        value_rows[at, :] = result[2 * cols :].T

    def attend_stored():
        query = queries[z]
        row_head = lax.broadcasted_iota(jnp.int32, (cols, 1), 0) // HEAD_DIM
        key_at = lax.broadcasted_iota(jnp.int32, (total_rows, 1), 0)
        query_at = lax.broadcasted_iota(jnp.int32, (1, step), 1) + z * step
        for h in range(head_count):
            own = jnp.where(row_head == h, query, jnp.zeros((), jnp.bfloat16))
            scores = jnp.dot(key_rows[...], own, preferred_element_type=jnp.float32) * factor
            scores = jnp.where(keep_rows[...] > 0.0, scores, masked_score)
            peak = jnp.max(scores, axis=0, keepdims=True)
            weights = jnp.exp(scores - peak) * multiplicity(
                key_at, query_at, hd * head_count + h
            )
            at = slice(h * HEAD_DIM, (h + 1) * HEAD_DIM)
            values = jnp.concatenate(
                [value_cols[at, :], jnp.ones((16, total_rows), jnp.bfloat16)], axis=0
            )
            total = jnp.dot(
                values, weights.astype(jnp.bfloat16), preferred_element_type=jnp.float32
            )
            mass = total[HEAD_DIM : HEAD_DIM + 1]
            mix_old[hd, at, :] = (total[:HEAD_DIM] / mass).astype(jnp.bfloat16)
            mix_mass[hd, h * 8 : (h + 1) * 8, :] = jnp.broadcast_to(peak + jnp.log(mass), (8, step))
        mix_query[hd] = query
        for k in range(1, heads):
            for index, buffer in enumerate((mix_query, mix_mass, mix_old)):
                send(
                    buffer.at[hd],
                    buffer.at[hd],
                    send_mix.at[index],
                    recv_mix.at[index],
                    {"head": head_peer(k)},
                )

    slot = pre_out.at[:, pl.ds(0, 2)]
    remote(slot, slot, send_fan.at[0], recv_mate.at[1], {"head": mate}).wait_recv()
    for t in range(n):
        sequence_step(t)
        if t == 1:
            for r in range(2, blocks_k):
                paced_weights(r)
            embed_copy(across, y, 1, {"head": across}).wait_recv()
            embed_copy(across, y, 2, {"groups": 1 - y}).start()
            embed_copy(across, y, 3, {"head": mate}).start()
        if t in (0, n - 2):
            which, index, event = (z_set, across, 1) if t == 0 else (y_set, across, 5)
            for part_of in range(2):
                token_event(which, index, event, part_of, ((event + 2, {"head": mate}),))
    for k in range(1, heads):
        send(
            wcol_parts.at[head_peer(k)],
            wcol_out.at[hd],
            send_aux.at[0],
            recv_aux.at[0],
            {"head": head_peer(k)},
        )
        send(narrow_ref, sub_out.at[hd], send_aux.at[1], recv_aux.at[1], {"head": head_peer(k)})
    attend_stored()
    for part_of in range(2):
        token_event(d_set, across, 9, part_of, ((11, {"head": mate}),))
    embed_copy(across, 1 - y, 2, {"groups": 1 - y}).wait_recv()
    embed_copy(across, 1 - y, 4, {"head": mate}).start()
    slot = normed.at[pl.ds(0, 3), pl.ds(0, 2)]
    remote(slot, slot, send_tok.at[0], recv_mate.at[0], {"head": mate}).wait_recv()
    whole = wall.at[:, :, :, pl.ds(0, LANES), :]
    pltpu.make_async_copy(whole, whole, local_sem.at[7]).wait()

    def arrived(u):
        r, c = unit(u)
        others = wall.at[r, c, :, pl.ds(0, (n - 1) * LANES), :]
        remote(others, others, send_w.at[0], recv_w.at[u], {"seq": partner}).wait_recv()

    def gathered(r, chosen):
        return jnp.concatenate([wall[r, c, g] for c in chosen for g in range(2)], axis=1)

    def token_block(s, r):
        return jnp.concatenate(
            [
                normed[s, :, :, b * depth + r * LANES : b * depth + (r + 1) * LANES].reshape(
                    rows, LANES
                )
                for b in range(n)
            ],
            axis=1,
        )

    def multiply(r):
        for c in range(blocks_c):
            arrived(r * blocks_c + c)
        w = gathered(r, range(blocks_c))

        for s in range(4):
            value = jnp.dot(token_block(s, r), w, preferred_element_type=jnp.float32)
            if r == 0:
                acc[s] = value
            else:
                acc[s] += value

    def pool():
        r = blocks_k - 1
        for c in range(blocks_c):
            arrived(r * blocks_c + c)
        w = gathered(r, range(blocks_c))
        place = y * n + z
        for other in (1, 0):
            yy = 1 - y if other else y
            for m in range(2):
                s = yy * 2 + m
                value = acc[s] + jnp.dot(token_block(s, r), w, preferred_element_type=jnp.float32)
                for c in range(blocks_c):
                    gate = value[:, 2 * c * LANES : (2 * c + 1) * LANES]
                    raised = value[:, (2 * c + 1) * LANES : (2 * c + 2) * LANES]
                    hidden = (gate / (1.0 + jnp.exp(-gate)) * raised).astype(jnp.bfloat16)
                    hidden = hidden.astype(jnp.float32)
                    for tile in range(tiles):
                        pool_mine[
                            yy, pl.ds(m * tiles + tile, 1), c * LANES : (c + 1) * LANES
                        ] = (
                            jnp.sum(hidden[tile * patch : (tile + 1) * patch], axis=0, keepdims=True)
                            / patch
                        )
            for k in reversed(range(n)):
                if k or other:
                    send(
                        pool_mine.at[yy],
                        pooled.at[place],
                        send_pool.at[0],
                        recv_pool.at[0],
                        {"groups": yy, "seq": ahead(k)},
                    )
        pooled[place] = pool_mine[y]

    for r in range(blocks_k - 1):
        multiply(r)
        if r == 0:
            remote(own_embed, own_embed, send_new.at[0], recv_new.at[0], {"head": mate}).wait_recv()
            for which, event in ((y, 3), (1 - y, 4)):
                embed_copy(beyond, which, event, {"head": mate}).wait_recv()
            for j in range(heads):
                embed_cols[:, j * cols : (j + 1) * cols] = embed_ref[j].T
    pool()

    seen = means.at[pl.ds(0, n - 1)]
    remote(seen, seen, send_mean.at[0], recv_mean.at[0], {"seq": partner}).wait_recv()
    slot = pooled.at[pl.ds(0, 2 * n - 1)]
    remote(slot, slot, send_pool.at[0], recv_pool.at[0], {"seq": partner}).wait_recv()
    loads[1].wait()
    everyone = jnp.concatenate(
        [
            jnp.concatenate(
                [pooled[yy * n + b + m] for m in range(2) for yy in range(2)],
                axis=1,
            )
            for b in range(0, n, 2)
        ],
        axis=0,
    )
    high = everyone.astype(jnp.bfloat16)
    rest = everyone - high.astype(jnp.float32)
    middle = rest.astype(jnp.bfloat16)
    low = (rest - middle.astype(jnp.float32)).astype(jnp.bfloat16)
    product = jnp.dot(
        jnp.concatenate([low, middle, high], axis=0),
        down_ref[...],
        preferred_element_type=jnp.float32,
    )
    local_part = sum(product[i * n * tiles : (i + 1) * n * tiles] for i in range(3))
    here = z * heads + hd
    parts[here] = local_part.astype(jnp.bfloat16)
    for k in reversed(range(n)):
        for j in reversed(range(heads)):
            if k or j:
                send(
                    parts.at[here],
                    parts.at[here],
                    send_part.at[0],
                    recv_part.at[0],
                    {"seq": ahead(k), "head": head_peer(j)},
                )
    for buffer, receives in ((wcol_out, recv_aux.at[0]), (sub_out, recv_aux.at[1])):
        slot = buffer.at[pl.ds(0, heads - 1)]
        remote(slot, slot, send_aux.at[0], receives, {"head": mate}).wait_recv()
    for j in range(heads):
        sub_col[pl.ds(j * cols, cols), :] = column(sub_out[j, 1:2])
    slot = parts.at[pl.ds(0, n * heads - 1)]
    remote(slot, slot, send_part.at[0], recv_part.at[0], {"seq": partner}).wait_recv()
    summed = jnp.concatenate(
        [
            sum(parts[b * heads + j].astype(jnp.float32) for j in range(heads))
            for b in range(n)
        ],
        axis=1,
    )
    average = jnp.concatenate([means[b] for b in range(n)], axis=0)
    feature = normalize(
        average + scale_ref[...].reshape(1, width) * summed, fc_ref[...].reshape(1, width)
    ).astype(jnp.bfloat16)
    shift = jnp.concatenate([sub_out[j, 0:1] for j in range(heads)], axis=1)
    fresh_values = (
        jnp.dot(feature, embed_cols[...], preferred_element_type=jnp.float32) + shift
    ).astype(jnp.bfloat16)
    for j in range(heads):
        new_out[j] = fresh_values[:, j * cols : (j + 1) * cols]
    fresh_values = fresh_values.astype(jnp.float32)

    def peers(buffer, receives):
        slot = buffer.at[pl.ds(0, heads - 1)]
        remote(slot, slot, send_aux.at[0], receives, {"head": mate}).wait_recv()

    normal = normalize(fresh_values, slide_ref[...].reshape(1, features)).astype(jnp.bfloat16)
    new_query, new_key, new_value = [
        jnp.dot(normal, qkv_cols[g], preferred_element_type=jnp.float32).astype(jnp.bfloat16)
        for g in range(3)
    ]
    new_kv[hd, 0] = new_key
    new_kv[hd, 1] = new_value
    for k in range(1, heads):
        send(new_kv.at[hd], new_kv.at[hd], send_kv.at[0], recv_kv.at[0], {"head": head_peer(k)})
    lane_head = lax.broadcasted_iota(jnp.int32, (1, cols), 1) // HEAD_DIM
    nothing = jnp.zeros((), jnp.bfloat16)

    def by_head(rows_in):
        return jnp.concatenate(
            [jnp.where(lane_head == h, rows_in, nothing) for h in range(head_count)], axis=0
        )

    key_at = lax.broadcasted_iota(jnp.int32, (new_count, total_rows), 1)
    placed = jnp.concatenate([fresh[t, :new_count].astype(jnp.float32) for t in range(n)], axis=1)
    new_at = jnp.sum(placed * key_at.astype(jnp.float32), axis=1, keepdims=True).astype(jnp.int32)
    other = lax.broadcasted_iota(jnp.int32, (1, LANES), 1)
    new_lane = jnp.sum(
        jnp.where(other == lax.broadcasted_iota(jnp.int32, (new_count, LANES), 0), new_at, 0),
        axis=0,
        keepdims=True,
    )[:, :new_count]

    many = by_head(new_query)
    scores = jnp.dot(many, key_cols[...], preferred_element_type=jnp.float32) * factor
    scores = jnp.where(keep_cols[...] > 0.0, scores, masked_score)
    recent = dot_rows(many, new_key) * factor
    recent = jnp.where(new_lane < limit, recent, masked_score)
    peak = jnp.maximum(
        jnp.max(scores, axis=1, keepdims=True), jnp.max(recent, axis=1, keepdims=True)
    )
    row_at = jnp.concatenate([new_at] * head_count, axis=0)
    offset = hd * head_count + lax.broadcasted_iota(
        jnp.int32, (head_count * new_count, 1), 0
    ) // new_count
    weights = jnp.exp(scores - peak) * multiplicity(key_at[:1], row_at, offset)
    recent = jnp.exp(recent - peak) * multiplicity(new_lane, row_at, offset)
    mass = jnp.sum(weights, axis=1, keepdims=True) + jnp.sum(recent, axis=1, keepdims=True)
    attended = (
        jnp.dot(
            weights.astype(jnp.bfloat16), value_rows[...], preferred_element_type=jnp.float32
        )
        + jnp.dot(recent.astype(jnp.bfloat16), new_value, preferred_element_type=jnp.float32)
    ) / mass
    new_mix[hd] = sum(
        jnp.where(lane_head == h, attended[h * new_count : (h + 1) * new_count], 0.0)
        for h in range(head_count)
    ).astype(jnp.bfloat16)
    for k in range(1, heads):
        send(new_mix.at[hd], new_mix.at[hd], send_kv.at[1], recv_kv.at[1], {"head": head_peer(k)})

    for index, buffer in enumerate((mix_query, mix_mass, mix_old)):
        peers(buffer, recv_mix.at[index])
    peers(new_kv, recv_kv.at[0])
    query_at = lax.broadcasted_iota(jnp.int32, (1, step), 1) + z * step
    here_fresh = fresh[z, :new_count]
    known = 1.0 - jnp.sum(here_fresh.astype(jnp.float32), axis=0, keepdims=True)
    known = jnp.where(query_at < limit, known, 0.0)
    betas, alphas = [], []
    for j in range(heads):
        scores = (
            jnp.dot(by_head(new_kv[j, 0]), mix_query[j], preferred_element_type=jnp.float32)
            * factor
        )
        scores = jnp.where(row_at < limit, scores, masked_score)
        offset = j * head_count + lax.broadcasted_iota(
            jnp.int32, (head_count * new_count, 1), 0
        ) // new_count
        grouped = (head_count, new_count, step)
        scores = scores.reshape(grouped)
        stored_mass = mix_mass[j].reshape(grouped)
        ceiling = jnp.maximum(jnp.max(scores, axis=1, keepdims=True), stored_mass)
        weights = jnp.exp(scores - ceiling) * multiplicity(row_at, query_at, offset).reshape(grouped)
        old = jnp.exp(stored_mass - ceiling)
        inverse = known / (old + jnp.sum(weights, axis=1, keepdims=True))
        betas.append((weights * inverse).reshape(head_count * new_count, step))
        alphas.append(old * inverse)

    inside_limit = jnp.where(query_at < limit, here_fresh.astype(jnp.float32), 0.0).astype(
        jnp.bfloat16
    )

    def contract(left, right):
        return lax.dot_general(
            left, right, (((0,), (0,)), ((), ())), preferred_element_type=jnp.float32
        )

    pieces = []
    for j in range(heads):
        share_of = jnp.concatenate(
            [
                mix_old[j, h * HEAD_DIM : (h + 1) * HEAD_DIM, :].astype(jnp.float32)
                * alphas[j][h, :1]
                for h in range(head_count)
            ],
            axis=0,
        )
        pieces.append(share_of + contract(by_head(new_kv[j, 1]), betas[j].astype(jnp.bfloat16)))
    branch = sequence[z, hd].astype(jnp.float32) + contract(new_out[hd], here_fresh)
    peers(new_mix, recv_kv.at[1])
    pieces = [piece + contract(new_mix[j], inside_limit) for j, piece in enumerate(pieces)]
    mean = sum(jnp.sum(p, axis=0, keepdims=True) for p in pieces) / features
    square = sum(jnp.sum(p * p, axis=0, keepdims=True) for p in pieces) / features
    scaling = lax.rsqrt(square - mean * mean + layer_eps)
    for j in range(heads):
        gain = sub_col[pl.ds(j * cols, cols), :]
        settled = ((pieces[j] - mean) * scaling * gain).astype(jnp.bfloat16)
        branch += jnp.dot(wcol_out[j], settled, preferred_element_type=jnp.float32)
    out_ref[...] = branch

    def drain(slot, sends):
        remote(slot, slot, sends, recv_new.at[0], {"head": mate}).wait_send()

    drain(normed.at[pl.ds(0, 3)], send_tok.at[0])
    drain(wall.at[:, :, :, pl.ds(0, (n - 1) * LANES), :], send_w.at[0])
    drain(pre_out.at[0, pl.ds(0, 2)], send_pre.at[0])

    @pl.when(inside)
    def _():
        drain(pre_out.at[0, pl.ds(0, 2)], send_pre.at[1])

    drain(pre_out.at[pl.ds(0, 3)], send_fan.at[0])
    drain(wcol_out.at[pl.ds(0, heads - 1)], send_aux.at[0])
    drain(sub_out.at[pl.ds(0, heads - 1)], send_aux.at[1])
    drain(pooled.at[pl.ds(0, 2 * n - 1)], send_pool.at[0])
    drain(means.at[pl.ds(0, n - 1)], send_mean.at[0])
    drain(parts.at[pl.ds(0, n * heads - 1)], send_part.at[0])
    drain(own_embed, send_new.at[0])
    drain(embed_ref.at[pl.ds(0, 2)], send_new.at[1])
    for index, buffer in enumerate((mix_query, mix_mass, mix_old)):
        drain(buffer.at[pl.ds(0, heads - 1)], send_mix.at[index])
    drain(new_kv.at[pl.ds(0, heads - 1)], send_kv.at[0])
    drain(new_mix.at[pl.ds(0, heads - 1)], send_kv.at[1])


def near_body(
    tile_tokens,
    tile_gain,
    w_gate_up,
    w_down,
    layer_scale,
    fc_gain,
    w_embed,
    embed_bias,
    pre_emb,
    tile_order,
    valid_count,
    slide_gain,
    w_qkv,
    sub_gain,
    w_out,
):
    n = lax.axis_size("seq")
    heads = lax.axis_size("head")
    tiles, patch, width = tile_tokens.shape
    depth, hidden_width = w_gate_up.shape[1:]
    rows = tiles * patch
    cols = w_embed.shape[1]
    head_count = cols // HEAD_DIM
    total_rows = tile_order.shape[0]
    block_rows = total_rows // n
    vmem = pl.BlockSpec(memory_space=pltpu.VMEM)
    anywhere = pl.BlockSpec(memory_space=pl.ANY)
    dma = pltpu.SemaphoreType.DMA
    f32, bf16 = jnp.float32, jnp.bfloat16
    quarter = rows // heads
    blocks_k = depth // LANES
    blocks_c = hidden_width // 4 // LANES
    out = pl.pallas_call(
        functools.partial(encode_kernel, tiles),
        out_shape=pltpu.VMEM((cols, block_rows), f32),
        in_specs=[pl.BlockSpec(memory_space=pltpu.SMEM)] + [anywhere] * 14,
        out_specs=vmem,
        scratch_shapes=[
            pltpu.VMEM((width,), f32),
            pltpu.VMEM((width,), f32),
            pltpu.VMEM((width,), f32),
            pltpu.VMEM((cols, block_rows - tiles), bf16),
            pltpu.VMEM((cols, heads * cols), bf16),
            pltpu.VMEM((cols,), f32),
            pltpu.VMEM((cols,), f32),
            pltpu.VMEM((total_rows // LANES, LANES), jnp.int32),
            pltpu.VMEM((heads * cols,), f32),
            pltpu.VMEM((rows, width), bf16),
            pltpu.VMEM(w_down.shape, bf16),
            pltpu.VMEM((heads, cols, width), bf16),
            pltpu.VMEM((3, cols, heads * cols), bf16),
            pltpu.VMEM((3, heads * cols, cols), bf16),
            pltpu.VMEM((width, heads * cols), bf16),
            pltpu.VMEM((heads, cols, cols), bf16),
            pltpu.VMEM((2, cols), f32),
            pltpu.VMEM((cols, block_rows), bf16),
            pltpu.VMEM((n, heads, cols, block_rows), bf16),
            pltpu.VMEM((heads, n * tiles, cols), bf16),
            pltpu.VMEM((heads, cols, cols), bf16),
            pltpu.VMEM((heads, 2, cols), f32),
            pltpu.VMEM((n, heads, cols, block_rows), bf16),
            pltpu.VMEM((n, cols, block_rows), bf16),
            pltpu.VMEM((total_rows, cols), bf16),
            pltpu.VMEM((cols, total_rows), bf16),
            pltpu.VMEM((total_rows, cols), bf16),
            pltpu.VMEM((cols, total_rows), bf16),
            pltpu.VMEM((n, LANES, block_rows), bf16),
            pltpu.VMEM((total_rows, 1), f32),
            pltpu.VMEM((1, total_rows), f32),
            pltpu.VMEM((heads * cols, 1), f32),
            pltpu.VMEM((heads * cols, 1), f32),
            pltpu.VMEM((heads, cols, block_rows), bf16),
            pltpu.VMEM((heads, cols, block_rows), bf16),
            pltpu.VMEM((heads, head_count * 8, block_rows), f32),
            pltpu.VMEM((heads, 2, n * tiles, cols), bf16),
            pltpu.VMEM((heads, n * tiles, cols), bf16),
            pltpu.VMEM((4, heads, quarter, width), bf16),
            pltpu.VMEM((blocks_k, blocks_c, 2, n * LANES, LANES), bf16),
            pltpu.VMEM((4, rows, blocks_c * 2 * LANES), f32),
            pltpu.VMEM((2, 2 * tiles, blocks_c * LANES), f32),
            pltpu.VMEM((2 * n, 2 * tiles, blocks_c * LANES), f32),
            pltpu.VMEM((heads, 1, width), f32),
            pltpu.VMEM((n, tiles, width), f32),
            pltpu.VMEM((n * heads, n * tiles, w_down.shape[1]), bf16),
            dma((17,)),
            dma((1,)),
            dma((6, 2)),
            dma((2,)),
            dma((1,)),
            dma((blocks_k * blocks_c,)),
            dma((2,)),
            dma((n,)),
            dma((1,)),
            dma((n,)),
            dma((2,)),
            dma((2,)),
            dma((1,)),
            dma((1,)),
            dma((1,)),
            dma((1,)),
            dma((1,)),
            dma((1,)),
            dma((2,)),
            dma((5,)),
            dma((3,)),
            dma((3,)),
            dma((2,)),
            dma((2,)),
        ],
        compiler_params=pltpu.CompilerParams(
            collective_id=0, has_side_effects=True, vmem_limit_bytes=58 * 1024 * 1024
        ),
    )(
        valid_count,
        tile_tokens.reshape(rows, width),
        tile_gain,
        layer_scale,
        fc_gain,
        w_gate_up,
        w_down,
        w_embed.T,
        pre_emb.T,
        w_out,
        embed_bias,
        sub_gain,
        tile_order.reshape(total_rows // LANES, LANES),
        slide_gain,
        w_qkv.swapaxes(1, 2),
    )
    return out.T


def body(*args):
    total_rows = args[9].shape[0]
    mesh_fits = all(lax.axis_size(a) == k for a, k in (("groups", 2), ("seq", 4), ("head", 4)))
    if total_rows <= SPAN0 and mesh_fits:
        return near_body(*args)
    return general_body(*args)


def solution(mesh):
    placed = (
        P(("groups", "seq"), None, None),
        P(),
        P(None, "seq", "head"),
        P("head", "seq"),
        P(),
        P(),
        P(None, "head"),
        P("head"),
        P(("groups", "seq"), "head"),
        P("groups"),
        P("groups"),
        P(),
        P(None, None, "head"),
        P("head"),
        P("head", None),
    )
    return jax.shard_map(
        body, mesh=mesh, in_specs=placed, out_specs=P(("groups", "seq"), "head"), check_vma=False
    )
```

```python
import functools
import math

import jax
import jax.numpy as jnp
from jax import lax
from jax.experimental import pallas as pl
from jax.experimental.pallas import tpu as pltpu
from jax.sharding import PartitionSpec as P

DS = 768
HEAD_DIM = 48
SPAN0 = 1024
SPAN1 = 4096
DILATION_SECOND = 4
DILATION_THIRD = 16


layer_eps = 1e-05
masked_score = -1e30


def from_partner(value, axis, bit):
    mask = 2**bit
    pairs = [(source, source ^ mask) for source in range(lax.axis_size(axis))]
    return lax.ppermute(value, axis, pairs)


def normalize(values, gain):
    centered = values - jnp.mean(values, axis=-1, keepdims=True)
    variance = jnp.mean(centered * centered, axis=-1, keepdims=True)
    return centered * lax.rsqrt(variance + layer_eps) * gain


def select_rows(stacked, dilation, offsets):
    group_count, row_count, row_width = stacked.shape
    head_count = offsets.shape[0]
    arranged = stacked.reshape(
        group_count, row_count // dilation, dilation, head_count, row_width // head_count
    )
    choose = jnp.arange(dilation, dtype=jnp.int32)[:, None] == offsets[None, :]
    chosen = jnp.sum(
        jnp.where(choose[None, None, :, :, None], arranged, jnp.zeros((), stacked.dtype)), axis=2
    )
    return chosen.reshape(group_count, row_count // dilation, row_width)


def scatter_rows(attended, log_mass, dilation, offsets):
    query_count, head_count, head_size = attended.shape
    choose = jnp.arange(dilation, dtype=jnp.int32)[:, None] == offsets[None, :]
    spread_out = jnp.where(choose[None, :, :, None], attended[:, None, :, :], 0.0).reshape(
        query_count * dilation, head_count, head_size
    )
    spread_mass = jnp.where(choose[None, :, :], log_mass[:, None, :], masked_score).reshape(
        query_count * dilation, head_count
    )
    selected = jnp.broadcast_to(choose[None, :, :], (query_count, dilation, head_count)).reshape(
        query_count * dilation, head_count
    )
    return (spread_out, spread_mass, selected)


def attend(query_rows, key_rows, value_rows, positions, valid_limit, head_count):
    head_size = query_rows.shape[1] // head_count
    query_heads = query_rows.reshape(query_rows.shape[0], head_count, head_size)
    key_heads = key_rows.reshape(key_rows.shape[0], head_count, head_size)
    value_heads = value_rows.reshape(value_rows.shape[0], head_count, head_size)
    scores = jnp.einsum(
        "qhe,khe->hqk", query_heads, key_heads, preferred_element_type=jnp.float32
    ) / math.sqrt(head_size)
    scores = jnp.where((positions < valid_limit)[:, None, :], scores, masked_score)
    highest = jnp.max(scores, axis=-1, keepdims=True)
    exponent = jnp.exp(scores - highest)
    mass_sum = jnp.sum(exponent, axis=-1, keepdims=True)
    weights = (exponent / mass_sum).astype(jnp.bfloat16)
    attended = jnp.einsum("hqk,khe->qhe", weights, value_heads, preferred_element_type=jnp.float32)
    return (attended, (highest[..., 0] + jnp.log(mass_sum[..., 0])).T)


def general_body(
    tile_tokens,
    tile_gain,
    w_gate_up,
    w_down,
    layer_scale,
    fc_gain,
    w_embed,
    embed_bias,
    pre_emb,
    tile_order,
    valid_count,
    slide_gain,
    w_qkv,
    sub_gain,
    w_out,
):
    new_count, patch_count, tile_width = tile_tokens.shape
    token_rows = tile_tokens.reshape(new_count * patch_count, tile_width)
    normed = normalize(token_rows.astype(jnp.float32), tile_gain).astype(jnp.bfloat16)
    hidden_width = w_gate_up.shape[2]
    gate_up = jnp.einsum(
        "rk,gkf->grf",
        normed,
        lax.all_gather(w_gate_up, "seq", axis=1, tiled=True),
        preferred_element_type=jnp.float32,
    )
    hidden = (jax.nn.silu(gate_up[0]) * gate_up[1]).astype(jnp.bfloat16)
    pooled_hidden = jnp.mean(
        hidden.reshape(new_count, patch_count, hidden_width), axis=1, dtype=jnp.float32
    )
    everyone = lax.all_gather(pooled_hidden, "seq", axis=0, tiled=True)
    local_part = jnp.dot(everyone, w_down.astype(jnp.float32), precision=lax.Precision.HIGHEST)
    pooled_part = lax.all_to_all(local_part, "seq", split_axis=0, concat_axis=1, tiled=True)
    summed = lax.psum(pooled_part, "head")
    pooled = jnp.mean(tile_tokens, axis=1, dtype=jnp.float32) + layer_scale * summed
    feature = normalize(pooled, fc_gain).astype(jnp.bfloat16)
    new_rows = (jnp.dot(feature, w_embed, preferred_element_type=jnp.float32) + embed_bias).astype(
        jnp.bfloat16
    )
    stored = jnp.concatenate([new_rows, pre_emb], axis=0)
    block_rows = stored.shape[0]
    total_rows = tile_order.shape[0]
    peer_rows = block_rows // lax.axis_size("seq")
    device = lax.axis_index("seq")
    local_index = jnp.arange(block_rows, dtype=jnp.int32)
    inverse = (
        jnp.zeros((total_rows,), jnp.int32)
        .at[tile_order]
        .set(jnp.arange(total_rows, dtype=jnp.int32))
    )
    placed = lax.dynamic_slice_in_dim(inverse, device * block_rows, block_rows)
    target = placed // block_rows
    before = (target[:, None] == target[None, :]) & (placed[None, :] < placed[:, None])
    slot_index = target * peer_rows + jnp.sum(before, axis=1, dtype=jnp.int32)
    routing = (slot_index[None, :] == local_index[:, None]).astype(jnp.bfloat16)
    outgoing = jnp.dot(routing, stored, preferred_element_type=jnp.float32).astype(jnp.bfloat16)
    incoming = lax.all_to_all(outgoing, "seq", split_axis=0, concat_axis=0, tiled=True)
    wanted = lax.dynamic_slice_in_dim(tile_order, device * block_rows, block_rows)
    source = wanted // block_rows
    earlier = (source[:, None] == source[None, :]) & (local_index[None, :] < local_index[:, None])
    arrival = source * peer_rows + jnp.sum(earlier, axis=1, dtype=jnp.int32)
    own_part = jnp.take(incoming, arrival, axis=0)
    sequence = lax.all_gather(own_part, "head", axis=1, tiled=True)
    slide_normed = normalize(sequence.astype(jnp.float32), slide_gain).astype(jnp.bfloat16)
    projected_rows = jnp.einsum(
        "rd,gdc->grc", slide_normed, w_qkv, preferred_element_type=jnp.float32
    ).astype(jnp.bfloat16)
    cols_here = projected_rows.shape[2]
    head_count = cols_here // HEAD_DIM
    head_indices = lax.axis_index("head") * head_count + jnp.arange(head_count, dtype=jnp.int32)
    valid_limit = valid_count[0]
    row_index = device * block_rows + local_index
    near_devices = min(SPAN0, total_rows) // block_rows
    near_rows = projected_rows[1:]
    for bit_index in range(near_devices.bit_length() - 1):
        partner = from_partner(near_rows, "seq", bit_index)
        upper_half = device // (1 << bit_index) % 2 == 1
        near_rows = jnp.where(
            upper_half,
            jnp.concatenate([partner, near_rows], 1),
            jnp.concatenate([near_rows, partner], 1),
        )
    near_start = device // near_devices * near_devices * block_rows
    near_pos = jnp.broadcast_to(
        near_start + jnp.arange(near_rows.shape[1], dtype=jnp.int32),
        (head_count, near_rows.shape[1]),
    )
    near_out, near_mass = attend(
        projected_rows[0], near_rows[0], near_rows[1], near_pos, valid_limit, head_count
    )
    near_sel = jnp.ones((block_rows, head_count), dtype=bool)
    middle_level_offsets = head_indices % DILATION_SECOND
    middle_level = select_rows(projected_rows, DILATION_SECOND, middle_level_offsets)
    middle_devices = min(SPAN1, total_rows) // block_rows
    middle_key_value = middle_level[1:]
    every_row = lax.all_gather(middle_key_value, "seq", axis=1, tiled=True)
    group_rows = middle_devices * middle_key_value.shape[1]
    middle_key_value = lax.dynamic_slice_in_dim(
        every_row, device // middle_devices * group_rows, group_rows, 1
    )
    middle_start = device // middle_devices * middle_devices * block_rows
    middle_pos = (
        middle_start
        + middle_level_offsets[:, None]
        + DILATION_SECOND * jnp.arange(middle_key_value.shape[1], dtype=jnp.int32)[None, :]
    )
    middle_attention, middle_log_sum = attend(
        middle_level[0],
        middle_key_value[0],
        middle_key_value[1],
        middle_pos,
        valid_limit,
        head_count,
    )
    middle_output, middle_level_mass, middle_selected = scatter_rows(
        middle_attention, middle_log_sum, DILATION_SECOND, middle_level_offsets
    )
    distant_offsets = head_indices % DILATION_THIRD
    distant_local_rows = select_rows(projected_rows, DILATION_THIRD, distant_offsets)
    distant_key_value = lax.all_gather(distant_local_rows[1:], "seq", axis=1, tiled=True)
    distant_positions = (
        distant_offsets[:, None]
        + DILATION_THIRD * jnp.arange(distant_key_value.shape[1], dtype=jnp.int32)[None, :]
    )
    distant_attention, distant_log_sum = attend(
        distant_local_rows[0],
        distant_key_value[0],
        distant_key_value[1],
        distant_positions,
        valid_limit,
        head_count,
    )
    distant_output, distant_mass, distant_selected = scatter_rows(
        distant_attention, distant_log_sum, DILATION_THIRD, distant_offsets
    )
    outputs = jnp.stack([near_out, middle_output, distant_output])
    masses = jnp.stack([near_mass, middle_level_mass, distant_mass])
    selects = jnp.stack([near_sel, middle_selected, distant_selected])
    ceiling = jnp.max(masses, axis=0)
    shares = jnp.where(selects, jnp.exp(masses - ceiling), 0.0)
    combined = jnp.sum(shares[..., None] * outputs, axis=0) / jnp.sum(shares, axis=0)[..., None]
    combined = jnp.where((row_index < valid_limit)[:, None, None], combined, 0.0).reshape(
        block_rows, cols_here
    )
    row_total, row_square = lax.psum(
        (jnp.sum(combined, axis=1), jnp.sum(combined * combined, axis=1)), "head"
    )
    mean_value = row_total / DS
    mean_square = row_square / DS
    scaling = lax.rsqrt(mean_square - mean_value * mean_value + layer_eps)
    settled = ((combined - mean_value[:, None]) * scaling[:, None] * sub_gain).astype(jnp.bfloat16)
    partial_rows = jnp.dot(settled, w_out, preferred_element_type=jnp.float32)
    branch_sum = lax.psum_scatter(partial_rows, "head", scatter_dimension=1, tiled=True)
    return own_part.astype(jnp.float32) + branch_sum


MESH = pl.DeviceIdType.MESH
LANES = 128


def remote(src, dst, send_sem, recv_sem, device):
    return pltpu.make_async_remote_copy(
        src_ref=src,
        dst_ref=dst,
        send_sem=send_sem,
        recv_sem=recv_sem,
        device_id=device,
        device_id_type=MESH,
    )


def dot_rows(left, right):
    return lax.dot_general(
        left, right, (((1,), (1,)), ((), ())), preferred_element_type=jnp.float32
    )


def encode_kernel(
    tiles,
    valid_ref,
    tok_hbm,
    gain_hbm,
    scale_hbm,
    fc_hbm,
    w_hbm,
    down_hbm,
    embed_hbm,
    pre_hbm,
    wcol_hbm,
    bias_hbm,
    sub_hbm,
    order_hbm,
    slide_hbm,
    qkv_hbm,
    out_ref,
    gain_ref,
    scale_ref,
    fc_ref,
    pre_ref,
    wcol_ref,
    bias_ref,
    sub_ref,
    order_ref,
    slide_ref,
    tok_ref,
    down_ref,
    embed_ref,
    qkv_ref,
    qkv_cols,
    embed_cols,
    wcol_parts,
    narrow_ref,
    pre_own,
    pre_out,
    new_out,
    wcol_out,
    sub_out,
    sequence,
    queries,
    key_rows,
    key_cols,
    value_rows,
    value_cols,
    fresh,
    keep_rows,
    keep_cols,
    slide_col,
    sub_col,
    mix_old,
    mix_query,
    mix_mass,
    new_kv,
    new_mix,
    normed,
    wall,
    acc,
    pool_mine,
    pooled,
    sums,
    means,
    mean_in,
    averages,
    parts,
    local_sem,
    send_tok,
    recv_tok,
    recv_mate,
    send_w,
    recv_w,
    send_pre,
    recv_pre,
    send_fan,
    recv_fan,
    send_aux,
    recv_aux,
    send_pool,
    recv_pool,
    send_mean,
    recv_mean,
    send_part,
    recv_part,
    send_new,
    recv_new,
    send_mix,
    recv_mix,
    send_kv,
    recv_kv,
):
    n = lax.axis_size("seq")
    heads = lax.axis_size("head")
    z = lax.axis_index("seq")
    hd = lax.axis_index("head")
    y = lax.axis_index("groups")
    rows, width = tok_hbm.shape
    patch = rows // tiles
    depth, hidden_width = w_hbm.shape[1:]
    quarter = rows // heads
    share = hidden_width // 4
    blocks_k = depth // LANES
    blocks_c = share // LANES
    narrow = wcol_hbm.shape[0]

    part = lax.rem(z, 2)
    pair = z // 2
    partner = z + 1 - 2 * part
    at_end = (z == 0) | (z == n - 1)
    inside = jnp.logical_not(at_end)
    inner = n - 1 - z
    outward = jnp.where(z < 2, 0, n - 1)
    toward = jnp.where(z < 2, 1, n - 1)
    across = lax.rem(hd + 2, heads)
    mate = hd + 1 - 2 * lax.rem(hd, 2)
    beyond = lax.rem(mate + 2, heads)

    def seq_peer(k):
        return lax.rem(z + k, n)

    def ahead(k):
        return lax.rem(z + k * toward, n)

    def head_peer(k):
        return lax.rem(hd + k, heads)

    def head_source(k):
        return lax.rem(hd + heads - k, heads)

    def quarter_rows(index):
        return pl.ds(pl.multiple_of(index * quarter, quarter), quarter)

    def unit(u):
        return u // blocks_c, u % blocks_c

    def weight_block(owner, u):
        r, c = unit(u)
        place = (lax.rem(owner, 2) * 2 + y) * share + c * LANES
        return w_hbm.at[
            :, pl.ds(r * LANES, LANES), pl.ds(pl.multiple_of(place, LANES), LANES)
        ]

    def wall_block(source, u):
        r, c = unit(u)
        return wall.at[r, c, :, pl.ds(pl.multiple_of(source * LANES, LANES), LANES), :]

    units = blocks_k * blocks_c
    half = quarter // 2
    first_quarters = (hd, across, mate, beyond)
    token_loads = [
        pltpu.make_async_copy(
            tok_hbm.at[quarter_rows(q)], tok_ref.at[quarter_rows(q)], local_sem.at[i]
        )
        for i, q in enumerate(first_quarters)
    ]
    loads = [
        pltpu.make_async_copy(source, target, local_sem.at[4 + i])
        for i, (source, target) in enumerate(
            ((qkv_hbm, qkv_ref), (down_hbm, down_ref), (embed_hbm, embed_ref.at[hd]))
        )
    ]
    weight_loads = [
        pltpu.make_async_copy(weight_block(z, u), wall_block(z, u), local_sem.at[7])
        for u in range(units)
    ]
    barrier = pltpu.get_barrier_semaphore()
    count = 0
    for k in range(n):
        for j in range(heads):
            if k or j:
                pl.semaphore_signal(
                    barrier,
                    inc=1,
                    device_id={"seq": seq_peer(k), "head": head_peer(j)},
                    device_id_type=MESH,
                )
                count += 1
    for k in range(n):
        pl.semaphore_signal(
            barrier, inc=1, device_id={"groups": 1 - y, "seq": seq_peer(k)}, device_id_type=MESH
        )
        count += 1
    small_loads = [
        pltpu.make_async_copy(source, target, local_sem.at[8 + i])
        for i, (source, target) in enumerate(
            (
                (pre_hbm, pre_ref),
                (gain_hbm, gain_ref),
                (scale_hbm, scale_ref),
                (fc_hbm, fc_ref),
                (wcol_hbm, wcol_ref),
                (bias_hbm, bias_ref),
                (sub_hbm, sub_ref),
                (order_hbm, order_ref),
                (slide_hbm, slide_ref),
            )
        )
    ]
    for load in token_loads[:1] + small_loads + token_loads[1:] + weight_loads + loads:
        load.start()

    block = 64

    def norm_quarter(position):
        index = first_quarters[position]
        token_loads[position].wait()

        def norm_rows(i, total):
            at = pl.ds(pl.multiple_of(index * quarter + i * block, block), block)
            values = tok_ref[at, :].astype(jnp.float32)
            out = normalize(values, gain_ref[...].reshape(1, width)).astype(jnp.bfloat16)
            normed[y * 2 + part, index, pl.ds(pl.multiple_of(i * block, block), block), :] = out
            return total + jnp.sum(values, axis=0, keepdims=True)

        sums[index] = lax.fori_loop(
            0, quarter // block, norm_rows, jnp.zeros((1, width), jnp.float32)
        )

    cols, stored_count = pre_hbm.shape
    stored_rows = stored_count + tiles
    small_loads[0].wait()
    small_loads[1].wait()
    pre_own[...] = jnp.concatenate(
        [pre_ref[...], jnp.zeros((cols, tiles), jnp.bfloat16)], axis=1
    )

    @pl.when(z < 2)
    def _():
        norm_quarter(0)

    pl.semaphore_wait(barrier, count)

    def send(source, target, sends, receives, device):
        remote(source, target, sends, receives, device).start()

    def send_weight(k, u):
        target = ahead(k)
        send(
            weight_block(target, u), wall_block(z, u), send_w.at[0], recv_w.at[u], {"seq": target}
        )

    def end_weights(r):
        for c in range(blocks_c):
            send_weight(1, r * blocks_c + c)
            send_weight(3, r * blocks_c + c)

    def paced_weights(r):
        @pl.when(at_end)
        def _():
            end_weights(r)

        @pl.when(inside)
        def _():
            for c in range(blocks_c):
                send_weight(2, r * blocks_c + c)

    own_set = y * 2 + part
    z_set = y * 2 + 1 - part
    y_set = (1 - y) * 2 + part
    d_set = (1 - y) * 2 + 1 - part

    def token_copy(which, index, event, part_of, device):
        slot = normed.at[which, index, pl.ds(part_of * half, half)]
        receives = recv_mate.at[0] if event % 4 > 1 else recv_tok.at[event // 4 * 2 + event % 4, part_of]
        return remote(slot, slot, send_tok.at[0], receives, device)

    def fan_copy(block_index, share_index, event, device):
        slot = pre_out.at[block_index, share_index]
        receives = recv_mate.at[1] if event else recv_fan.at[block_index]
        return remote(slot, slot, send_fan.at[0], receives, device)

    for index in range(2):
        target = jnp.where(
            at_end,
            jnp.where(z == 0, 1 + index, n - 2 - index),
            outward if index == 0 else inner,
        )
        send(pre_own, pre_out.at[z, hd], send_pre.at[0], recv_pre.at[z], {"seq": target})

    @pl.when(z >= 2)
    def _():
        norm_quarter(0)

    token_copy(own_set, hd, 0, 0, {"seq": partner}).start()
    for part_of in range(2):
        token_copy(own_set, hd, 4, part_of, {"groups": 1 - y}).start()

    @pl.when(at_end)
    def _():
        token_copy(own_set, hd, 0, 1, {"seq": partner}).start()

    @pl.when(at_end)
    def _():
        for u in range(units):
            send_weight(2, u)
        end_weights(0)

    @pl.when(inside)
    def _():
        for u in range(units):
            send_weight(1, u)

    cols_half = cols // 2

    def embed_half(owner, which):
        return embed_ref.at[
            owner, pl.ds(pl.multiple_of(which * cols_half, cols_half), cols_half)
        ]

    def embed_copy(owner, which, event, device):
        slot = embed_half(owner, which)
        return remote(slot, slot, send_new.at[1], recv_new.at[event], device)

    loads[2].wait()
    own_embed = embed_ref.at[hd]
    send(own_embed, own_embed, send_new.at[0], recv_new.at[0], {"head": mate})
    embed_copy(hd, y, 1, {"head": across}).start()
    pre_out[z, hd] = pre_own[...]
    norm_quarter(1)

    def fan_first(b):
        fan_copy(b, hd, 0, {"head": across}).start()
        fan_copy(b, hd, 1, {"head": mate}).start()

    def fan_second(b):
        fan_copy(b, across, 0, {"head": across}).wait_recv()
        fan_copy(b, across, 2, {"head": mate}).start()

    def stored_block(b, forward=False):
        slot = pre_out.at[b, hd]
        remote(slot, slot, send_pre.at[0], recv_pre.at[b], {"seq": partner}).wait_recv()
        if forward:
            send(slot, slot, send_pre.at[1], recv_pre.at[b], {"seq": outward})
        fan_first(b)

    fan_first(z)
    second_end = jnp.where(z == 0, 2, n - 3)

    @pl.when(at_end)
    def _():
        stored_block(partner)

    @pl.when(inside)
    def _():
        stored_block(inner, True)
        token_copy(own_set, hd, 0, 1, {"seq": partner}).start()
        stored_block(outward)

    norm_quarter(2)
    norm_quarter(3)
    for tile in range(tiles):
        per = heads // tiles
        means[pl.ds(tile, 1), :] = sum(sums[tile * per + i] for i in range(per)) / patch
    def mean_columns(owner):
        return pl.ds(pl.multiple_of(owner * depth, LANES), depth)

    averages[...] = jnp.zeros(averages.shape, jnp.float32)

    @pl.when(hd == 0)
    def _():
        averages[z] = means[:, mean_columns(z)]
        for k in range(1, n):
            target = seq_peer(k)
            send(
                means.at[:, mean_columns(target)],
                mean_in.at[z],
                send_mean.at[0],
                recv_mean.at[0],
                {"seq": target},
            )

    for load in small_loads[2:]:
        load.wait()
    narrow_ref[pl.ds(0, 1), :] = bias_ref[...].reshape(1, narrow)
    narrow_ref[pl.ds(1, 1), :] = sub_ref[...].reshape(1, narrow)
    for j in range(heads):
        wcol_parts[j] = wcol_ref[:, j * narrow : (j + 1) * narrow].T
    wcol_out[hd] = wcol_parts[hd]
    sub_out[hd] = narrow_ref[...]

    def column(row):
        size = row.shape[1]
        same = lax.broadcasted_iota(jnp.int32, (size, size), 0) == lax.broadcasted_iota(
            jnp.int32, (size, size), 1
        )
        return jnp.sum(jnp.where(same, row, 0.0), axis=1, keepdims=True)

    loads[0].wait()
    for g in range(3):
        qkv_cols[g] = qkv_ref[g].T
    features = heads * cols
    for start in range(0, features, LANES):
        at = pl.ds(start, LANES)
        slide_col[at, :] = column(slide_ref[...].reshape(1, features)[:, start : start + LANES])

    def token_event(which, index, event, part_of, forwards):
        token_copy(which, index, event, part_of, {"head": mate}).wait_recv()
        for to, device in forwards:
            token_copy(which, index, to, part_of, device).start()

    from_z = ((8, {"groups": 1 - y}), (1, {"head": across}), (2, {"head": mate}))
    token_event(y_set, hd, 4, 0, ((6, {"head": mate}),))

    @pl.when(inside)
    def _():
        stored_block(n - 1 - outward, True)

    token_event(z_set, hd, 0, 0, from_z)
    token_event(y_set, hd, 4, 1, ((6, {"head": mate}),))

    @pl.when(at_end)
    def _():
        stored_block(second_end)

    token_event(z_set, hd, 0, 1, (from_z[0], from_z[2]))
    for part_of in range(2):
        token_copy(own_set, across, 5, part_of, {"groups": 1 - y}).start()

    @pl.when(at_end)
    def _():
        stored_block(n - 1 - z)

    @pl.when(inside)
    def _():
        for u in range(units):
            send_weight(3, u)

    fan_second(z)

    @pl.when(at_end)
    def _():
        fan_second(partner)
        fan_second(second_end)

    @pl.when(inside)
    def _():
        fan_second(inner)
        fan_second(outward)
        for c in range(blocks_c):
            send_weight(2, c)

    token_copy(z_set, hd, 1, 1, {"head": across}).start()
    for part_of in range(2):
        token_event(d_set, hd, 8, part_of, ((9, {"head": across}), (10, {"head": mate})))
    paced_weights(1)
    fan_second(jnp.where(at_end, n - 1 - z, n - 1 - outward))
    step = stored_rows
    total_rows = n * step
    limit = valid_ref[0]
    new_count = n * tiles
    factor = 1.0 / math.sqrt(HEAD_DIM)
    head_count = cols // HEAD_DIM

    def multiplicity(first, second, offset):
        middle = (first % DILATION_SECOND == offset % DILATION_SECOND) & (
            second % DILATION_SECOND == offset % DILATION_SECOND
        )
        distant = (first % DILATION_THIRD == offset % DILATION_THIRD) & (
            second % DILATION_THIRD == offset % DILATION_THIRD
        )
        return 1.0 + jnp.where(middle, 1.0, 0.0) + jnp.where(distant, 1.0, 0.0)

    def sequence_step(t):
        at = pl.ds(t * step, step)
        per = step // LANES
        order = jnp.concatenate([order_ref[pl.ds(t * per + i, 1), :] for i in range(per)], axis=1)
        label = lax.broadcasted_iota(jnp.int32, (step, step), 0)
        label = jnp.where(label < stored_count, label + tiles, -n * step)
        picks = jnp.concatenate(
            [jnp.where(order == label + b * step, 1.0, 0.0).astype(jnp.bfloat16) for b in range(n)],
            axis=0,
        )
        label = lax.broadcasted_iota(jnp.int32, (LANES, step), 0)
        wanted = jnp.where(label < new_count, label // tiles * step + label % tiles, -1)
        found = jnp.where(order == wanted, 1.0, 0.0)
        fresh[t] = found.astype(jnp.bfloat16)
        lane = lax.broadcasted_iota(jnp.int32, (1, step), 1) + t * step
        keep_cols[:, t * step : (t + 1) * step] = jnp.where(
            lane < limit, 1.0 - jnp.sum(found, axis=0, keepdims=True), 0.0
        )
        row = lax.broadcasted_iota(jnp.int32, (step, 1), 0) + t * step
        keep_rows[at, :] = jnp.where(
            row < limit, 1.0 - jnp.sum(found.T, axis=1, keepdims=True), 0.0
        )
        stored = jnp.concatenate(
            [jnp.concatenate([pre_out[b, j] for b in range(n)], axis=1) for j in range(heads)],
            axis=0,
        )
        values = jnp.dot(stored, picks, preferred_element_type=jnp.float32)
        sequence[t] = values.astype(jnp.bfloat16).reshape(heads, cols, step)
        centered = values - jnp.sum(values, axis=0, keepdims=True) / features
        variance = jnp.sum(centered * centered, axis=0, keepdims=True) / features
        normal = (centered * lax.rsqrt(variance + layer_eps) * slide_col[...]).astype(jnp.bfloat16)
        result = jnp.dot(
            qkv_ref[...].reshape(3 * cols, features), normal, preferred_element_type=jnp.float32
        ).astype(jnp.bfloat16)
        queries[t] = result[:cols]
        key_rows[at, :] = result[cols : 2 * cols].T
        key_cols[:, t * step : (t + 1) * step] = result[cols : 2 * cols]
        value_cols[:, t * step : (t + 1) * step] = result[2 * cols :]
        value_rows[at, :] = result[2 * cols :].T

    def attend_stored():
        query = queries[z]
        row_head = lax.broadcasted_iota(jnp.int32, (cols, 1), 0) // HEAD_DIM
        key_at = lax.broadcasted_iota(jnp.int32, (total_rows, 1), 0)
        query_at = lax.broadcasted_iota(jnp.int32, (1, step), 1) + z * step
        for h in range(head_count):
            own = jnp.where(row_head == h, query, jnp.zeros((), jnp.bfloat16))
            scores = jnp.dot(key_rows[...], own, preferred_element_type=jnp.float32) * factor
            scores = jnp.where(keep_rows[...] > 0.0, scores, masked_score)
            peak = jnp.max(scores, axis=0, keepdims=True)
            weights = jnp.exp(scores - peak) * multiplicity(
                key_at, query_at, hd * head_count + h
            )
            at = slice(h * HEAD_DIM, (h + 1) * HEAD_DIM)
            values = jnp.concatenate(
                [value_cols[at, :], jnp.ones((16, total_rows), jnp.bfloat16)], axis=0
            )
            total = jnp.dot(
                values, weights.astype(jnp.bfloat16), preferred_element_type=jnp.float32
            )
            mass = total[HEAD_DIM : HEAD_DIM + 1]
            mix_old[hd, at, :] = (total[:HEAD_DIM] / mass).astype(jnp.bfloat16)
            mix_mass[hd, h * 8 : (h + 1) * 8, :] = jnp.broadcast_to(peak + jnp.log(mass), (8, step))
        mix_query[hd] = query
        for k in range(1, heads):
            for index, buffer in enumerate((mix_query, mix_mass, mix_old)):
                send(
                    buffer.at[hd],
                    buffer.at[hd],
                    send_mix.at[index],
                    recv_mix.at[index],
                    {"head": head_peer(k)},
                )

    slot = pre_out.at[:, pl.ds(0, 2)]
    remote(slot, slot, send_fan.at[0], recv_mate.at[1], {"head": mate}).wait_recv()
    for t in range(n):
        sequence_step(t)
        if t == 1:
            for r in range(2, blocks_k):
                paced_weights(r)
            embed_copy(across, y, 1, {"head": across}).wait_recv()
            embed_copy(across, y, 2, {"groups": 1 - y}).start()
            embed_copy(across, y, 3, {"head": mate}).start()
        if t in (0, n - 2):
            which, index, event = (z_set, across, 1) if t == 0 else (y_set, across, 5)
            for part_of in range(2):
                token_event(which, index, event, part_of, ((event + 2, {"head": mate}),))
    for k in range(1, heads):
        send(
            wcol_parts.at[head_peer(k)],
            wcol_out.at[hd],
            send_aux.at[0],
            recv_aux.at[0],
            {"head": head_peer(k)},
        )
        send(narrow_ref, sub_out.at[hd], send_aux.at[1], recv_aux.at[1], {"head": head_peer(k)})
    attend_stored()
    for part_of in range(2):
        token_event(d_set, across, 9, part_of, ((11, {"head": mate}),))
    embed_copy(across, 1 - y, 2, {"groups": 1 - y}).wait_recv()
    embed_copy(across, 1 - y, 4, {"head": mate}).start()
    slot = normed.at[pl.ds(0, 3), pl.ds(0, 2)]
    remote(slot, slot, send_tok.at[0], recv_mate.at[0], {"head": mate}).wait_recv()
    whole = wall.at[:, :, :, pl.ds(0, LANES), :]
    pltpu.make_async_copy(whole, whole, local_sem.at[7]).wait()

    def arrived(u):
        r, c = unit(u)
        others = wall.at[r, c, :, pl.ds(0, (n - 1) * LANES), :]
        remote(others, others, send_w.at[0], recv_w.at[u], {"seq": partner}).wait_recv()

    def gathered(r, chosen):
        return jnp.concatenate([wall[r, c, g] for c in chosen for g in range(2)], axis=1)

    def token_block(s, r):
        return jnp.concatenate(
            [
                normed[s, :, :, b * depth + r * LANES : b * depth + (r + 1) * LANES].reshape(
                    rows, LANES
                )
                for b in range(n)
            ],
            axis=1,
        )

    def multiply(r):
        for c in range(blocks_c):
            arrived(r * blocks_c + c)
        w = gathered(r, range(blocks_c))

        for s in range(4):
            value = jnp.dot(token_block(s, r), w, preferred_element_type=jnp.float32)
            if r == 0:
                acc[s] = value
            else:
                acc[s] += value

    def pool():
        r = blocks_k - 1
        for c in range(blocks_c):
            arrived(r * blocks_c + c)
        w = gathered(r, range(blocks_c))
        place = y * n + z
        for other in (1, 0):
            yy = 1 - y if other else y
            for m in range(2):
                s = yy * 2 + m
                value = acc[s] + jnp.dot(token_block(s, r), w, preferred_element_type=jnp.float32)
                for c in range(blocks_c):
                    gate = value[:, 2 * c * LANES : (2 * c + 1) * LANES]
                    raised = value[:, (2 * c + 1) * LANES : (2 * c + 2) * LANES]
                    hidden = (gate / (1.0 + jnp.exp(-gate)) * raised).astype(jnp.bfloat16)
                    hidden = hidden.astype(jnp.float32)
                    for tile in range(tiles):
                        pool_mine[
                            yy, pl.ds(m * tiles + tile, 1), c * LANES : (c + 1) * LANES
                        ] = (
                            jnp.sum(hidden[tile * patch : (tile + 1) * patch], axis=0, keepdims=True)
                            / patch
                        )
            for k in reversed(range(n)):
                if k or other:
                    send(
                        pool_mine.at[yy],
                        pooled.at[place],
                        send_pool.at[0],
                        recv_pool.at[0],
                        {"groups": yy, "seq": ahead(k)},
                    )
        pooled[place] = pool_mine[y]

    for r in range(blocks_k - 1):
        multiply(r)
        if r == 0:
            remote(own_embed, own_embed, send_new.at[0], recv_new.at[0], {"head": mate}).wait_recv()
            for which, event in ((y, 3), (1 - y, 4)):
                embed_copy(beyond, which, event, {"head": mate}).wait_recv()
            for j in range(heads):
                embed_cols[:, j * cols : (j + 1) * cols] = embed_ref[j].T
    pool()


    @pl.when(hd == 0)
    def _():
        seen = mean_in.at[pl.ds(0, n - 1)]
        remote(seen, seen, send_mean.at[0], recv_mean.at[0], {"seq": partner}).wait_recv()
        for k in range(1, n):
            averages[seq_peer(k)] = mean_in[seq_peer(k)]

    slot = pooled.at[pl.ds(0, 2 * n - 1)]
    remote(slot, slot, send_pool.at[0], recv_pool.at[0], {"seq": partner}).wait_recv()
    loads[1].wait()
    everyone = jnp.concatenate(
        [
            jnp.concatenate(
                [pooled[yy * n + b + m] for m in range(2) for yy in range(2)],
                axis=1,
            )
            for b in range(0, n, 2)
        ],
        axis=0,
    )
    high = everyone.astype(jnp.bfloat16)
    rest = everyone - high.astype(jnp.float32)
    middle = rest.astype(jnp.bfloat16)
    low = (rest - middle.astype(jnp.float32)).astype(jnp.bfloat16)
    product = jnp.dot(
        jnp.concatenate([low, middle, high], axis=0),
        down_ref[...],
        preferred_element_type=jnp.float32,
    )
    local_part = sum(product[i * n * tiles : (i + 1) * n * tiles] for i in range(3))
    local_part = local_part * scale_ref[mean_columns(z)].reshape(1, depth) + jnp.concatenate(
        [averages[b] for b in range(n)], axis=0
    )
    here = z * heads + hd
    parts[here] = local_part.astype(jnp.bfloat16)
    for k in reversed(range(n)):
        for j in reversed(range(heads)):
            if k or j:
                send(
                    parts.at[here],
                    parts.at[here],
                    send_part.at[0],
                    recv_part.at[0],
                    {"seq": ahead(k), "head": head_peer(j)},
                )
    for buffer, receives in ((wcol_out, recv_aux.at[0]), (sub_out, recv_aux.at[1])):
        slot = buffer.at[pl.ds(0, heads - 1)]
        remote(slot, slot, send_aux.at[0], receives, {"head": mate}).wait_recv()
    for j in range(heads):
        sub_col[pl.ds(j * cols, cols), :] = column(sub_out[j, 1:2])
    slot = parts.at[pl.ds(0, n * heads - 1)]
    remote(slot, slot, send_part.at[0], recv_part.at[0], {"seq": partner}).wait_recv()
    summed = jnp.concatenate(
        [
            sum(parts[b * heads + j].astype(jnp.float32) for j in range(heads))
            for b in range(n)
        ],
        axis=1,
    )
    feature = normalize(summed, fc_ref[...].reshape(1, width)).astype(jnp.bfloat16)
    shift = jnp.concatenate([sub_out[j, 0:1] for j in range(heads)], axis=1)
    fresh_values = (
        jnp.dot(feature, embed_cols[...], preferred_element_type=jnp.float32) + shift
    ).astype(jnp.bfloat16)
    for j in range(heads):
        new_out[j] = fresh_values[:, j * cols : (j + 1) * cols]
    fresh_values = fresh_values.astype(jnp.float32)

    def peers(buffer, receives):
        slot = buffer.at[pl.ds(0, heads - 1)]
        remote(slot, slot, send_aux.at[0], receives, {"head": mate}).wait_recv()

    normal = normalize(fresh_values, slide_ref[...].reshape(1, features)).astype(jnp.bfloat16)
    new_query, new_key, new_value = [
        jnp.dot(normal, qkv_cols[g], preferred_element_type=jnp.float32).astype(jnp.bfloat16)
        for g in range(3)
    ]
    new_kv[hd, 0] = new_key
    new_kv[hd, 1] = new_value
    for k in range(1, heads):
        send(new_kv.at[hd], new_kv.at[hd], send_kv.at[0], recv_kv.at[0], {"head": head_peer(k)})
    lane_head = lax.broadcasted_iota(jnp.int32, (1, cols), 1) // HEAD_DIM
    nothing = jnp.zeros((), jnp.bfloat16)

    def by_head(rows_in):
        return jnp.concatenate(
            [jnp.where(lane_head == h, rows_in, nothing) for h in range(head_count)], axis=0
        )

    key_at = lax.broadcasted_iota(jnp.int32, (new_count, total_rows), 1)
    placed = jnp.concatenate([fresh[t, :new_count].astype(jnp.float32) for t in range(n)], axis=1)
    new_at = jnp.sum(placed * key_at.astype(jnp.float32), axis=1, keepdims=True).astype(jnp.int32)
    other = lax.broadcasted_iota(jnp.int32, (1, LANES), 1)
    new_lane = jnp.sum(
        jnp.where(other == lax.broadcasted_iota(jnp.int32, (new_count, LANES), 0), new_at, 0),
        axis=0,
        keepdims=True,
    )[:, :new_count]

    many = by_head(new_query)
    scores = jnp.dot(many, key_cols[...], preferred_element_type=jnp.float32) * factor
    scores = jnp.where(keep_cols[...] > 0.0, scores, masked_score)
    recent = dot_rows(many, new_key) * factor
    recent = jnp.where(new_lane < limit, recent, masked_score)
    peak = jnp.maximum(
        jnp.max(scores, axis=1, keepdims=True), jnp.max(recent, axis=1, keepdims=True)
    )
    row_at = jnp.concatenate([new_at] * head_count, axis=0)
    offset = hd * head_count + lax.broadcasted_iota(
        jnp.int32, (head_count * new_count, 1), 0
    ) // new_count
    weights = jnp.exp(scores - peak) * multiplicity(key_at[:1], row_at, offset)
    recent = jnp.exp(recent - peak) * multiplicity(new_lane, row_at, offset)
    mass = jnp.sum(weights, axis=1, keepdims=True) + jnp.sum(recent, axis=1, keepdims=True)
    attended = (
        jnp.dot(
            weights.astype(jnp.bfloat16), value_rows[...], preferred_element_type=jnp.float32
        )
        + jnp.dot(recent.astype(jnp.bfloat16), new_value, preferred_element_type=jnp.float32)
    ) / mass
    new_mix[hd] = sum(
        jnp.where(lane_head == h, attended[h * new_count : (h + 1) * new_count], 0.0)
        for h in range(head_count)
    ).astype(jnp.bfloat16)
    for k in range(1, heads):
        send(new_mix.at[hd], new_mix.at[hd], send_kv.at[1], recv_kv.at[1], {"head": head_peer(k)})

    for index, buffer in enumerate((mix_query, mix_mass, mix_old)):
        peers(buffer, recv_mix.at[index])
    peers(new_kv, recv_kv.at[0])
    query_at = lax.broadcasted_iota(jnp.int32, (1, step), 1) + z * step
    here_fresh = fresh[z, :new_count]
    known = 1.0 - jnp.sum(here_fresh.astype(jnp.float32), axis=0, keepdims=True)
    known = jnp.where(query_at < limit, known, 0.0)
    betas, alphas = [], []
    for j in range(heads):
        scores = (
            jnp.dot(by_head(new_kv[j, 0]), mix_query[j], preferred_element_type=jnp.float32)
            * factor
        )
        scores = jnp.where(row_at < limit, scores, masked_score)
        offset = j * head_count + lax.broadcasted_iota(
            jnp.int32, (head_count * new_count, 1), 0
        ) // new_count
        grouped = (head_count, new_count, step)
        scores = scores.reshape(grouped)
        stored_mass = mix_mass[j].reshape(grouped)
        ceiling = jnp.maximum(jnp.max(scores, axis=1, keepdims=True), stored_mass)
        weights = jnp.exp(scores - ceiling) * multiplicity(row_at, query_at, offset).reshape(grouped)
        old = jnp.exp(stored_mass - ceiling)
        inverse = known / (old + jnp.sum(weights, axis=1, keepdims=True))
        betas.append((weights * inverse).reshape(head_count * new_count, step))
        alphas.append(old * inverse)

    inside_limit = jnp.where(query_at < limit, here_fresh.astype(jnp.float32), 0.0).astype(
        jnp.bfloat16
    )

    def contract(left, right):
        return lax.dot_general(
            left, right, (((0,), (0,)), ((), ())), preferred_element_type=jnp.float32
        )

    pieces = []
    for j in range(heads):
        share_of = jnp.concatenate(
            [
                mix_old[j, h * HEAD_DIM : (h + 1) * HEAD_DIM, :].astype(jnp.float32)
                * alphas[j][h, :1]
                for h in range(head_count)
            ],
            axis=0,
        )
        pieces.append(share_of + contract(by_head(new_kv[j, 1]), betas[j].astype(jnp.bfloat16)))
    branch = sequence[z, hd].astype(jnp.float32) + contract(new_out[hd], here_fresh)
    peers(new_mix, recv_kv.at[1])
    pieces = [piece + contract(new_mix[j], inside_limit) for j, piece in enumerate(pieces)]
    mean = sum(jnp.sum(p, axis=0, keepdims=True) for p in pieces) / features
    square = sum(jnp.sum(p * p, axis=0, keepdims=True) for p in pieces) / features
    scaling = lax.rsqrt(square - mean * mean + layer_eps)
    for j in range(heads):
        gain = sub_col[pl.ds(j * cols, cols), :]
        settled = ((pieces[j] - mean) * scaling * gain).astype(jnp.bfloat16)
        branch += jnp.dot(wcol_out[j], settled, preferred_element_type=jnp.float32)
    out_ref[...] = branch

    def drain(slot, sends):
        remote(slot, slot, sends, recv_new.at[0], {"head": mate}).wait_send()

    drain(normed.at[pl.ds(0, 3)], send_tok.at[0])
    drain(wall.at[:, :, :, pl.ds(0, (n - 1) * LANES), :], send_w.at[0])
    drain(pre_out.at[0, pl.ds(0, 2)], send_pre.at[0])

    @pl.when(inside)
    def _():
        drain(pre_out.at[0, pl.ds(0, 2)], send_pre.at[1])

    drain(pre_out.at[pl.ds(0, 3)], send_fan.at[0])
    drain(wcol_out.at[pl.ds(0, heads - 1)], send_aux.at[0])
    drain(sub_out.at[pl.ds(0, heads - 1)], send_aux.at[1])
    drain(pooled.at[pl.ds(0, 2 * n - 1)], send_pool.at[0])

    @pl.when(hd == 0)
    def _():
        drain(mean_in.at[pl.ds(0, n - 1)], send_mean.at[0])

    drain(parts.at[pl.ds(0, n * heads - 1)], send_part.at[0])
    drain(own_embed, send_new.at[0])
    drain(embed_ref.at[pl.ds(0, 2)], send_new.at[1])
    for index, buffer in enumerate((mix_query, mix_mass, mix_old)):
        drain(buffer.at[pl.ds(0, heads - 1)], send_mix.at[index])
    drain(new_kv.at[pl.ds(0, heads - 1)], send_kv.at[0])
    drain(new_mix.at[pl.ds(0, heads - 1)], send_kv.at[1])


def near_body(
    tile_tokens,
    tile_gain,
    w_gate_up,
    w_down,
    layer_scale,
    fc_gain,
    w_embed,
    embed_bias,
    pre_emb,
    tile_order,
    valid_count,
    slide_gain,
    w_qkv,
    sub_gain,
    w_out,
):
    n = lax.axis_size("seq")
    heads = lax.axis_size("head")
    tiles, patch, width = tile_tokens.shape
    depth, hidden_width = w_gate_up.shape[1:]
    rows = tiles * patch
    cols = w_embed.shape[1]
    head_count = cols // HEAD_DIM
    total_rows = tile_order.shape[0]
    block_rows = total_rows // n
    vmem = pl.BlockSpec(memory_space=pltpu.VMEM)
    anywhere = pl.BlockSpec(memory_space=pl.ANY)
    dma = pltpu.SemaphoreType.DMA
    f32, bf16 = jnp.float32, jnp.bfloat16
    quarter = rows // heads
    blocks_k = depth // LANES
    blocks_c = hidden_width // 4 // LANES
    out = pl.pallas_call(
        functools.partial(encode_kernel, tiles),
        out_shape=pltpu.VMEM((cols, block_rows), f32),
        in_specs=[pl.BlockSpec(memory_space=pltpu.SMEM)] + [anywhere] * 14,
        out_specs=vmem,
        scratch_shapes=[
            pltpu.VMEM((width,), f32),
            pltpu.VMEM((width,), f32),
            pltpu.VMEM((width,), f32),
            pltpu.VMEM((cols, block_rows - tiles), bf16),
            pltpu.VMEM((cols, heads * cols), bf16),
            pltpu.VMEM((cols,), f32),
            pltpu.VMEM((cols,), f32),
            pltpu.VMEM((total_rows // LANES, LANES), jnp.int32),
            pltpu.VMEM((heads * cols,), f32),
            pltpu.VMEM((rows, width), bf16),
            pltpu.VMEM(w_down.shape, bf16),
            pltpu.VMEM((heads, cols, width), bf16),
            pltpu.VMEM((3, cols, heads * cols), bf16),
            pltpu.VMEM((3, heads * cols, cols), bf16),
            pltpu.VMEM((width, heads * cols), bf16),
            pltpu.VMEM((heads, cols, cols), bf16),
            pltpu.VMEM((2, cols), f32),
            pltpu.VMEM((cols, block_rows), bf16),
            pltpu.VMEM((n, heads, cols, block_rows), bf16),
            pltpu.VMEM((heads, n * tiles, cols), bf16),
            pltpu.VMEM((heads, cols, cols), bf16),
            pltpu.VMEM((heads, 2, cols), f32),
            pltpu.VMEM((n, heads, cols, block_rows), bf16),
            pltpu.VMEM((n, cols, block_rows), bf16),
            pltpu.VMEM((total_rows, cols), bf16),
            pltpu.VMEM((cols, total_rows), bf16),
            pltpu.VMEM((total_rows, cols), bf16),
            pltpu.VMEM((cols, total_rows), bf16),
            pltpu.VMEM((n, LANES, block_rows), bf16),
            pltpu.VMEM((total_rows, 1), f32),
            pltpu.VMEM((1, total_rows), f32),
            pltpu.VMEM((heads * cols, 1), f32),
            pltpu.VMEM((heads * cols, 1), f32),
            pltpu.VMEM((heads, cols, block_rows), bf16),
            pltpu.VMEM((heads, cols, block_rows), bf16),
            pltpu.VMEM((heads, head_count * 8, block_rows), f32),
            pltpu.VMEM((heads, 2, n * tiles, cols), bf16),
            pltpu.VMEM((heads, n * tiles, cols), bf16),
            pltpu.VMEM((4, heads, quarter, width), bf16),
            pltpu.VMEM((blocks_k, blocks_c, 2, n * LANES, LANES), bf16),
            pltpu.VMEM((4, rows, blocks_c * 2 * LANES), f32),
            pltpu.VMEM((2, 2 * tiles, blocks_c * LANES), f32),
            pltpu.VMEM((2 * n, 2 * tiles, blocks_c * LANES), f32),
            pltpu.VMEM((heads, 1, width), f32),
            pltpu.VMEM((tiles, width), f32),
            pltpu.VMEM((n, tiles, depth), f32),
            pltpu.VMEM((n, tiles, depth), f32),
            pltpu.VMEM((n * heads, n * tiles, w_down.shape[1]), bf16),
            dma((17,)),
            dma((1,)),
            dma((6, 2)),
            dma((2,)),
            dma((1,)),
            dma((blocks_k * blocks_c,)),
            dma((2,)),
            dma((n,)),
            dma((1,)),
            dma((n,)),
            dma((2,)),
            dma((2,)),
            dma((1,)),
            dma((1,)),
            dma((1,)),
            dma((1,)),
            dma((1,)),
            dma((1,)),
            dma((2,)),
            dma((5,)),
            dma((3,)),
            dma((3,)),
            dma((2,)),
            dma((2,)),
        ],
        compiler_params=pltpu.CompilerParams(
            collective_id=0, has_side_effects=True, vmem_limit_bytes=58 * 1024 * 1024
        ),
    )(
        valid_count,
        tile_tokens.reshape(rows, width),
        tile_gain,
        layer_scale,
        fc_gain,
        w_gate_up,
        w_down,
        w_embed.T,
        pre_emb.T,
        w_out,
        embed_bias,
        sub_gain,
        tile_order.reshape(total_rows // LANES, LANES),
        slide_gain,
        w_qkv.swapaxes(1, 2),
    )
    return out.T


def body(*args):
    total_rows = args[9].shape[0]
    mesh_fits = all(lax.axis_size(a) == k for a, k in (("groups", 2), ("seq", 4), ("head", 4)))
    if total_rows <= SPAN0 and mesh_fits:
        return near_body(*args)
    return general_body(*args)


def solution(mesh):
    placed = (
        P(("groups", "seq"), None, None),
        P(),
        P(None, "seq", "head"),
        P("head", "seq"),
        P(),
        P(),
        P(None, "head"),
        P("head"),
        P(("groups", "seq"), "head"),
        P("groups"),
        P("groups"),
        P(),
        P(None, None, "head"),
        P("head"),
        P("head", None),
    )
    return jax.shard_map(
        body, mesh=mesh, in_specs=placed, out_specs=P(("groups", "seq"), "head"), check_vma=False
    )
```

```python
import functools
import math

import jax
import jax.numpy as jnp
from jax import lax
from jax.experimental import pallas as pl
from jax.experimental.pallas import tpu as pltpu
from jax.sharding import PartitionSpec as P

DS = 768
HEAD_DIM = 48
SPAN0 = 1024
SPAN1 = 4096
DILATION_SECOND = 4
DILATION_THIRD = 16


layer_eps = 1e-05
masked_score = -1e30


def from_partner(value, axis, bit):
    mask = 2**bit
    pairs = [(source, source ^ mask) for source in range(lax.axis_size(axis))]
    return lax.ppermute(value, axis, pairs)


def normalize(values, gain):
    centered = values - jnp.mean(values, axis=-1, keepdims=True)
    variance = jnp.mean(centered * centered, axis=-1, keepdims=True)
    return centered * lax.rsqrt(variance + layer_eps) * gain


def select_rows(stacked, dilation, offsets):
    group_count, row_count, row_width = stacked.shape
    head_count = offsets.shape[0]
    arranged = stacked.reshape(
        group_count, row_count // dilation, dilation, head_count, row_width // head_count
    )
    choose = jnp.arange(dilation, dtype=jnp.int32)[:, None] == offsets[None, :]
    chosen = jnp.sum(
        jnp.where(choose[None, None, :, :, None], arranged, jnp.zeros((), stacked.dtype)), axis=2
    )
    return chosen.reshape(group_count, row_count // dilation, row_width)


def scatter_rows(attended, log_mass, dilation, offsets):
    query_count, head_count, head_size = attended.shape
    choose = jnp.arange(dilation, dtype=jnp.int32)[:, None] == offsets[None, :]
    spread_out = jnp.where(choose[None, :, :, None], attended[:, None, :, :], 0.0).reshape(
        query_count * dilation, head_count, head_size
    )
    spread_mass = jnp.where(choose[None, :, :], log_mass[:, None, :], masked_score).reshape(
        query_count * dilation, head_count
    )
    selected = jnp.broadcast_to(choose[None, :, :], (query_count, dilation, head_count)).reshape(
        query_count * dilation, head_count
    )
    return (spread_out, spread_mass, selected)


def attend(query_rows, key_rows, value_rows, positions, valid_limit, head_count):
    head_size = query_rows.shape[1] // head_count
    query_heads = query_rows.reshape(query_rows.shape[0], head_count, head_size)
    key_heads = key_rows.reshape(key_rows.shape[0], head_count, head_size)
    value_heads = value_rows.reshape(value_rows.shape[0], head_count, head_size)
    scores = jnp.einsum(
        "qhe,khe->hqk", query_heads, key_heads, preferred_element_type=jnp.float32
    ) / math.sqrt(head_size)
    scores = jnp.where((positions < valid_limit)[:, None, :], scores, masked_score)
    highest = jnp.max(scores, axis=-1, keepdims=True)
    exponent = jnp.exp(scores - highest)
    mass_sum = jnp.sum(exponent, axis=-1, keepdims=True)
    weights = (exponent / mass_sum).astype(jnp.bfloat16)
    attended = jnp.einsum("hqk,khe->qhe", weights, value_heads, preferred_element_type=jnp.float32)
    return (attended, (highest[..., 0] + jnp.log(mass_sum[..., 0])).T)


def general_body(
    tile_tokens,
    tile_gain,
    w_gate_up,
    w_down,
    layer_scale,
    fc_gain,
    w_embed,
    embed_bias,
    pre_emb,
    tile_order,
    valid_count,
    slide_gain,
    w_qkv,
    sub_gain,
    w_out,
):
    new_count, patch_count, tile_width = tile_tokens.shape
    token_rows = tile_tokens.reshape(new_count * patch_count, tile_width)
    normed = normalize(token_rows.astype(jnp.float32), tile_gain).astype(jnp.bfloat16)
    hidden_width = w_gate_up.shape[2]
    gate_up = jnp.einsum(
        "rk,gkf->grf",
        normed,
        lax.all_gather(w_gate_up, "seq", axis=1, tiled=True),
        preferred_element_type=jnp.float32,
    )
    hidden = (jax.nn.silu(gate_up[0]) * gate_up[1]).astype(jnp.bfloat16)
    pooled_hidden = jnp.mean(
        hidden.reshape(new_count, patch_count, hidden_width), axis=1, dtype=jnp.float32
    )
    everyone = lax.all_gather(pooled_hidden, "seq", axis=0, tiled=True)
    local_part = jnp.dot(everyone, w_down.astype(jnp.float32), precision=lax.Precision.HIGHEST)
    pooled_part = lax.all_to_all(local_part, "seq", split_axis=0, concat_axis=1, tiled=True)
    summed = lax.psum(pooled_part, "head")
    pooled = jnp.mean(tile_tokens, axis=1, dtype=jnp.float32) + layer_scale * summed
    feature = normalize(pooled, fc_gain).astype(jnp.bfloat16)
    new_rows = (jnp.dot(feature, w_embed, preferred_element_type=jnp.float32) + embed_bias).astype(
        jnp.bfloat16
    )
    stored = jnp.concatenate([new_rows, pre_emb], axis=0)
    block_rows = stored.shape[0]
    total_rows = tile_order.shape[0]
    peer_rows = block_rows // lax.axis_size("seq")
    device = lax.axis_index("seq")
    local_index = jnp.arange(block_rows, dtype=jnp.int32)
    inverse = (
        jnp.zeros((total_rows,), jnp.int32)
        .at[tile_order]
        .set(jnp.arange(total_rows, dtype=jnp.int32))
    )
    placed = lax.dynamic_slice_in_dim(inverse, device * block_rows, block_rows)
    target = placed // block_rows
    before = (target[:, None] == target[None, :]) & (placed[None, :] < placed[:, None])
    slot_index = target * peer_rows + jnp.sum(before, axis=1, dtype=jnp.int32)
    routing = (slot_index[None, :] == local_index[:, None]).astype(jnp.bfloat16)
    outgoing = jnp.dot(routing, stored, preferred_element_type=jnp.float32).astype(jnp.bfloat16)
    incoming = lax.all_to_all(outgoing, "seq", split_axis=0, concat_axis=0, tiled=True)
    wanted = lax.dynamic_slice_in_dim(tile_order, device * block_rows, block_rows)
    source = wanted // block_rows
    earlier = (source[:, None] == source[None, :]) & (local_index[None, :] < local_index[:, None])
    arrival = source * peer_rows + jnp.sum(earlier, axis=1, dtype=jnp.int32)
    own_part = jnp.take(incoming, arrival, axis=0)
    sequence = lax.all_gather(own_part, "head", axis=1, tiled=True)
    slide_normed = normalize(sequence.astype(jnp.float32), slide_gain).astype(jnp.bfloat16)
    projected_rows = jnp.einsum(
        "rd,gdc->grc", slide_normed, w_qkv, preferred_element_type=jnp.float32
    ).astype(jnp.bfloat16)
    cols_here = projected_rows.shape[2]
    head_count = cols_here // HEAD_DIM
    head_indices = lax.axis_index("head") * head_count + jnp.arange(head_count, dtype=jnp.int32)
    valid_limit = valid_count[0]
    row_index = device * block_rows + local_index
    near_devices = min(SPAN0, total_rows) // block_rows
    near_rows = projected_rows[1:]
    for bit_index in range(near_devices.bit_length() - 1):
        partner = from_partner(near_rows, "seq", bit_index)
        upper_half = device // (1 << bit_index) % 2 == 1
        near_rows = jnp.where(
            upper_half,
            jnp.concatenate([partner, near_rows], 1),
            jnp.concatenate([near_rows, partner], 1),
        )
    near_start = device // near_devices * near_devices * block_rows
    near_pos = jnp.broadcast_to(
        near_start + jnp.arange(near_rows.shape[1], dtype=jnp.int32),
        (head_count, near_rows.shape[1]),
    )
    near_out, near_mass = attend(
        projected_rows[0], near_rows[0], near_rows[1], near_pos, valid_limit, head_count
    )
    near_sel = jnp.ones((block_rows, head_count), dtype=bool)
    middle_level_offsets = head_indices % DILATION_SECOND
    middle_level = select_rows(projected_rows, DILATION_SECOND, middle_level_offsets)
    middle_devices = min(SPAN1, total_rows) // block_rows
    middle_key_value = middle_level[1:]
    every_row = lax.all_gather(middle_key_value, "seq", axis=1, tiled=True)
    group_rows = middle_devices * middle_key_value.shape[1]
    middle_key_value = lax.dynamic_slice_in_dim(
        every_row, device // middle_devices * group_rows, group_rows, 1
    )
    middle_start = device // middle_devices * middle_devices * block_rows
    middle_pos = (
        middle_start
        + middle_level_offsets[:, None]
        + DILATION_SECOND * jnp.arange(middle_key_value.shape[1], dtype=jnp.int32)[None, :]
    )
    middle_attention, middle_log_sum = attend(
        middle_level[0],
        middle_key_value[0],
        middle_key_value[1],
        middle_pos,
        valid_limit,
        head_count,
    )
    middle_output, middle_level_mass, middle_selected = scatter_rows(
        middle_attention, middle_log_sum, DILATION_SECOND, middle_level_offsets
    )
    distant_offsets = head_indices % DILATION_THIRD
    distant_local_rows = select_rows(projected_rows, DILATION_THIRD, distant_offsets)
    distant_key_value = lax.all_gather(distant_local_rows[1:], "seq", axis=1, tiled=True)
    distant_positions = (
        distant_offsets[:, None]
        + DILATION_THIRD * jnp.arange(distant_key_value.shape[1], dtype=jnp.int32)[None, :]
    )
    distant_attention, distant_log_sum = attend(
        distant_local_rows[0],
        distant_key_value[0],
        distant_key_value[1],
        distant_positions,
        valid_limit,
        head_count,
    )
    distant_output, distant_mass, distant_selected = scatter_rows(
        distant_attention, distant_log_sum, DILATION_THIRD, distant_offsets
    )
    outputs = jnp.stack([near_out, middle_output, distant_output])
    masses = jnp.stack([near_mass, middle_level_mass, distant_mass])
    selects = jnp.stack([near_sel, middle_selected, distant_selected])
    ceiling = jnp.max(masses, axis=0)
    shares = jnp.where(selects, jnp.exp(masses - ceiling), 0.0)
    combined = jnp.sum(shares[..., None] * outputs, axis=0) / jnp.sum(shares, axis=0)[..., None]
    combined = jnp.where((row_index < valid_limit)[:, None, None], combined, 0.0).reshape(
        block_rows, cols_here
    )
    row_total, row_square = lax.psum(
        (jnp.sum(combined, axis=1), jnp.sum(combined * combined, axis=1)), "head"
    )
    mean_value = row_total / DS
    mean_square = row_square / DS
    scaling = lax.rsqrt(mean_square - mean_value * mean_value + layer_eps)
    settled = ((combined - mean_value[:, None]) * scaling[:, None] * sub_gain).astype(jnp.bfloat16)
    partial_rows = jnp.dot(settled, w_out, preferred_element_type=jnp.float32)
    branch_sum = lax.psum_scatter(partial_rows, "head", scatter_dimension=1, tiled=True)
    return own_part.astype(jnp.float32) + branch_sum


MESH = pl.DeviceIdType.MESH
LANES = 128


def remote(src, dst, send_sem, recv_sem, device):
    return pltpu.make_async_remote_copy(
        src_ref=src,
        dst_ref=dst,
        send_sem=send_sem,
        recv_sem=recv_sem,
        device_id=device,
        device_id_type=MESH,
    )


def dot_rows(left, right):
    return lax.dot_general(
        left, right, (((1,), (1,)), ((), ())), preferred_element_type=jnp.float32
    )


def encode_kernel(
    tiles,
    valid_ref,
    tok_hbm,
    gain_hbm,
    scale_hbm,
    fc_hbm,
    w_hbm,
    down_hbm,
    embed_hbm,
    pre_hbm,
    wcol_hbm,
    bias_hbm,
    sub_hbm,
    order_hbm,
    slide_hbm,
    qkv_hbm,
    out_ref,
    gain_ref,
    scale_ref,
    fc_ref,
    pre_ref,
    wcol_ref,
    bias_ref,
    sub_ref,
    order_ref,
    slide_ref,
    tok_ref,
    down_ref,
    embed_ref,
    qkv_ref,
    qkv_cols,
    embed_cols,
    wcol_parts,
    narrow_ref,
    pre_own,
    pre_out,
    new_out,
    wcol_out,
    sub_out,
    sequence,
    queries,
    key_rows,
    key_cols,
    value_rows,
    value_cols,
    fresh,
    keep_rows,
    keep_cols,
    slide_col,
    sub_col,
    mix_old,
    mix_query,
    mix_mass,
    new_kv,
    new_mix,
    normed,
    wall,
    acc,
    pool_mine,
    pooled,
    sums,
    means,
    mean_in,
    averages,
    parts,
    local_sem,
    send_tok,
    recv_tok,
    recv_mate,
    send_w,
    recv_w,
    send_pre,
    recv_pre,
    send_fan,
    recv_fan,
    send_aux,
    recv_aux,
    send_pool,
    recv_pool,
    send_mean,
    recv_mean,
    send_part,
    recv_part,
    send_new,
    recv_new,
    send_mix,
    recv_mix,
    send_kv,
    recv_kv,
):
    n = lax.axis_size("seq")
    heads = lax.axis_size("head")
    z = lax.axis_index("seq")
    hd = lax.axis_index("head")
    y = lax.axis_index("groups")
    rows, width = tok_hbm.shape
    patch = rows // tiles
    depth, hidden_width = w_hbm.shape[1:]
    quarter = rows // heads
    share = hidden_width // 4
    blocks_k = depth // LANES
    blocks_c = share // LANES
    narrow = wcol_hbm.shape[0]

    part = lax.rem(z, 2)
    pair = z // 2
    partner = z + 1 - 2 * part
    at_end = (z == 0) | (z == n - 1)
    inside = jnp.logical_not(at_end)
    inner = n - 1 - z
    outward = jnp.where(z < 2, 0, n - 1)
    toward = jnp.where(z < 2, 1, n - 1)
    across = lax.rem(hd + 2, heads)
    mate = hd + 1 - 2 * lax.rem(hd, 2)
    beyond = lax.rem(mate + 2, heads)

    def seq_peer(k):
        return lax.rem(z + k, n)

    def ahead(k):
        return lax.rem(z + k * toward, n)

    def head_peer(k):
        return lax.rem(hd + k, heads)

    def head_source(k):
        return lax.rem(hd + heads - k, heads)

    def quarter_rows(index):
        return pl.ds(pl.multiple_of(index * quarter, quarter), quarter)

    def unit(u):
        return u // blocks_c, u % blocks_c

    def weight_block(owner, u):
        r, c = unit(u)
        place = (lax.rem(owner, 2) * 2 + y) * share + c * LANES
        return w_hbm.at[
            :, pl.ds(r * LANES, LANES), pl.ds(pl.multiple_of(place, LANES), LANES)
        ]

    def wall_block(source, u):
        r, c = unit(u)
        return wall.at[r, c, :, pl.ds(pl.multiple_of(source * LANES, LANES), LANES), :]

    units = blocks_k * blocks_c
    half = quarter // 2
    first_quarters = (hd, across, mate, beyond)
    token_loads = [
        pltpu.make_async_copy(
            tok_hbm.at[quarter_rows(q)], tok_ref.at[quarter_rows(q)], local_sem.at[i]
        )
        for i, q in enumerate(first_quarters)
    ]
    loads = [
        pltpu.make_async_copy(source, target, local_sem.at[4 + i])
        for i, (source, target) in enumerate(
            ((qkv_hbm, qkv_ref), (down_hbm, down_ref), (embed_hbm, embed_ref.at[hd]))
        )
    ]
    weight_loads = [
        pltpu.make_async_copy(weight_block(z, u), wall_block(z, u), local_sem.at[7])
        for u in range(units)
    ]
    barrier = pltpu.get_barrier_semaphore()
    count = 0
    for k in range(n):
        for j in range(heads):
            if k or j:
                pl.semaphore_signal(
                    barrier,
                    inc=1,
                    device_id={"seq": seq_peer(k), "head": head_peer(j)},
                    device_id_type=MESH,
                )
                count += 1
    for k in range(n):
        pl.semaphore_signal(
            barrier, inc=1, device_id={"groups": 1 - y, "seq": seq_peer(k)}, device_id_type=MESH
        )
        count += 1
    small_loads = [
        pltpu.make_async_copy(source, target, local_sem.at[8 + i])
        for i, (source, target) in enumerate(
            (
                (pre_hbm, pre_ref),
                (gain_hbm, gain_ref),
                (scale_hbm, scale_ref),
                (fc_hbm, fc_ref),
                (wcol_hbm, wcol_ref),
                (bias_hbm, bias_ref),
                (sub_hbm, sub_ref),
                (order_hbm, order_ref),
                (slide_hbm, slide_ref),
            )
        )
    ]
    for load in token_loads[:1] + small_loads + token_loads[1:] + weight_loads + loads:
        load.start()

    block = 64

    def norm_quarter(position):
        index = first_quarters[position]
        token_loads[position].wait()

        def norm_rows(i, total):
            at = pl.ds(pl.multiple_of(index * quarter + i * block, block), block)
            values = tok_ref[at, :].astype(jnp.float32)
            out = normalize(values, gain_ref[...].reshape(1, width)).astype(jnp.bfloat16)
            normed[y * 2 + part, index, pl.ds(pl.multiple_of(i * block, block), block), :] = out
            return total + jnp.sum(values, axis=0, keepdims=True)

        sums[index] = lax.fori_loop(
            0, quarter // block, norm_rows, jnp.zeros((1, width), jnp.float32)
        )

    cols, stored_count = pre_hbm.shape
    stored_rows = stored_count + tiles
    small_loads[0].wait()
    small_loads[1].wait()
    pre_own[...] = jnp.concatenate(
        [pre_ref[...], jnp.zeros((cols, tiles), jnp.bfloat16)], axis=1
    )

    @pl.when(z < 2)
    def _():
        norm_quarter(0)

    pl.semaphore_wait(barrier, count)

    def send(source, target, sends, receives, device):
        remote(source, target, sends, receives, device).start()

    def send_weight(k, u):
        target = ahead(k)
        send(
            weight_block(target, u), wall_block(z, u), send_w.at[0], recv_w.at[u], {"seq": target}
        )

    def end_weights(r):
        for c in range(blocks_c):
            send_weight(1, r * blocks_c + c)
            send_weight(3, r * blocks_c + c)

    def paced_weights(r):
        @pl.when(at_end)
        def _():
            end_weights(r)

        @pl.when(inside)
        def _():
            for c in range(blocks_c):
                send_weight(2, r * blocks_c + c)

    own_set = y * 2 + part
    z_set = y * 2 + 1 - part
    y_set = (1 - y) * 2 + part
    d_set = (1 - y) * 2 + 1 - part

    def token_copy(which, index, event, part_of, device):
        slot = normed.at[which, index, pl.ds(part_of * half, half)]
        receives = recv_mate.at[0] if event % 4 > 1 else recv_tok.at[event // 4 * 2 + event % 4, part_of]
        return remote(slot, slot, send_tok.at[0], receives, device)

    def fan_copy(block_index, share_index, event, device):
        slot = pre_out.at[block_index, share_index]
        receives = recv_mate.at[1] if event else recv_fan.at[block_index]
        return remote(slot, slot, send_fan.at[0], receives, device)

    for index in range(2):
        target = jnp.where(
            at_end,
            jnp.where(z == 0, 1 + index, n - 2 - index),
            outward if index == 0 else inner,
        )
        send(pre_own, pre_out.at[z, hd], send_pre.at[0], recv_pre.at[z], {"seq": target})

    @pl.when(z >= 2)
    def _():
        norm_quarter(0)

    token_copy(own_set, hd, 0, 0, {"seq": partner}).start()
    for part_of in range(2):
        token_copy(own_set, hd, 4, part_of, {"groups": 1 - y}).start()

    @pl.when(at_end)
    def _():
        token_copy(own_set, hd, 0, 1, {"seq": partner}).start()

    @pl.when(at_end)
    def _():
        for u in range(units):
            send_weight(2, u)
        end_weights(0)

    @pl.when(inside)
    def _():
        for u in range(units):
            send_weight(1, u)

    cols_half = cols // 2

    def embed_half(owner, which):
        return embed_ref.at[
            owner, pl.ds(pl.multiple_of(which * cols_half, cols_half), cols_half)
        ]

    def embed_copy(owner, which, event, device):
        slot = embed_half(owner, which)
        return remote(slot, slot, send_new.at[1], recv_new.at[event], device)

    loads[2].wait()
    own_embed = embed_ref.at[hd]
    send(own_embed, own_embed, send_new.at[0], recv_new.at[0], {"head": mate})
    embed_copy(hd, y, 1, {"head": across}).start()
    pre_out[z, hd] = pre_own[...]
    norm_quarter(1)

    def fan_first(b):
        fan_copy(b, hd, 0, {"head": across}).start()
        fan_copy(b, hd, 1, {"head": mate}).start()

    def fan_second(b):
        fan_copy(b, across, 0, {"head": across}).wait_recv()
        fan_copy(b, across, 2, {"head": mate}).start()

    def stored_block(b, forward=False):
        slot = pre_out.at[b, hd]
        remote(slot, slot, send_pre.at[0], recv_pre.at[b], {"seq": partner}).wait_recv()
        if forward:
            send(slot, slot, send_pre.at[1], recv_pre.at[b], {"seq": outward})
        fan_first(b)

    fan_first(z)
    second_end = jnp.where(z == 0, 2, n - 3)

    @pl.when(at_end)
    def _():
        stored_block(partner)

    @pl.when(inside)
    def _():
        stored_block(inner, True)
        token_copy(own_set, hd, 0, 1, {"seq": partner}).start()
        stored_block(outward)

    norm_quarter(2)
    norm_quarter(3)
    for tile in range(tiles):
        per = heads // tiles
        means[pl.ds(tile, 1), :] = sum(sums[tile * per + i] for i in range(per)) / patch
    def mean_columns(owner):
        return pl.ds(pl.multiple_of(owner * depth, LANES), depth)

    averages[...] = jnp.zeros(averages.shape, jnp.float32)

    @pl.when(hd == 0)
    def _():
        averages[z] = means[:, mean_columns(z)]
        for k in range(1, n):
            target = seq_peer(k)
            send(
                means.at[:, mean_columns(target)],
                mean_in.at[z],
                send_mean.at[0],
                recv_mean.at[0],
                {"seq": target},
            )

    for load in small_loads[2:]:
        load.wait()
    narrow_ref[pl.ds(0, 1), :] = bias_ref[...].reshape(1, narrow)
    narrow_ref[pl.ds(1, 1), :] = sub_ref[...].reshape(1, narrow)
    for j in range(heads):
        wcol_parts[j] = wcol_ref[:, j * narrow : (j + 1) * narrow].T
    wcol_out[hd] = wcol_parts[hd]
    sub_out[hd] = narrow_ref[...]

    def column(row):
        size = row.shape[1]
        same = lax.broadcasted_iota(jnp.int32, (size, size), 0) == lax.broadcasted_iota(
            jnp.int32, (size, size), 1
        )
        return jnp.sum(jnp.where(same, row, 0.0), axis=1, keepdims=True)

    loads[0].wait()
    for g in range(3):
        qkv_cols[g] = qkv_ref[g].T
    features = heads * cols
    for start in range(0, features, LANES):
        at = pl.ds(start, LANES)
        slide_col[at, :] = column(slide_ref[...].reshape(1, features)[:, start : start + LANES])

    def token_event(which, index, event, part_of, forwards):
        token_copy(which, index, event, part_of, {"head": mate}).wait_recv()
        for to, device in forwards:
            token_copy(which, index, to, part_of, device).start()

    from_z = ((8, {"groups": 1 - y}), (1, {"head": across}), (2, {"head": mate}))
    token_event(y_set, hd, 4, 0, ((6, {"head": mate}),))

    @pl.when(inside)
    def _():
        stored_block(n - 1 - outward, True)

    token_event(z_set, hd, 0, 0, from_z)
    token_event(y_set, hd, 4, 1, ((6, {"head": mate}),))

    @pl.when(at_end)
    def _():
        stored_block(second_end)

    token_event(z_set, hd, 0, 1, (from_z[0], from_z[2]))
    for part_of in range(2):
        token_copy(own_set, across, 5, part_of, {"groups": 1 - y}).start()

    @pl.when(at_end)
    def _():
        stored_block(n - 1 - z)

    @pl.when(inside)
    def _():
        for u in range(units):
            send_weight(3, u)

    fan_second(z)

    @pl.when(at_end)
    def _():
        fan_second(partner)
        fan_second(second_end)

    @pl.when(inside)
    def _():
        fan_second(inner)
        fan_second(outward)
        for c in range(blocks_c):
            send_weight(2, c)

    token_copy(z_set, hd, 1, 1, {"head": across}).start()
    for part_of in range(2):
        token_event(d_set, hd, 8, part_of, ((9, {"head": across}), (10, {"head": mate})))
    paced_weights(1)
    fan_second(jnp.where(at_end, n - 1 - z, n - 1 - outward))
    step = stored_rows
    total_rows = n * step
    limit = valid_ref[0]
    new_count = n * tiles
    factor = 1.0 / math.sqrt(HEAD_DIM)
    head_count = cols // HEAD_DIM

    def multiplicity(first, second, offset):
        middle = (first % DILATION_SECOND == offset % DILATION_SECOND) & (
            second % DILATION_SECOND == offset % DILATION_SECOND
        )
        distant = (first % DILATION_THIRD == offset % DILATION_THIRD) & (
            second % DILATION_THIRD == offset % DILATION_THIRD
        )
        return 1.0 + jnp.where(middle, 1.0, 0.0) + jnp.where(distant, 1.0, 0.0)

    def sequence_step(t):
        at = pl.ds(t * step, step)
        per = step // LANES
        order = jnp.concatenate([order_ref[pl.ds(t * per + i, 1), :] for i in range(per)], axis=1)
        label = lax.broadcasted_iota(jnp.int32, (step, step), 0)
        label = jnp.where(label < stored_count, label + tiles, -n * step)
        picks = jnp.concatenate(
            [jnp.where(order == label + b * step, 1.0, 0.0).astype(jnp.bfloat16) for b in range(n)],
            axis=0,
        )
        label = lax.broadcasted_iota(jnp.int32, (LANES, step), 0)
        wanted = jnp.where(label < new_count, label // tiles * step + label % tiles, -1)
        found = jnp.where(order == wanted, 1.0, 0.0)
        fresh[t] = found.astype(jnp.bfloat16)
        lane = lax.broadcasted_iota(jnp.int32, (1, step), 1) + t * step
        keep_cols[:, t * step : (t + 1) * step] = jnp.where(
            lane < limit, 1.0 - jnp.sum(found, axis=0, keepdims=True), 0.0
        )
        row = lax.broadcasted_iota(jnp.int32, (step, 1), 0) + t * step
        keep_rows[at, :] = jnp.where(
            row < limit, 1.0 - jnp.sum(found.T, axis=1, keepdims=True), 0.0
        )
        stored = jnp.concatenate(
            [jnp.concatenate([pre_out[b, j] for b in range(n)], axis=1) for j in range(heads)],
            axis=0,
        )
        values = jnp.dot(stored, picks, preferred_element_type=jnp.float32)
        sequence[t] = values.astype(jnp.bfloat16).reshape(heads, cols, step)
        centered = values - jnp.sum(values, axis=0, keepdims=True) / features
        variance = jnp.sum(centered * centered, axis=0, keepdims=True) / features
        normal = (centered * lax.rsqrt(variance + layer_eps) * slide_col[...]).astype(jnp.bfloat16)
        result = jnp.dot(
            qkv_ref[...].reshape(3 * cols, features), normal, preferred_element_type=jnp.float32
        ).astype(jnp.bfloat16)
        queries[t] = result[:cols]
        key_rows[at, :] = result[cols : 2 * cols].T
        key_cols[:, t * step : (t + 1) * step] = result[cols : 2 * cols]
        value_cols[:, t * step : (t + 1) * step] = result[2 * cols :]
        value_rows[at, :] = result[2 * cols :].T

    def attend_stored():
        query = queries[z]
        row_head = lax.broadcasted_iota(jnp.int32, (cols, 1), 0) // HEAD_DIM
        key_at = lax.broadcasted_iota(jnp.int32, (total_rows, 1), 0)
        query_at = lax.broadcasted_iota(jnp.int32, (1, step), 1) + z * step
        for h in range(head_count):
            own = jnp.where(row_head == h, query, jnp.zeros((), jnp.bfloat16))
            scores = jnp.dot(key_rows[...], own, preferred_element_type=jnp.float32) * factor
            scores = jnp.where(keep_rows[...] > 0.0, scores, masked_score)
            peak = jnp.max(scores, axis=0, keepdims=True)
            weights = jnp.exp(scores - peak) * multiplicity(
                key_at, query_at, hd * head_count + h
            )
            at = slice(h * HEAD_DIM, (h + 1) * HEAD_DIM)
            values = jnp.concatenate(
                [value_cols[at, :], jnp.ones((16, total_rows), jnp.bfloat16)], axis=0
            )
            total = jnp.dot(
                values, weights.astype(jnp.bfloat16), preferred_element_type=jnp.float32
            )
            mass = total[HEAD_DIM : HEAD_DIM + 1]
            mix_old[hd, at, :] = (total[:HEAD_DIM] / mass).astype(jnp.bfloat16)
            mix_mass[hd, h * 8 : (h + 1) * 8, :] = jnp.broadcast_to(peak + jnp.log(mass), (8, step))
        mix_query[hd] = query
        for k in range(1, heads):
            for index, buffer in enumerate((mix_query, mix_mass, mix_old)):
                send(
                    buffer.at[hd],
                    buffer.at[hd],
                    send_mix.at[index],
                    recv_mix.at[index],
                    {"head": head_peer(k)},
                )

    slot = pre_out.at[:, pl.ds(0, 2)]
    remote(slot, slot, send_fan.at[0], recv_mate.at[1], {"head": mate}).wait_recv()
    for t in range(n):
        sequence_step(t)
        if t == 1:
            for r in range(2, blocks_k):
                paced_weights(r)
            embed_copy(across, y, 1, {"head": across}).wait_recv()
            embed_copy(across, y, 2, {"groups": 1 - y}).start()
            embed_copy(across, y, 3, {"head": mate}).start()
        if t in (0, n - 2):
            which, index, event = (z_set, across, 1) if t == 0 else (y_set, across, 5)
            for part_of in range(2):
                token_event(which, index, event, part_of, ((event + 2, {"head": mate}),))
    for k in range(1, heads):
        send(
            wcol_parts.at[head_peer(k)],
            wcol_out.at[hd],
            send_aux.at[0],
            recv_aux.at[0],
            {"head": head_peer(k)},
        )
        send(narrow_ref, sub_out.at[hd], send_aux.at[1], recv_aux.at[1], {"head": head_peer(k)})
    attend_stored()
    for part_of in range(2):
        token_event(d_set, across, 9, part_of, ((11, {"head": mate}),))
    embed_copy(across, 1 - y, 2, {"groups": 1 - y}).wait_recv()
    embed_copy(across, 1 - y, 4, {"head": mate}).start()
    slot = normed.at[pl.ds(0, 3), pl.ds(0, 2)]
    remote(slot, slot, send_tok.at[0], recv_mate.at[0], {"head": mate}).wait_recv()
    whole = wall.at[:, :, :, pl.ds(0, LANES), :]
    pltpu.make_async_copy(whole, whole, local_sem.at[7]).wait()

    def arrived(u):
        r, c = unit(u)
        others = wall.at[r, c, :, pl.ds(0, (n - 1) * LANES), :]
        remote(others, others, send_w.at[0], recv_w.at[u], {"seq": partner}).wait_recv()

    def gathered(r, chosen):
        return jnp.concatenate([wall[r, c, g] for c in chosen for g in range(2)], axis=1)

    def token_block(s, r):
        return jnp.concatenate(
            [
                normed[s, :, :, b * depth + r * LANES : b * depth + (r + 1) * LANES].reshape(
                    rows, LANES
                )
                for b in range(n)
            ],
            axis=1,
        )

    def multiply(r):
        for c in range(blocks_c):
            arrived(r * blocks_c + c)
        w = gathered(r, range(blocks_c))

        for s in range(4):
            value = jnp.dot(token_block(s, r), w, preferred_element_type=jnp.float32)
            if r == 0:
                acc[s] = value
            else:
                acc[s] += value

    def pool():
        r = blocks_k - 1
        for c in range(blocks_c):
            arrived(r * blocks_c + c)
        w = gathered(r, range(blocks_c))
        place = y * n + z
        for other in (1, 0):
            yy = 1 - y if other else y
            for m in range(2):
                s = yy * 2 + m
                value = acc[s] + jnp.dot(token_block(s, r), w, preferred_element_type=jnp.float32)
                for c in range(blocks_c):
                    gate = value[:, 2 * c * LANES : (2 * c + 1) * LANES]
                    raised = value[:, (2 * c + 1) * LANES : (2 * c + 2) * LANES]
                    hidden = (gate / (1.0 + jnp.exp(-gate)) * raised).astype(jnp.bfloat16)
                    hidden = hidden.astype(jnp.float32)
                    for tile in range(tiles):
                        pool_mine[
                            yy, pl.ds(m * tiles + tile, 1), c * LANES : (c + 1) * LANES
                        ] = (
                            jnp.sum(hidden[tile * patch : (tile + 1) * patch], axis=0, keepdims=True)
                            / patch
                        )
            for k in reversed(range(n)):
                if k or other:
                    send(
                        pool_mine.at[yy],
                        pooled.at[place],
                        send_pool.at[0],
                        recv_pool.at[0],
                        {"groups": yy, "seq": ahead(k)},
                    )
        pooled[place] = pool_mine[y]

    for r in range(blocks_k - 1):
        multiply(r)
        if r == 0:
            remote(own_embed, own_embed, send_new.at[0], recv_new.at[0], {"head": mate}).wait_recv()
            for which, event in ((y, 3), (1 - y, 4)):
                embed_copy(beyond, which, event, {"head": mate}).wait_recv()
            for j in range(heads):
                embed_cols[:, j * cols : (j + 1) * cols] = embed_ref[j].T
    pool()


    @pl.when(hd == 0)
    def _():
        seen = mean_in.at[pl.ds(0, n - 1)]
        remote(seen, seen, send_mean.at[0], recv_mean.at[0], {"seq": partner}).wait_recv()
        for k in range(1, n):
            averages[seq_peer(k)] = mean_in[seq_peer(k)]

    slot = pooled.at[pl.ds(0, 2 * n - 1)]
    remote(slot, slot, send_pool.at[0], recv_pool.at[0], {"seq": partner}).wait_recv()
    loads[1].wait()
    everyone = jnp.concatenate(
        [
            jnp.concatenate(
                [pooled[yy * n + b + m] for m in range(2) for yy in range(2)],
                axis=1,
            )
            for b in range(0, n, 2)
        ],
        axis=0,
    )
    high = everyone.astype(jnp.bfloat16)
    rest = everyone - high.astype(jnp.float32)
    middle = rest.astype(jnp.bfloat16)
    low = (rest - middle.astype(jnp.float32)).astype(jnp.bfloat16)
    product = jnp.dot(
        jnp.concatenate([low, middle, high], axis=0),
        down_ref[...],
        preferred_element_type=jnp.float32,
    )
    local_part = sum(product[i * n * tiles : (i + 1) * n * tiles] for i in range(3))
    local_part = local_part * scale_ref[mean_columns(z)].reshape(1, depth) + jnp.concatenate(
        [averages[b] for b in range(n)], axis=0
    )
    here = z * heads + hd
    parts[here] = local_part.astype(jnp.bfloat16)
    for k in reversed(range(n)):
        for j in reversed(range(heads)):
            if k or j:
                send(
                    parts.at[here],
                    parts.at[here],
                    send_part.at[0],
                    recv_part.at[0],
                    {"seq": ahead(k), "head": head_peer(j)},
                )
    for buffer, receives in ((wcol_out, recv_aux.at[0]), (sub_out, recv_aux.at[1])):
        slot = buffer.at[pl.ds(0, heads - 1)]
        remote(slot, slot, send_aux.at[0], receives, {"head": mate}).wait_recv()
    for j in range(heads):
        sub_col[pl.ds(j * cols, cols), :] = column(sub_out[j, 1:2])
    slot = parts.at[pl.ds(0, n * heads - 1)]
    remote(slot, slot, send_part.at[0], recv_part.at[0], {"seq": partner}).wait_recv()
    summed = jnp.concatenate(
        [
            sum(parts[b * heads + j].astype(jnp.float32) for j in range(heads))
            for b in range(n)
        ],
        axis=1,
    )
    feature = normalize(summed, fc_ref[...].reshape(1, width)).astype(jnp.bfloat16)
    shift = jnp.concatenate([sub_out[j, 0:1] for j in range(heads)], axis=1)
    fresh_values = (
        jnp.dot(feature, embed_cols[...], preferred_element_type=jnp.float32) + shift
    ).astype(jnp.bfloat16)
    for j in range(heads):
        new_out[j] = fresh_values[:, j * cols : (j + 1) * cols]
    fresh_values = fresh_values.astype(jnp.float32)

    def peers(buffer, receives):
        slot = buffer.at[pl.ds(0, heads - 1)]
        remote(slot, slot, send_aux.at[0], receives, {"head": mate}).wait_recv()

    normal = normalize(fresh_values, slide_ref[...].reshape(1, features)).astype(jnp.bfloat16)

    def project_new(g):
        return jnp.dot(normal, qkv_cols[g], preferred_element_type=jnp.float32).astype(jnp.bfloat16)

    new_key, new_value = project_new(1), project_new(2)
    new_kv[hd, 0] = new_key
    new_kv[hd, 1] = new_value
    for k in range(1, heads):
        send(new_kv.at[hd], new_kv.at[hd], send_kv.at[0], recv_kv.at[0], {"head": head_peer(k)})
    new_query = project_new(0)
    lane_head = lax.broadcasted_iota(jnp.int32, (1, cols), 1) // HEAD_DIM
    nothing = jnp.zeros((), jnp.bfloat16)

    def by_head(rows_in):
        return jnp.concatenate(
            [jnp.where(lane_head == h, rows_in, nothing) for h in range(head_count)], axis=0
        )

    key_at = lax.broadcasted_iota(jnp.int32, (new_count, total_rows), 1)
    placed = jnp.concatenate([fresh[t, :new_count].astype(jnp.float32) for t in range(n)], axis=1)
    new_at = jnp.sum(placed * key_at.astype(jnp.float32), axis=1, keepdims=True).astype(jnp.int32)
    other = lax.broadcasted_iota(jnp.int32, (1, LANES), 1)
    new_lane = jnp.sum(
        jnp.where(other == lax.broadcasted_iota(jnp.int32, (new_count, LANES), 0), new_at, 0),
        axis=0,
        keepdims=True,
    )[:, :new_count]

    many = by_head(new_query)
    scores = jnp.dot(many, key_cols[...], preferred_element_type=jnp.float32) * factor
    scores = jnp.where(keep_cols[...] > 0.0, scores, masked_score)
    recent = dot_rows(many, new_key) * factor
    recent = jnp.where(new_lane < limit, recent, masked_score)
    peak = jnp.maximum(
        jnp.max(scores, axis=1, keepdims=True), jnp.max(recent, axis=1, keepdims=True)
    )
    row_at = jnp.concatenate([new_at] * head_count, axis=0)
    offset = hd * head_count + lax.broadcasted_iota(
        jnp.int32, (head_count * new_count, 1), 0
    ) // new_count
    weights = jnp.exp(scores - peak) * multiplicity(key_at[:1], row_at, offset)
    recent = jnp.exp(recent - peak) * multiplicity(new_lane, row_at, offset)
    mass = jnp.sum(weights, axis=1, keepdims=True) + jnp.sum(recent, axis=1, keepdims=True)
    attended = (
        jnp.dot(
            weights.astype(jnp.bfloat16), value_rows[...], preferred_element_type=jnp.float32
        )
        + jnp.dot(recent.astype(jnp.bfloat16), new_value, preferred_element_type=jnp.float32)
    ) / mass
    new_mix[hd] = sum(
        jnp.where(lane_head == h, attended[h * new_count : (h + 1) * new_count], 0.0)
        for h in range(head_count)
    ).astype(jnp.bfloat16)
    for k in range(1, heads):
        send(new_mix.at[hd], new_mix.at[hd], send_kv.at[1], recv_kv.at[1], {"head": head_peer(k)})

    for index, buffer in enumerate((mix_query, mix_mass, mix_old)):
        peers(buffer, recv_mix.at[index])
    peers(new_kv, recv_kv.at[0])
    query_at = lax.broadcasted_iota(jnp.int32, (1, step), 1) + z * step
    here_fresh = fresh[z, :new_count]
    known = 1.0 - jnp.sum(here_fresh.astype(jnp.float32), axis=0, keepdims=True)
    known = jnp.where(query_at < limit, known, 0.0)
    betas, alphas = [], []
    for j in range(heads):
        scores = (
            jnp.dot(by_head(new_kv[j, 0]), mix_query[j], preferred_element_type=jnp.float32)
            * factor
        )
        scores = jnp.where(row_at < limit, scores, masked_score)
        offset = j * head_count + lax.broadcasted_iota(
            jnp.int32, (head_count * new_count, 1), 0
        ) // new_count
        grouped = (head_count, new_count, step)
        scores = scores.reshape(grouped)
        stored_mass = mix_mass[j].reshape(grouped)
        ceiling = jnp.maximum(jnp.max(scores, axis=1, keepdims=True), stored_mass)
        weights = jnp.exp(scores - ceiling) * multiplicity(row_at, query_at, offset).reshape(grouped)
        old = jnp.exp(stored_mass - ceiling)
        inverse = known / (old + jnp.sum(weights, axis=1, keepdims=True))
        betas.append((weights * inverse).reshape(head_count * new_count, step))
        alphas.append(old * inverse)

    inside_limit = jnp.where(query_at < limit, here_fresh.astype(jnp.float32), 0.0).astype(
        jnp.bfloat16
    )

    def contract(left, right):
        return lax.dot_general(
            left, right, (((0,), (0,)), ((), ())), preferred_element_type=jnp.float32
        )

    pieces = []
    for j in range(heads):
        share_of = jnp.concatenate(
            [
                mix_old[j, h * HEAD_DIM : (h + 1) * HEAD_DIM, :].astype(jnp.float32)
                * alphas[j][h, :1]
                for h in range(head_count)
            ],
            axis=0,
        )
        pieces.append(share_of + contract(by_head(new_kv[j, 1]), betas[j].astype(jnp.bfloat16)))
    branch = sequence[z, hd].astype(jnp.float32) + contract(new_out[hd], here_fresh)
    peers(new_mix, recv_kv.at[1])
    pieces = [piece + contract(new_mix[j], inside_limit) for j, piece in enumerate(pieces)]
    mean = sum(jnp.sum(p, axis=0, keepdims=True) for p in pieces) / features
    square = sum(jnp.sum(p * p, axis=0, keepdims=True) for p in pieces) / features
    scaling = lax.rsqrt(square - mean * mean + layer_eps)
    for j in range(heads):
        gain = sub_col[pl.ds(j * cols, cols), :]
        settled = ((pieces[j] - mean) * scaling * gain).astype(jnp.bfloat16)
        branch += jnp.dot(wcol_out[j], settled, preferred_element_type=jnp.float32)
    out_ref[...] = branch

    def drain(slot, sends):
        remote(slot, slot, sends, recv_new.at[0], {"head": mate}).wait_send()

    drain(normed.at[pl.ds(0, 3)], send_tok.at[0])
    drain(wall.at[:, :, :, pl.ds(0, (n - 1) * LANES), :], send_w.at[0])
    drain(pre_out.at[0, pl.ds(0, 2)], send_pre.at[0])

    @pl.when(inside)
    def _():
        drain(pre_out.at[0, pl.ds(0, 2)], send_pre.at[1])

    drain(pre_out.at[pl.ds(0, 3)], send_fan.at[0])
    drain(wcol_out.at[pl.ds(0, heads - 1)], send_aux.at[0])
    drain(sub_out.at[pl.ds(0, heads - 1)], send_aux.at[1])
    drain(pooled.at[pl.ds(0, 2 * n - 1)], send_pool.at[0])

    @pl.when(hd == 0)
    def _():
        drain(mean_in.at[pl.ds(0, n - 1)], send_mean.at[0])

    drain(parts.at[pl.ds(0, n * heads - 1)], send_part.at[0])
    drain(own_embed, send_new.at[0])
    drain(embed_ref.at[pl.ds(0, 2)], send_new.at[1])
    for index, buffer in enumerate((mix_query, mix_mass, mix_old)):
        drain(buffer.at[pl.ds(0, heads - 1)], send_mix.at[index])
    drain(new_kv.at[pl.ds(0, heads - 1)], send_kv.at[0])
    drain(new_mix.at[pl.ds(0, heads - 1)], send_kv.at[1])


def near_body(
    tile_tokens,
    tile_gain,
    w_gate_up,
    w_down,
    layer_scale,
    fc_gain,
    w_embed,
    embed_bias,
    pre_emb,
    tile_order,
    valid_count,
    slide_gain,
    w_qkv,
    sub_gain,
    w_out,
):
    n = lax.axis_size("seq")
    heads = lax.axis_size("head")
    tiles, patch, width = tile_tokens.shape
    depth, hidden_width = w_gate_up.shape[1:]
    rows = tiles * patch
    cols = w_embed.shape[1]
    head_count = cols // HEAD_DIM
    total_rows = tile_order.shape[0]
    block_rows = total_rows // n
    vmem = pl.BlockSpec(memory_space=pltpu.VMEM)
    anywhere = pl.BlockSpec(memory_space=pl.ANY)
    dma = pltpu.SemaphoreType.DMA
    f32, bf16 = jnp.float32, jnp.bfloat16
    quarter = rows // heads
    blocks_k = depth // LANES
    blocks_c = hidden_width // 4 // LANES
    out = pl.pallas_call(
        functools.partial(encode_kernel, tiles),
        out_shape=pltpu.VMEM((cols, block_rows), f32),
        in_specs=[pl.BlockSpec(memory_space=pltpu.SMEM)] + [anywhere] * 14,
        out_specs=vmem,
        scratch_shapes=[
            pltpu.VMEM((width,), f32),
            pltpu.VMEM((width,), f32),
            pltpu.VMEM((width,), f32),
            pltpu.VMEM((cols, block_rows - tiles), bf16),
            pltpu.VMEM((cols, heads * cols), bf16),
            pltpu.VMEM((cols,), f32),
            pltpu.VMEM((cols,), f32),
            pltpu.VMEM((total_rows // LANES, LANES), jnp.int32),
            pltpu.VMEM((heads * cols,), f32),
            pltpu.VMEM((rows, width), bf16),
            pltpu.VMEM(w_down.shape, bf16),
            pltpu.VMEM((heads, cols, width), bf16),
            pltpu.VMEM((3, cols, heads * cols), bf16),
            pltpu.VMEM((3, heads * cols, cols), bf16),
            pltpu.VMEM((width, heads * cols), bf16),
            pltpu.VMEM((heads, cols, cols), bf16),
            pltpu.VMEM((2, cols), f32),
            pltpu.VMEM((cols, block_rows), bf16),
            pltpu.VMEM((n, heads, cols, block_rows), bf16),
            pltpu.VMEM((heads, n * tiles, cols), bf16),
            pltpu.VMEM((heads, cols, cols), bf16),
            pltpu.VMEM((heads, 2, cols), f32),
            pltpu.VMEM((n, heads, cols, block_rows), bf16),
            pltpu.VMEM((n, cols, block_rows), bf16),
            pltpu.VMEM((total_rows, cols), bf16),
            pltpu.VMEM((cols, total_rows), bf16),
            pltpu.VMEM((total_rows, cols), bf16),
            pltpu.VMEM((cols, total_rows), bf16),
            pltpu.VMEM((n, LANES, block_rows), bf16),
            pltpu.VMEM((total_rows, 1), f32),
            pltpu.VMEM((1, total_rows), f32),
            pltpu.VMEM((heads * cols, 1), f32),
            pltpu.VMEM((heads * cols, 1), f32),
            pltpu.VMEM((heads, cols, block_rows), bf16),
            pltpu.VMEM((heads, cols, block_rows), bf16),
            pltpu.VMEM((heads, head_count * 8, block_rows), f32),
            pltpu.VMEM((heads, 2, n * tiles, cols), bf16),
            pltpu.VMEM((heads, n * tiles, cols), bf16),
            pltpu.VMEM((4, heads, quarter, width), bf16),
            pltpu.VMEM((blocks_k, blocks_c, 2, n * LANES, LANES), bf16),
            pltpu.VMEM((4, rows, blocks_c * 2 * LANES), f32),
            pltpu.VMEM((2, 2 * tiles, blocks_c * LANES), f32),
            pltpu.VMEM((2 * n, 2 * tiles, blocks_c * LANES), f32),
            pltpu.VMEM((heads, 1, width), f32),
            pltpu.VMEM((tiles, width), f32),
            pltpu.VMEM((n, tiles, depth), f32),
            pltpu.VMEM((n, tiles, depth), f32),
            pltpu.VMEM((n * heads, n * tiles, w_down.shape[1]), bf16),
            dma((17,)),
            dma((1,)),
            dma((6, 2)),
            dma((2,)),
            dma((1,)),
            dma((blocks_k * blocks_c,)),
            dma((2,)),
            dma((n,)),
            dma((1,)),
            dma((n,)),
            dma((2,)),
            dma((2,)),
            dma((1,)),
            dma((1,)),
            dma((1,)),
            dma((1,)),
            dma((1,)),
            dma((1,)),
            dma((2,)),
            dma((5,)),
            dma((3,)),
            dma((3,)),
            dma((2,)),
            dma((2,)),
        ],
        compiler_params=pltpu.CompilerParams(
            collective_id=0, has_side_effects=True, vmem_limit_bytes=58 * 1024 * 1024
        ),
    )(
        valid_count,
        tile_tokens.reshape(rows, width),
        tile_gain,
        layer_scale,
        fc_gain,
        w_gate_up,
        w_down,
        w_embed.T,
        pre_emb.T,
        w_out,
        embed_bias,
        sub_gain,
        tile_order.reshape(total_rows // LANES, LANES),
        slide_gain,
        w_qkv.swapaxes(1, 2),
    )
    return out.T


def body(*args):
    total_rows = args[9].shape[0]
    mesh_fits = all(lax.axis_size(a) == k for a, k in (("groups", 2), ("seq", 4), ("head", 4)))
    if total_rows <= SPAN0 and mesh_fits:
        return near_body(*args)
    return general_body(*args)


def solution(mesh):
    placed = (
        P(("groups", "seq"), None, None),
        P(),
        P(None, "seq", "head"),
        P("head", "seq"),
        P(),
        P(),
        P(None, "head"),
        P("head"),
        P(("groups", "seq"), "head"),
        P("groups"),
        P("groups"),
        P(),
        P(None, None, "head"),
        P("head"),
        P("head", None),
    )
    return jax.shard_map(
        body, mesh=mesh, in_specs=placed, out_specs=P(("groups", "seq"), "head"), check_vma=False
    )
```
